32 devices in a mesh: seq: 8 (over z, x), head: 4 (over y, core).
Axes of the slice: x: 2, y: 2, z: 4, core: 2. Of those that a mesh axis runs over, the one named last changes fastest.
Arguments:
- queries: bfloat16 [2048, 4096], P('seq', 'head'), may hold values from -48 to 48
- key_rows: bfloat16 [2048, 4096], P('seq', 'head'), may hold values from -4 to 4
- value_rows: bfloat16 [2048, 4096], P('seq', 'head'), may hold values from -6 to 6
- out_grad: bfloat16 [2048, 2048], P('seq', 'head'), may hold values from -6 to 6
- out_proj: bfloat16 [4096, 2048], P('head'), may hold values from -0.125 to 0.125
- section_table: int32 [32, 3], P('head'), may hold values 0 or 1
- block_active: int32 [8, 3], P('seq'), may hold values 0 or 1
Outputs:
- query_grad: bfloat16 [2048, 4096], P('seq', 'head')
- key_grad: bfloat16 [2048, 4096], P('seq', 'head')
- value_grad: bfloat16 [2048, 4096], P('seq', 'head')
The draws below stay inside these ranges and needn't reach their ends.
All inputs are finite; a program needn't handle non-finite values.
Results may differ from the reference program's by a relative error of at most 0.008.
Values may be sent and summed in bfloat16 or wider, within the bound.
No kernel may reach another device: no remote copies, remote signals or barrier semaphores. Data moves between devices by JAX's collectives and lax.ppermute only.
A program may use at most 64 MiB of HBM per device.

```python
import math
from functools import partial
from functools import reduce
import jax
import jax.numpy as jnp
from jax import lax

BLK = 256
HEADS = 32
HDIM = 128
DMODEL = 2048
SECTIONS = 3
NBLOCKS = 8
TOKENS = 2048


def paired_fields(key):
    base_key = jax.random.fold_in(key, 4021)
    field_shape = (TOKENS, HEADS * HDIM)
    key_field = jnp.clip(jax.random.normal(jax.random.fold_in(base_key, 1), field_shape, jnp.float32), -4.0, 4.0)
    query_field = jnp.clip(jax.random.normal(jax.random.fold_in(base_key, 2), field_shape, jnp.float32), -4.0, 4.0)
    return (query_field, key_field)


def draw_queries(key, part):
    return paired_fields(key)[0].astype(jnp.bfloat16)


def draw_key_rows(key, part):
    return paired_fields(key)[1].astype(jnp.bfloat16)


def plant(values, key, smallest, top_value):
    shape = values.shape
    spot = [jax.random.randint(jax.random.fold_in(key, axis), (), 0, shape[axis]) for axis in range(len(shape))]
    values = values.at[tuple(spot)].set(smallest)
    longest = shape.index(max(shape))
    spot[longest] = (spot[longest] + 1) % shape[longest]
    return values.at[tuple(spot)].set(top_value)


def steps_of(rng, shape, shards, smallest, largest):
    factor_of, own = 1.0, jax.random.fold_in(rng, 6)
    for dim, shards_of in shards:
        heights = jnp.exp(jax.random.uniform(jax.random.fold_in(own, dim), (shards_of,), jnp.float32, smallest / len(shards), largest / len(shards)))
        factor_of = factor_of * jnp.repeat(heights, shape[dim] // shards_of).reshape([-1 if axis == dim else 1 for axis in range(len(shape))])
    return factor_of


def centred(own_key, dims, width, bound, split=(), held_as=jnp.bfloat16):
    drawn = width * jax.random.normal(own_key, dims, jnp.float32)
    if split:
        drawn = drawn * steps_of(own_key, dims, split, -0.22, 0.18)
    return jnp.clip(drawn, -bound, bound).astype(held_as)


def setup_inputs(seed: int = 0) -> dict:
    key_list = jax.random.split(jax.random.key(seed), 8)
    return {
        "queries": draw_queries(jax.random.fold_in(key_list[7], 71), 0),
        "key_rows": draw_key_rows(jax.random.fold_in(key_list[7], 71), 0),
        "value_rows": centred(key_list[2], (TOKENS, HEADS * HDIM), 1.0, 6.0, ((0, 8), (1, 4))),
        "out_grad": centred(key_list[3], (TOKENS, DMODEL), 1.0, 6.0, ((0, 8), (1, 4))),
        "out_proj": centred(key_list[4], (HEADS * HDIM, DMODEL), DMODEL ** -0.5, 0.125, ((0, 4),)),
        "section_table": plant((jax.random.randint(key_list[5], (HEADS, SECTIONS), 0, 3) < 2).astype(jnp.int32), jax.random.fold_in(key_list[5], 1), 0, 1),
        "block_active": plant((jax.random.randint(key_list[6], (NBLOCKS, SECTIONS), 0, 4) < 3).astype(jnp.int32), jax.random.fold_in(key_list[6], 1), 0, 1),
    }


def shift_down(blocks, count):
    filler = jnp.zeros((count,) + blocks.shape[1:], blocks.dtype)
    return jnp.concatenate([filler, blocks[:blocks.shape[0] - count]], axis=0)

def shift_up(blocks, count):
    filler = jnp.zeros((count,) + blocks.shape[1:], blocks.dtype)
    return jnp.concatenate([blocks[count:], filler], axis=0)

def to_wide(array):
    return array.astype(jnp.float32)

def narrow(array):
    return lax.optimization_barrier(array.astype(jnp.bfloat16)).astype(jnp.float32)

def head_grads(block_active, operands):
    query_h, key_h, value_h, grad_h, head_flags = operands
    score_scale = 1.0 / math.sqrt(HDIM)
    query_wide = to_wide(query_h)
    key_wide = to_wide(key_h)
    value_wide = to_wide(value_h)
    grad_wide = to_wide(grad_h)
    row_ids = jnp.arange(BLK)
    causal = (row_ids[:, None] >= row_ids[None, :])[None]
    block_ids = jnp.arange(NBLOCKS)
    key_sets = [(key_wide, value_wide, causal, 0)]
    for section_index in range(SECTIONS):
        shift_count = NBLOCKS // 2 ** (section_index + 1)
        usable = (head_flags[section_index] * block_active[:, section_index] > 0) & (block_ids >= shift_count)
        key_sets.append((shift_down(key_wide, shift_count), shift_down(value_wide, shift_count), usable[:, None, None], shift_count))
    logits = []
    for key_entry in key_sets:
        raw_scores = jnp.einsum('bid,bjd->bij', query_wide, key_entry[0]) * score_scale
        logits.append(jnp.where(key_entry[2], raw_scores, -1e+30))
    row_max = reduce(jnp.maximum, [lax.optimization_barrier(jnp.max(logit_set, axis=-1)) for logit_set in logits])
    row_sum = reduce(jnp.add, [lax.optimization_barrier(jnp.sum(jnp.exp(logit_set - row_max[..., None]), axis=-1)) for logit_set in logits])
    log_norm = row_max + jnp.log(row_sum)
    probs_list = [jnp.where(key_entry[2], jnp.exp(logit_set - log_norm[..., None]), 0.0) for logit_set, key_entry in zip(logits, key_sets)]
    weight_list = [narrow(prob_set) for prob_set in probs_list]
    context = reduce(jnp.add, [jnp.einsum('bij,bjd->bid', weight_set, key_entry[1]) for weight_set, key_entry in zip(weight_list, key_sets)])
    row_delta = lax.optimization_barrier(jnp.sum(grad_wide * context, axis=-1))
    query_grad = jnp.zeros_like(query_wide)
    key_grad = jnp.zeros_like(query_wide)
    value_grad = jnp.zeros_like(query_wide)
    for set_index in range(SECTIONS + 1):
        key_part, value_part, allowed, shift_count = key_sets[set_index]
        prob_grad = jnp.einsum('bid,bjd->bij', grad_wide, value_part)
        dlogit = narrow(probs_list[set_index] * (prob_grad - row_delta[..., None]) * score_scale)
        query_grad = query_grad + jnp.einsum('bij,bjd->bid', dlogit, key_part)
        key_term = jnp.einsum('bij,bid->bjd', dlogit, query_wide)
        value_term = jnp.einsum('bij,bid->bjd', weight_list[set_index], grad_wide)
        if set_index > 0:
            key_term = narrow(key_term)
            value_term = narrow(value_term)
        key_grad = key_grad + shift_up(key_term, shift_count)
        value_grad = value_grad + shift_up(value_term, shift_count)
    return (query_grad.astype(jnp.bfloat16), key_grad.astype(jnp.bfloat16), value_grad.astype(jnp.bfloat16))

def by_heads(matrix):
    return matrix.reshape(NBLOCKS, BLK, HEADS, HDIM).transpose(2, 0, 1, 3)

def from_heads(stacked):
    return stacked.transpose(1, 2, 0, 3).reshape(TOKENS, HEADS * HDIM)

def reference(queries, key_rows, value_rows, out_grad, out_proj, section_table, block_active):
    attn_grad = jnp.dot(out_grad, out_proj.T, preferred_element_type=jnp.float32).astype(jnp.bfloat16)
    operands = (by_heads(queries), by_heads(key_rows), by_heads(value_rows), by_heads(attn_grad), section_table)
    query_out, key_out, value_out = lax.map(partial(head_grads, block_active), operands)
    return (from_heads(query_out), from_heads(key_out), from_heads(value_out))
```

```python
import math

import jax
import jax.numpy as jnp
from jax import lax
from jax.experimental import pallas as pl
from jax.experimental.pallas import tpu as pltpu
from jax.sharding import PartitionSpec as P

HDIM = 128
SECTIONS = 3
CHUNK_HEADS = 2
NEG = -1e30
SCALE = 1.0 / math.sqrt(HDIM)
EXP_SCALE = SCALE * math.log2(math.e)


def shift(value, steps):
    count = lax.axis_size("seq")
    low, high = max(0, -steps), min(count, count - steps)
    return lax.ppermute(value, "seq", [(src, src + steps) for src in range(low, high)])


def swap(value, axis, bit):
    return lax.ppermute(value, axis, [(src, src ^ bit) for src in range(lax.axis_size(axis))])


def dot(lhs, rhs, lhs_dim, rhs_dim):
    return lax.dot_general(
        lhs, rhs, (((lhs_dim,), (rhs_dim,)), ((), ())), preferred_element_type=jnp.float32
    )


def gathered_pieces(out_grad):
    pieces = {0: out_grad}
    bit = lax.axis_size("head") // 2
    while bit:
        for offset in list(pieces):
            pieces[offset | bit] = swap(pieces[offset], "head", bit)
        bit //= 2
    return [pieces[offset] for offset in range(len(pieces))]


def grad_kernel(head_ref, *refs):
    *piece_refs, proj_ref, out_ref = refs
    width = piece_refs[0].shape[1]
    total = None
    for offset, piece in enumerate(piece_refs):
        start = pl.multiple_of((head_ref[0] ^ offset) * width, width)
        part = dot(piece[...], proj_ref[:, pl.ds(start, width)], 1, 1)
        total = part if total is None else total + part
    out_ref[...] = total.astype(out_ref.dtype)


def attn_grad_of(out_grad, out_proj):
    pieces = gathered_pieces(out_grad)
    rows, width = out_grad.shape
    cols, features = out_proj.shape
    block = 2 * HDIM
    return pl.pallas_call(
        grad_kernel,
        grid=(cols // block,),
        in_specs=[pl.BlockSpec(memory_space=pltpu.SMEM)]
        + [pl.BlockSpec((rows, width), lambda i: (0, 0)) for _ in pieces]
        + [pl.BlockSpec((block, features), lambda i: (i, 0))],
        out_specs=pl.BlockSpec((rows, block), lambda i: (0, i)),
        out_shape=jax.ShapeDtypeStruct((rows, cols), jnp.bfloat16),
        cost_estimate=pl.CostEstimate(
            flops=2 * rows * cols * features,
            bytes_accessed=2 * (rows * features + cols * features + rows * cols),
            transcendentals=0,
        ),
        name="grad_matmul",
    )(lax.axis_index("head").astype(jnp.int32).reshape(1), *pieces, out_proj)


def attn_kernel(first_head, usable_ref, q_ref, g_ref, *refs):
    sets = refs[:4]
    dq_ref, own_ref, near_ref, mid_ref, far_ref, score, pgrad = refs[-7:]
    outs = (own_ref, near_ref, mid_ref, far_ref)
    head = first_head + pl.program_id(0)
    rows = q_ref.shape[0]
    query = q_ref[...]
    grad = g_ref[...]
    key_at = lax.broadcasted_iota(jnp.int32, (rows, rows), 0)
    query_at = lax.broadcasted_iota(jnp.int32, (rows, rows), 1)
    bias = [0.0] + [jnp.where(usable_ref[head, k] > 0, 0.0, NEG) for k in range(3)]
    top = None
    for k, kv in enumerate(sets):
        raw = dot(kv[:rows, :], query, 1, 1)
        if k == 0:
            raw = jnp.where(key_at <= query_at, raw, NEG)
        score[k] = raw
        peak = jnp.max(raw, axis=0, keepdims=True) + bias[k]
        top = peak if top is None else jnp.maximum(top, peak)
    norm = jnp.zeros((1, rows), jnp.float32)
    delta = jnp.zeros((1, rows), jnp.float32)
    for k, kv in enumerate(sets):
        prob = jnp.exp2((score[k] - (top - bias[k])) * EXP_SCALE)
        pg = dot(kv[rows:, :], grad, 1, 1)
        norm = norm + jnp.sum(prob, axis=0, keepdims=True)
        delta = delta + jnp.sum(prob * pg, axis=0, keepdims=True)
        score[k] = prob
        pgrad[k] = pg
    inv = 1.0 / norm
    delta = delta * inv
    dq = None
    for k, kv in enumerate(sets):
        prob = score[k] * inv
        weight = prob.astype(jnp.bfloat16)
        dlogit = (prob * (pgrad[k] - delta)).astype(jnp.bfloat16)
        out = outs[k]
        out[:rows, :] = (dot(dlogit, query, 1, 0) * SCALE).astype(out.dtype)
        out[rows:, :] = dot(weight, grad, 1, 0).astype(out.dtype)
        part = dot(kv[:rows, :], dlogit, 0, 0)
        dq = part if dq is None else dq + part
    dq_ref[...] = (dq * SCALE).T.astype(dq_ref.dtype)


def attention_chunk(chunk, heads, usable, queries, grads, key_sets, previous):
    rows = queries.shape[0]
    width = heads * HDIM
    first = chunk * heads

    def wide(i):
        return (0, first + i)

    def local(i):
        return (0, i)

    term = pl.BlockSpec((2 * rows, HDIM), local)
    in_specs = [
        pl.BlockSpec(memory_space=pltpu.SMEM),
        pl.BlockSpec((rows, HDIM), wide),
        pl.BlockSpec((rows, HDIM), wide),
    ] + [term] * 4
    args = [usable, queries, grads, *key_sets]
    aliases = {}
    if previous is not None:
        in_specs.append(pl.BlockSpec(memory_space=pl.ANY))
        args.append(previous)
        aliases = {len(args) - 1: 0}
    sent = jax.ShapeDtypeStruct((2 * rows, width), jnp.bfloat16)

    def body(*refs):
        attn_kernel(first, *refs)

    return pl.pallas_call(
        body,
        grid=(heads,),
        in_specs=in_specs,
        out_specs=[pl.BlockSpec((rows, HDIM), wide)] + [term] * 4,
        out_shape=[
            jax.ShapeDtypeStruct(queries.shape, jnp.bfloat16),
            jax.ShapeDtypeStruct((2 * rows, width), jnp.float32),
            sent,
            sent,
            sent,
        ],
        scratch_shapes=[
            pltpu.VMEM((4, rows, rows), jnp.float32),
            pltpu.VMEM((4, rows, rows), jnp.float32),
        ],
        input_output_aliases=aliases,
        cost_estimate=pl.CostEstimate(
            flops=heads * 4 * 5 * 2 * rows * rows * HDIM * 2,
            bytes_accessed=heads * rows * HDIM * 2 * 20,
            transcendentals=heads * 4 * rows * rows,
        ),
        name="attn_chunk",
    )(*args)


def finish_kernel(odd_ref, own_ref, far_ref, near_ref, *refs):
    key_ref, value_ref = refs[-2:]
    rows = key_ref.shape[0]
    near = near_ref[...].astype(jnp.float32)
    near = jnp.where(odd_ref[0] > 0, jnp.zeros_like(near), near)
    total = own_ref[...] + far_ref[...].astype(jnp.float32) + near
    key_ref[...] = total[:rows].astype(key_ref.dtype)
    value_ref[...] = total[rows:].astype(value_ref.dtype)


def finish_chunk(chunk, odd, own, far, near, shape, previous):
    rows = shape[0]
    width = own.shape[1]
    whole = pl.BlockSpec((2 * rows, width), lambda i: (0, 0))
    in_specs = [pl.BlockSpec(memory_space=pltpu.SMEM), whole, whole, whole]
    args = [odd, own, far, near]
    aliases = {}
    if previous is not None:
        in_specs += [pl.BlockSpec(memory_space=pl.ANY)] * 2
        args += list(previous)
        aliases = {4: 0, 5: 1}
    out = jax.ShapeDtypeStruct(shape, jnp.bfloat16)
    return pl.pallas_call(
        finish_kernel,
        grid=(1,),
        in_specs=in_specs,
        out_specs=[pl.BlockSpec((rows, width), lambda i: (0, chunk))] * 2,
        out_shape=[out, out],
        input_output_aliases=aliases,
        cost_estimate=pl.CostEstimate(
            flops=4 * rows * width, bytes_accessed=24 * rows * width, transcendentals=0
        ),
        name="finish_chunk",
    )(*args)


def body(queries, key_rows, value_rows, out_grad, out_proj, section_table, block_active):
    seq_count = lax.axis_size("seq")
    position = lax.axis_index("seq")
    spans = [seq_count // 2 ** (index + 1) for index in range(SECTIONS)]
    far_span, mid_span, near_span = spans
    assert far_span == 2 * mid_span and mid_span == 2 * near_span
    rows, cols = queries.shape
    heads = CHUNK_HEADS
    width = heads * HDIM
    chunks = cols // width
    is_odd = (position // near_span) % 2 == 1
    odd = is_odd.astype(jnp.int32).reshape(1)
    reach = jnp.stack([position >= span for span in reversed(spans)]).astype(jnp.int32)
    usable = section_table[:, ::-1] * block_active[:, ::-1] * reach[None, :]

    packed = [
        jnp.concatenate(
            [array[:, chunk * width : (chunk + 1) * width] for array in (key_rows, value_rows)],
            axis=0,
        )
        for chunk in range(chunks)
    ]
    received = []
    for own in packed:
        mid = shift(own, mid_span)
        far = shift(mid, mid_span)
        near = swap(jnp.where(is_odd, mid, own), "seq", near_span)
        received.append((own, near, mid, far))
    grads = attn_grad_of(out_grad, out_proj)
    query_grad = None
    finished = None
    for chunk in range(chunks):
        query_grad, own, near, mid, far = attention_chunk(
            chunk, heads, usable, queries, grads, received[chunk], query_grad
        )
        far_back = shift(far, -mid_span)
        near_back = swap(near, "seq", near_span)
        relay = mid.astype(jnp.float32) + far_back.astype(jnp.float32)
        relay = relay + jnp.where(is_odd, near_back.astype(jnp.float32), 0.0)
        mid_back = shift(relay.astype(jnp.bfloat16), -mid_span)
        finished = finish_chunk(chunk, odd, own, mid_back, near_back, queries.shape, finished)
    return query_grad, finished[0], finished[1]


def solution(mesh):
    return jax.shard_map(
        body,
        mesh=mesh,
        in_specs=(
            P("seq", "head"),
            P("seq", "head"),
            P("seq", "head"),
            P("seq", "head"),
            P("head", None),
            P("head", None),
            P("seq", None),
        ),
        out_specs=(P("seq", "head"), P("seq", "head"), P("seq", "head")),
        check_vma=False,
    )
```

```python
import math

import jax
import jax.numpy as jnp
from jax import lax
from jax.experimental import pallas as pl
from jax.experimental.pallas import tpu as pltpu
from jax.sharding import PartitionSpec as P


HDIM = 128
SECTIONS = 3
CHUNK_HEADS = 2
NEG = -1e30
SCALE = 1.0 / math.sqrt(HDIM)
EXP_SCALE = SCALE * math.log2(math.e)


def shift(value, steps):
    count = lax.axis_size("seq")
    low, high = max(0, -steps), min(count, count - steps)
    return lax.ppermute(value, "seq", [(src, src + steps) for src in range(low, high)])


def swap(value, axis, bit):
    return lax.ppermute(value, axis, [(src, src ^ bit) for src in range(lax.axis_size(axis))])


def dot(lhs, rhs, lhs_dim, rhs_dim):
    return lax.dot_general(
        lhs, rhs, (((lhs_dim,), (rhs_dim,)), ((), ())), preferred_element_type=jnp.float32
    )


def gathered_pieces(out_grad):
    pieces = {0: out_grad}
    bit = lax.axis_size("head") // 2
    while bit:
        for offset in list(pieces):
            pieces[offset | bit] = swap(pieces[offset], "head", bit)
        bit //= 2
    return [pieces[offset] for offset in range(len(pieces))]


def grad_kernel(head_ref, *refs):
    *piece_refs, proj_ref, out_ref = refs
    width = piece_refs[0].shape[1]
    total = None
    for offset, piece in enumerate(piece_refs):
        start = pl.multiple_of((head_ref[0] ^ offset) * width, width)
        part = dot(piece[...], proj_ref[:, pl.ds(start, width)], 1, 1)
        total = part if total is None else total + part
    out_ref[...] = total.astype(out_ref.dtype)


def attn_grad_of(out_grad, out_proj):
    pieces = gathered_pieces(out_grad)
    rows, width = out_grad.shape
    cols, features = out_proj.shape
    block = 2 * HDIM
    return pl.pallas_call(
        grad_kernel,
        grid=(cols // block,),
        in_specs=[pl.BlockSpec(memory_space=pltpu.SMEM)]
        + [pl.BlockSpec((rows, width), lambda i: (0, 0)) for _ in pieces]
        + [pl.BlockSpec((block, features), lambda i: (i, 0))],
        out_specs=pl.BlockSpec((rows, block), lambda i: (0, i)),
        out_shape=jax.ShapeDtypeStruct((rows, cols), jnp.bfloat16),
        cost_estimate=pl.CostEstimate(
            flops=2 * rows * cols * features,
            bytes_accessed=2 * (rows * features + cols * features + rows * cols),
            transcendentals=0,
        ),
        name="grad_matmul",
    )(lax.axis_index("head").astype(jnp.int32).reshape(1), *pieces, out_proj)


def attn_kernel(first_head, usable_ref, q_ref, g_ref, *refs):
    sets = refs[:4]
    dq_ref, own_ref, near_ref, mid_ref, far_ref, score, pgrad = refs[-7:]
    outs = (own_ref, near_ref, mid_ref, far_ref)
    head = first_head + pl.program_id(0)
    rows = q_ref.shape[0]
    query = q_ref[...]
    grad = g_ref[...]
    key_at = lax.broadcasted_iota(jnp.int32, (rows, rows), 0)
    query_at = lax.broadcasted_iota(jnp.int32, (rows, rows), 1)
    bias = [0.0] + [jnp.where(usable_ref[head, k] > 0, 0.0, NEG) for k in range(3)]
    top = None
    for k, kv in enumerate(sets):
        raw = dot(kv[:rows, :], query, 1, 1)
        if k == 0:
            raw = jnp.where(key_at <= query_at, raw, NEG)
        score[k] = raw
        peak = jnp.max(raw, axis=0, keepdims=True) + bias[k]
        top = peak if top is None else jnp.maximum(top, peak)
    norm = jnp.zeros((1, rows), jnp.float32)
    delta = jnp.zeros((1, rows), jnp.float32)
    for k, kv in enumerate(sets):
        prob = jnp.exp2((score[k] - (top - bias[k])) * EXP_SCALE)
        pg = dot(kv[rows:, :], grad, 1, 1)
        norm = norm + jnp.sum(prob, axis=0, keepdims=True)
        delta = delta + jnp.sum(prob * pg, axis=0, keepdims=True)
        score[k] = prob
        pgrad[k] = pg
    inv = 1.0 / norm
    delta = delta * inv
    dq = None
    for k, kv in enumerate(sets):
        prob = score[k] * inv
        weight = prob.astype(jnp.bfloat16)
        dlogit = (prob * (pgrad[k] - delta)).astype(jnp.bfloat16)
        out = outs[k]
        out[:rows, :] = (dot(dlogit, query, 1, 0) * SCALE).astype(out.dtype)
        out[rows:, :] = dot(weight, grad, 1, 0).astype(out.dtype)
        part = dot(kv[:rows, :], dlogit, 0, 0)
        dq = part if dq is None else dq + part
    dq_ref[...] = (dq * SCALE).T.astype(dq_ref.dtype)


def attention_chunk(chunk, heads, usable, queries, grads, key_sets, previous):
    rows = queries.shape[0]
    width = heads * HDIM
    first = chunk * heads

    def wide(i):
        return (0, first + i)

    def local(i):
        return (0, i)

    term = pl.BlockSpec((2 * rows, HDIM), local)
    in_specs = [
        pl.BlockSpec(memory_space=pltpu.SMEM),
        pl.BlockSpec((rows, HDIM), wide),
        pl.BlockSpec((rows, HDIM), wide),
    ] + [term] * 4
    args = [usable, queries, grads, *key_sets]
    aliases = {}
    if previous is not None:
        in_specs.append(pl.BlockSpec(memory_space=pl.ANY))
        args.append(previous)
        aliases = {len(args) - 1: 0}
    sent = jax.ShapeDtypeStruct((2 * rows, width), jnp.bfloat16)

    def body(*refs):
        attn_kernel(first, *refs)

    return pl.pallas_call(
        body,
        grid=(heads,),
        in_specs=in_specs,
        out_specs=[pl.BlockSpec((rows, HDIM), wide)] + [term] * 4,
        out_shape=[
            jax.ShapeDtypeStruct(queries.shape, jnp.bfloat16),
            jax.ShapeDtypeStruct((2 * rows, width), jnp.float32),
            sent,
            sent,
            sent,
        ],
        scratch_shapes=[
            pltpu.VMEM((4, rows, rows), jnp.float32),
            pltpu.VMEM((4, rows, rows), jnp.float32),
        ],
        input_output_aliases=aliases,
        cost_estimate=pl.CostEstimate(
            flops=heads * 4 * 5 * 2 * rows * rows * HDIM * 2,
            bytes_accessed=heads * rows * HDIM * 2 * 20,
            transcendentals=heads * 4 * rows * rows,
        ),
        name="attn_chunk",
    )(*args)


def body(queries, key_rows, value_rows, out_grad, out_proj, section_table, block_active):
    seq_count = lax.axis_size("seq")
    position = lax.axis_index("seq")
    spans = [seq_count // 2 ** (index + 1) for index in range(SECTIONS)]
    far_span, mid_span, near_span = spans
    assert far_span == 2 * mid_span and mid_span == 2 * near_span
    rows, cols = queries.shape
    heads = CHUNK_HEADS
    width = heads * HDIM
    chunks = cols // width
    is_odd = (position // near_span) % 2 == 1
    reach = jnp.stack([position >= span for span in reversed(spans)]).astype(jnp.int32)
    usable = section_table[:, ::-1] * block_active[:, ::-1] * reach[None, :]

    packed = [
        jnp.concatenate(
            [array[:, chunk * width : (chunk + 1) * width] for array in (key_rows, value_rows)],
            axis=0,
        )
        for chunk in range(chunks)
    ]
    received = []
    for own in packed:
        mid = shift(own, mid_span)
        far = shift(mid, mid_span)
        near = swap(jnp.where(is_odd, mid, own), "seq", near_span)
        received.append((own, near, mid, far))
    grads = attn_grad_of(out_grad, out_proj)
    query_grad = None
    key_grad = jnp.zeros(queries.shape, jnp.bfloat16)
    value_grad = jnp.zeros(queries.shape, jnp.bfloat16)
    for chunk in range(chunks):
        query_grad, own, near, mid, far = attention_chunk(
            chunk, heads, usable, queries, grads, received[chunk], query_grad
        )
        far_back = shift(far, -mid_span)
        near_back = swap(near, "seq", near_span)
        relay = mid.astype(jnp.float32) + far_back.astype(jnp.float32)
        relay = relay + jnp.where(is_odd, near_back.astype(jnp.float32), 0.0)
        mid_back = shift(relay.astype(jnp.bfloat16), -mid_span)
        total = own + mid_back.astype(jnp.float32)
        total = total + jnp.where(is_odd, 0.0, near_back.astype(jnp.float32))
        total = total.astype(jnp.bfloat16)
        key_grad = lax.dynamic_update_slice(key_grad, total[:rows], (0, chunk * width))
        value_grad = lax.dynamic_update_slice(value_grad, total[rows:], (0, chunk * width))
    return query_grad, key_grad, value_grad


def solution(mesh):
    return jax.shard_map(
        body,
        mesh=mesh,
        in_specs=(
            P("seq", "head"),
            P("seq", "head"),
            P("seq", "head"),
            P("seq", "head"),
            P("head", None),
            P("head", None),
            P("seq", None),
        ),
        out_specs=(P("seq", "head"), P("seq", "head"), P("seq", "head")),
        check_vma=False,
    )
```

```python
import math

import jax
import jax.numpy as jnp
from jax import lax
from jax.experimental import pallas as pl
from jax.experimental.pallas import tpu as pltpu
from jax.sharding import PartitionSpec as P


HDIM = 128
FAR, MID, NEAR = range(3)
SECTIONS = 3
GROUPS = 2
STAT_ROWS = 8
BIG = 1e30
SCALE = 1.0 / math.sqrt(HDIM)
LOG2E = math.log2(math.e)
EXP_SCALE = SCALE * LOG2E


def shift(value, steps):
    count = lax.axis_size("seq")
    low, high = max(0, -steps), min(count, count - steps)
    return lax.ppermute(value, "seq", [(src, src + steps) for src in range(low, high)])


def swap(value, axis, bit):
    pairs = [(src, src ^ bit) for src in range(lax.axis_size(axis))]
    return lax.ppermute(value, axis, pairs)


def dot(lhs, rhs, lhs_dim, rhs_dim):
    return lax.dot_general(
        lhs, rhs, (((lhs_dim,), (rhs_dim,)), ((), ())), preferred_element_type=jnp.float32
    )


def call(kernel, grid, ins, outs, work, aliases=None, scratch=()):
    arrays, in_specs = zip(*ins)
    shapes, out_specs = zip(*outs)
    moved = sum(math.prod(a.shape) * a.dtype.itemsize for a in (*arrays, *shapes))
    return pl.pallas_call(
        kernel,
        grid=grid,
        in_specs=in_specs,
        out_specs=out_specs,
        out_shape=shapes,
        scratch_shapes=scratch,
        input_output_aliases=aliases or {},
        cost_estimate=pl.CostEstimate(
            flops=2 * work, bytes_accessed=moved, transcendentals=work // HDIM
        ),
    )(*arrays)


def gathered_pieces(out_grad):
    pieces = {0: out_grad}
    bit = lax.axis_size("head") // 2
    while bit:
        for offset in list(pieces):
            pieces[offset | bit] = swap(pieces[offset], "head", bit)
        bit //= 2
    return [pieces[offset] for offset in range(len(pieces))]


def grad_kernel(head_ref, *refs):
    *piece_refs, proj_ref, out_ref = refs
    width = piece_refs[0].shape[1]
    total = None
    for offset, piece in enumerate(piece_refs):
        start = pl.multiple_of((head_ref[0] ^ offset) * width, width)
        part = dot(piece[...], proj_ref[:, pl.ds(start, width)], 1, 1)
        total = part if total is None else total + part
    out_ref[...] = total.astype(out_ref.dtype)


def attn_grad_of(out_grad, out_proj):
    pieces = gathered_pieces(out_grad)
    rows, width = out_grad.shape
    cols, features = out_proj.shape
    block = 2 * HDIM
    head = lax.axis_index("head").astype(jnp.int32).reshape(1)
    (result,) = call(
        grad_kernel,
        (cols // block,),
        [(head, pl.BlockSpec(memory_space=pltpu.SMEM))]
        + [(piece, pl.BlockSpec((rows, width), lambda i: (0, 0))) for piece in pieces]
        + [(out_proj, pl.BlockSpec((block, features), lambda i: (i, 0)))],
        [
            (
                jax.ShapeDtypeStruct((rows, cols), jnp.bfloat16),
                pl.BlockSpec((rows, block), lambda i: (0, i)),
            )
        ],
        rows * cols * features,
    )
    return result


def causal(raw, fill):
    key_at = lax.broadcasted_iota(jnp.int32, raw.shape, 0)
    query_at = lax.broadcasted_iota(jnp.int32, raw.shape, 1)
    return jnp.where(key_at <= query_at, raw, fill)


class Flags:
    def __init__(self, spans, table_ref, active_ref, place_ref):
        self.spans, self.table = spans, table_ref
        self.active, self.place = active_ref, place_ref

    def usable(self, head, section):
        used = self.table[head, section] * self.active[0, section] > 0
        return used & (self.place[0] >= self.spans[section])

    def is_odd(self):
        return (self.place[0] // self.spans[NEAR]) % 2 == 1


def row_stats(raws, pgrads):
    top = None
    for raw in raws:
        peak = jnp.max(raw, axis=0, keepdims=True)
        top = peak if top is None else jnp.maximum(top, peak)
    norm, delta = 0.0, 0.0
    for raw, pgrad in zip(raws, pgrads):
        prob = jnp.exp2((raw - top) * EXP_SCALE)
        norm = norm + jnp.sum(prob, axis=0, keepdims=True)
        delta = delta + jnp.sum(prob * pgrad, axis=0, keepdims=True)
    return top, norm, delta


def put_rows(ref, *rows):
    for index, row in enumerate(rows):
        ref[0, index : index + 1, :] = row


def stats_own_kernel(spans, t, a, p, q, g, k, v, k_up, v_up, out):
    flags = Flags(spans, t, a, p)
    bias = jnp.where(flags.usable(pl.program_id(0), MID), 0.0, -BIG)
    query, grad = q[...], g[...]
    raws = [causal(dot(k[...], query, 1, 1), -BIG), dot(k_up[...], query, 1, 1) + bias]
    pgrads = [dot(v[...], grad, 1, 1), dot(v_up[...], grad, 1, 1)]
    put_rows(out, *row_stats(raws, pgrads))


def near_keys(odd, own, up):
    return jnp.where(odd, up[...], own[...])


def stats_guest_kernel(spans, t, a, p, qf, gf, qn, gn, k, v, k_up, v_up, far, near):
    odd = Flags(spans, t, a, p).is_odd()
    for query, grad, keys, values, out in (
        (qf, gf, k_up[...], v_up[...], far),
        (qn, gn, near_keys(odd, k, k_up), near_keys(odd, v, v_up), near),
    ):
        raw = dot(keys, query[...], 1, 1)
        pgrad = dot(values, grad[...], 1, 1)
        put_rows(out, *row_stats([raw], [pgrad]))


def combine_kernel(spans, t, a, p, own, far, near, own_out, far_out, near_out):
    flags = Flags(spans, t, a, p)
    for head in range(own.shape[0]):
        uses = [(own, True, own_out)]
        uses += [(far, flags.usable(head, FAR), far_out)]
        uses += [(near, flags.usable(head, NEAR), near_out)]
        peaks = []
        for ref, usable, _ in uses:
            peak = ref[head, 0:1, :]
            peaks.append(peak if usable is True else jnp.where(usable, peak, -BIG))
        top = jnp.maximum(jnp.maximum(peaks[0], peaks[1]), peaks[2])
        norm, delta = 0.0, 0.0
        for (ref, _, _), peak in zip(uses, peaks):
            factor = jnp.exp2((peak - top) * EXP_SCALE)
            norm = norm + factor * ref[head, 1:2, :]
            delta = delta + factor * ref[head, 2:3, :]
        offset = top * EXP_SCALE + jnp.log(norm) * LOG2E
        delta = delta / norm
        for _, usable, out in uses:
            out[head, 0:1, :] = offset if usable is True else jnp.where(usable, offset, BIG)
            out[head, 1:2, :] = delta


def pair_terms(query, grad, keys, values, offset, delta, diagonal=False):
    raw = dot(keys, query, 1, 1)
    prob = jnp.exp2(raw * EXP_SCALE - offset)
    if diagonal:
        prob = causal(prob, 0.0)
    pgrad = dot(values, grad, 1, 1)
    weight = prob.astype(jnp.bfloat16)
    dlogit = (prob * (pgrad - delta)).astype(jnp.bfloat16)
    key_term = dot(dlogit, query, 1, 0)
    value_term = dot(weight, grad, 1, 0)
    query_term = dot(keys, dlogit, 0, 0)
    return query_term, key_term, value_term


def own_kernel(q, g, k, v, stats, dq, dk, dv):
    query_term, key_term, value_term = pair_terms(
        q[...], g[...], k[...], v[...], stats[0, 0:1, :], stats[0, 1:2, :], True
    )
    dq[...] = query_term.T
    dk[...] = key_term
    dv[...] = value_term


def pairs_kernel(
    spans, first, t, a, p, q, g, qf, gf, qn, gn, k, v, k_up, v_up, own_st, far_st, near_st,
    dq_own, dk_own, dv_own, *refs,
):
    dq, dqf, dqn, back, dk, dv = refs[-6:]
    flags = Flags(spans, t, a, p)
    odd = flags.is_odd()
    rows = q.shape[0]
    bias = jnp.where(flags.usable(first + pl.program_id(0), MID), 0.0, BIG)
    keys, values = k_up[...], v_up[...]
    query_term, key_up, value_up = pair_terms(
        q[...], g[...], keys, values, own_st[0, 0:1, :] + bias, own_st[0, 1:2, :]
    )
    dq[...] = (dq_own[...] + query_term.T) * SCALE
    query_term, key_term, value_term = pair_terms(
        qf[...], gf[...], keys, values, far_st[0, 0:1, :], far_st[0, 1:2, :]
    )
    dqf[...] = (query_term * SCALE).T.astype(dqf.dtype)
    key_up = key_up + key_term
    value_up = value_up + value_term
    query_term, key_term, value_term = pair_terms(
        qn[...], gn[...], near_keys(odd, k, k_up), near_keys(odd, v, v_up),
        near_st[0, 0:1, :], near_st[0, 1:2, :],
    )
    dqn[...] = (query_term * SCALE).T.astype(dqn.dtype)
    zero = jnp.zeros_like(key_term)
    back[:rows, :] = ((key_up + jnp.where(odd, key_term, zero)) * SCALE).astype(back.dtype)
    back[rows:, :] = (value_up + jnp.where(odd, value_term, zero)).astype(back.dtype)
    dk[...] = (dk_own[...] + jnp.where(odd, zero, key_term)) * SCALE
    dv[...] = dv_own[...] + jnp.where(odd, zero, value_term)


def body(queries, key_rows, value_rows, out_grad, out_proj, section_table, block_active):
    seq_count = lax.axis_size("seq")
    place = lax.axis_index("seq")
    spans = [seq_count // 2 ** (index + 1) for index in range(SECTIONS)]
    mid_span, near_span = spans[MID], spans[NEAR]
    assert spans[FAR] == 2 * mid_span and mid_span == 2 * near_span
    assert block_active.shape[0] == 1
    rows, cols = queries.shape
    heads = cols // HDIM
    group = heads // GROUPS
    pair_work = rows * rows * HDIM

    smem = pl.BlockSpec(memory_space=pltpu.SMEM)
    flags = [
        (section_table, smem),
        (block_active, smem),
        (place.astype(jnp.int32).reshape(1), smem),
    ]

    def tile(first=0):
        return pl.BlockSpec((rows, HDIM), lambda i: (0, first + i))

    def stat(first=0):
        return pl.BlockSpec((1, STAT_ROWS, rows), lambda i: (first + i, 0, 0))

    def tiles(*arrays, first=0):
        return [(array, tile(first)) for array in arrays]

    stat_shape = jax.ShapeDtypeStruct((heads, STAT_ROWS, rows), jnp.float32)
    wide_f32 = jax.ShapeDtypeStruct((rows, cols), jnp.float32)
    wide_bf16 = jax.ShapeDtypeStruct((rows, cols), jnp.bfloat16)

    key_up = shift(key_rows, mid_span)
    value_up = shift(value_rows, mid_span)
    query_far = shift(queries, -mid_span)
    query_near = swap(queries, "seq", near_span)
    grads = attn_grad_of(out_grad, out_proj)
    grad_far = shift(grads, -mid_span)
    grad_near = swap(grads, "seq", near_span)

    local = (key_rows, value_rows, key_up, value_up)
    guests = (query_far, grad_far, query_near, grad_near)

    def stats_own(*refs):
        stats_own_kernel(spans, *refs)

    def stats_guest(*refs):
        stats_guest_kernel(spans, *refs)

    def combine(*refs):
        combine_kernel(spans, *refs)

    (own_stats,) = call(
        stats_own,
        (heads,),
        flags + tiles(queries, grads, *local),
        [(stat_shape, stat())],
        heads * 4 * pair_work,
    )
    far_stats, near_stats = call(
        stats_guest,
        (heads,),
        flags + tiles(*guests, *local),
        [(stat_shape, stat())] * 2,
        heads * 4 * pair_work,
    )
    far_stats = shift(far_stats, mid_span)
    near_stats = swap(near_stats, "seq", near_span)
    whole = pl.BlockSpec((heads, STAT_ROWS, rows), lambda i: (0, 0, 0))
    own_norm, far_norm, near_norm = call(
        combine,
        (1,),
        flags + [(array, whole) for array in (own_stats, far_stats, near_stats)],
        [(stat_shape, whole)] * 3,
        heads * rows * HDIM,
    )
    far_norm = shift(far_norm, -mid_span)
    near_norm = swap(near_norm, "seq", near_span)
    own_parts = call(
        own_kernel,
        (heads,),
        tiles(queries, grads, key_rows, value_rows) + [(own_norm, stat())],
        [(wide_f32, tile())] * 3,
        heads * 5 * pair_work,
    )

    query_part = query_far_part = query_near_part = None
    key_grad = jnp.zeros((rows, cols), jnp.bfloat16)
    value_grad = jnp.zeros((rows, cols), jnp.bfloat16)
    for index in range(GROUPS):
        first = index * group

        def pairs(*refs, first=first):
            pairs_kernel(spans, first, *refs)

        ins = flags + tiles(queries, grads, *guests, *local, first=first)
        ins += [(array, stat(first)) for array in (own_norm, far_norm, near_norm)]
        ins += tiles(*own_parts, first=first)
        aliases = {}
        if index:
            for number, array in enumerate((query_part, query_far_part, query_near_part)):
                aliases[len(ins)] = number
                ins.append((array, pl.BlockSpec(memory_space=pl.ANY)))
        half_f32 = jax.ShapeDtypeStruct((rows, group * HDIM), jnp.float32)
        half_back = jax.ShapeDtypeStruct((2 * rows, group * HDIM), jnp.bfloat16)
        query_part, query_far_part, query_near_part, back, key_part, value_part = call(
            pairs,
            (group,),
            ins,
            [
                (wide_f32, tile(first)),
                (wide_bf16, tile(first)),
                (wide_bf16, tile(first)),
                (half_back, pl.BlockSpec((2 * rows, HDIM), lambda i: (0, i))),
                (half_f32, tile()),
                (half_f32, tile()),
            ],
            group * 15 * pair_work,
            aliases,
        )
        back = shift(back, -mid_span).astype(jnp.float32)
        key_part = (key_part + back[:rows]).astype(jnp.bfloat16)
        value_part = (value_part + back[rows:]).astype(jnp.bfloat16)
        at = (0, first * HDIM)
        key_grad = lax.dynamic_update_slice(key_grad, key_part, at)
        value_grad = lax.dynamic_update_slice(value_grad, value_part, at)
    query_far_part = shift(query_far_part, mid_span)
    query_near_part = swap(query_near_part, "seq", near_span)
    query_grad = query_part + query_far_part.astype(jnp.float32)
    query_grad = query_grad + query_near_part.astype(jnp.float32)
    return query_grad.astype(jnp.bfloat16), key_grad, value_grad


def solution(mesh):
    return jax.shard_map(
        body,
        mesh=mesh,
        in_specs=(
            P("seq", "head"),
            P("seq", "head"),
            P("seq", "head"),
            P("seq", "head"),
            P("head", None),
            P("head", None),
            P("seq", None),
        ),
        out_specs=(P("seq", "head"), P("seq", "head"), P("seq", "head")),
        check_vma=False,
    )
```

```python
import math

import jax
import jax.numpy as jnp
from jax import lax
from jax.experimental import pallas as pl
from jax.experimental.pallas import tpu as pltpu
from jax.sharding import PartitionSpec as P


HDIM = 128
FAR, MID, NEAR = range(3)
SECTIONS = 3
GROUPS = 2
HEADS_PER_STEP = 2
KERNEL_VMEM = 8 * 2**20
STAT_ROWS = 8
BIG = 1e30
SCALE = 1.0 / math.sqrt(HDIM)
LOG2E = math.log2(math.e)
EXP_SCALE = SCALE * LOG2E


def shift(value, steps):
    count = lax.axis_size("seq")
    low, high = max(0, -steps), min(count, count - steps)
    return lax.ppermute(value, "seq", [(src, src + steps) for src in range(low, high)])


def swap(value, axis, bit):
    pairs = [(src, src ^ bit) for src in range(lax.axis_size(axis))]
    return lax.ppermute(value, axis, pairs)


def dot(lhs, rhs, lhs_dim, rhs_dim):
    return lax.dot_general(
        lhs, rhs, (((lhs_dim,), (rhs_dim,)), ((), ())), preferred_element_type=jnp.float32
    )


def on_chip(array):
    return pltpu.with_memory_space_constraint(array, pltpu.VMEM)


def call(kernel, scalars, ins, outs, work, aliases=None):
    smem = pl.BlockSpec(memory_space=pltpu.SMEM)
    vmem = pl.BlockSpec(memory_space=pltpu.VMEM)
    return pl.pallas_call(
        kernel,
        in_specs=[smem] * len(scalars) + [vmem] * len(ins),
        out_specs=[vmem] * len(outs),
        out_shape=[pltpu.VMEM(shape, dtype) for shape, dtype in outs],
        input_output_aliases=aliases or {},
        compiler_params=pltpu.CompilerParams(vmem_limit_bytes=KERNEL_VMEM),
        cost_estimate=pl.CostEstimate(
            flops=2 * work, bytes_accessed=0, transcendentals=work // HDIM
        ),
    )(*scalars, *[on_chip(array) for array in ins])


def each_head(first, count, step):
    def pair(index, carry):
        for offset in range(HEADS_PER_STEP):
            step(first + index * HEADS_PER_STEP + offset)
        return carry

    lax.fori_loop(0, count // HEADS_PER_STEP, pair, None)


def columns(head):
    return pl.ds(pl.multiple_of(head * HDIM, HDIM), HDIM)


def gathered_pieces(out_grad):
    pieces = {0: out_grad}
    bit = lax.axis_size("head") // 2
    while bit:
        for offset in list(pieces):
            pieces[offset | bit] = swap(pieces[offset], "head", bit)
        bit //= 2
    return [pieces[offset] for offset in range(len(pieces))]


def grad_kernel(head_ref, *refs):
    *piece_refs, proj_ref, out_ref = refs
    width = piece_refs[0].shape[1]
    block = 2 * HDIM

    def step(index, carry):
        rows = pl.ds(pl.multiple_of(index * block, block), block)
        total = None
        for offset, piece in enumerate(piece_refs):
            start = pl.multiple_of((head_ref[0] ^ offset) * width, width)
            part = dot(piece[...], proj_ref[rows, pl.ds(start, width)], 1, 1)
            total = part if total is None else total + part
        out_ref[:, rows] = total.astype(out_ref.dtype)
        return carry

    lax.fori_loop(0, out_ref.shape[1] // block, step, None)


def attn_grad_of(out_grad, out_proj):
    pieces = gathered_pieces(out_grad)
    rows = out_grad.shape[0]
    cols, features = out_proj.shape
    head = lax.axis_index("head").astype(jnp.int32).reshape(1)
    (result,) = call(
        grad_kernel,
        [head],
        [*pieces, out_proj],
        [((rows, cols), jnp.bfloat16)],
        rows * cols * features,
    )
    return result


def causal(raw, fill):
    key_at = lax.broadcasted_iota(jnp.int32, raw.shape, 0)
    query_at = lax.broadcasted_iota(jnp.int32, raw.shape, 1)
    return jnp.where(key_at <= query_at, raw, fill)


class Flags:
    def __init__(self, spans, table_ref, active_ref, place_ref):
        self.spans, self.table = spans, table_ref
        self.active, self.place = active_ref, place_ref

    def usable(self, head, section):
        used = self.table[head, section] * self.active[0, section] > 0
        return used & (self.place[0] >= self.spans[section])

    def is_odd(self):
        return (self.place[0] // self.spans[NEAR]) % 2 == 1


def row_stats(head, raws, pgrads, probs, stats):
    top = None
    for raw in raws:
        peak = jnp.max(raw, axis=0, keepdims=True)
        top = peak if top is None else jnp.maximum(top, peak)
    norm, delta = 0.0, 0.0
    for raw, pgrad, out in zip(raws, pgrads, probs):
        prob = jnp.exp2((raw - top) * EXP_SCALE)
        out[head] = prob
        norm = norm + jnp.sum(prob, axis=0, keepdims=True)
        delta = delta + jnp.sum(prob * pgrad, axis=0, keepdims=True)
    for index, row in enumerate((top, norm, delta)):
        stats[head, index : index + 1, :] = row


def stats_own_kernel(spans, t, a, p, q, g, k, v, k_up, v_up, out, pr, pr_up, pg, pg_up):
    flags = Flags(spans, t, a, p)

    def step(head):
        at = columns(head)
        query, grad = q[:, at], g[:, at]
        bias = jnp.where(flags.usable(head, MID), 0.0, -BIG)
        raws = [causal(dot(k[:, at], query, 1, 1), -BIG), dot(k_up[:, at], query, 1, 1) + bias]
        pgrads = [dot(v[:, at], grad, 1, 1), dot(v_up[:, at], grad, 1, 1)]
        pg[head], pg_up[head] = pgrads
        row_stats(head, raws, pgrads, [pr, pr_up], out)

    each_head(0, out.shape[0], step)


def stats_guest_kernel(
    spans, t, a, p, qf, gf, qn, gn, k, v, k_up, v_up, far, near, pr_far, pr_near, pg_far, pg_near
):
    odd = Flags(spans, t, a, p).is_odd()

    def step(head):
        at = columns(head)
        key_up, value_up = k_up[:, at], v_up[:, at]
        key_near = jnp.where(odd, key_up, k[:, at])
        value_near = jnp.where(odd, value_up, v[:, at])
        for query, grad, keys, values, stats, probs, pgrads in (
            (qf, gf, key_up, value_up, far, pr_far, pg_far),
            (qn, gn, key_near, value_near, near, pr_near, pg_near),
        ):
            raw = dot(keys, query[:, at], 1, 1)
            pgrad = dot(values, grad[:, at], 1, 1)
            pgrads[head] = pgrad
            row_stats(head, [raw], [pgrad], [probs], stats)

    each_head(0, far.shape[0], step)


def combine_kernel(spans, t, a, p, own, far, near, own_out, far_out, near_out):
    flags = Flags(spans, t, a, p)
    for head in range(own.shape[0]):
        uses = (True, flags.usable(head, FAR), flags.usable(head, NEAR))
        peaks = []
        for ref, usable in zip((own, far, near), uses):
            peak = ref[head, 0:1, :]
            peaks.append(peak if usable is True else jnp.where(usable, peak, -BIG))
        top = jnp.maximum(jnp.maximum(peaks[0], peaks[1]), peaks[2])
        factors = [jnp.exp2((peak - top) * EXP_SCALE) for peak in peaks]
        norm, delta = 0.0, 0.0
        for ref, factor in zip((own, far, near), factors):
            norm = norm + factor * ref[head, 1:2, :]
            delta = delta + factor * ref[head, 2:3, :]
        inverse = 1.0 / norm
        delta = delta * inverse
        for out, factor in zip((own_out, far_out, near_out), factors):
            out[head, 0:1, :] = factor * inverse
            out[head, 1:2, :] = delta


def pair_terms(head, query, grad, keys, probs, pgrads, norm):
    prob = probs[head] * norm[head, 0:1, :]
    weight = prob.astype(jnp.bfloat16)
    dlogit = (prob * (pgrads[head] - norm[head, 1:2, :])).astype(jnp.bfloat16)
    return dot(keys, dlogit, 0, 0), dot(dlogit, query, 1, 0), dot(weight, grad, 1, 0)


def own_kernel(q, g, k, k_up, norm, pr, pr_up, pg, pg_up, dq, dk, dv, dk_up, dv_up):
    def step(head):
        at = columns(head)
        query, grad = q[:, at], g[:, at]
        dq_own, dk[:, at], dv[:, at] = pair_terms(head, query, grad, k[:, at], pr, pg, norm)
        dq_mid, dk_up[:, at], dv_up[:, at] = pair_terms(
            head, query, grad, k_up[:, at], pr_up, pg_up, norm
        )
        dq[:, at] = ((dq_own + dq_mid) * SCALE).T

    each_head(0, norm.shape[0], step)


def pairs_kernel(
    spans, first, t, a, p, qf, gf, qn, gn, k, k_up, norm_far, norm_near,
    pr_far, pr_near, pg_far, pg_near, dk_own, dv_own, dk_up, dv_up, *refs,
):
    dqf, dqn, back, dk, dv = refs[-5:]
    odd = Flags(spans, t, a, p).is_odd()
    rows = qf.shape[0]

    def step(head):
        at, out = columns(head), columns(head - first)
        key_up = k_up[:, at]
        dq, key_far, value_far = pair_terms(
            head, qf[:, at], gf[:, at], key_up, pr_far, pg_far, norm_far
        )
        dqf[:, at] = (dq * SCALE).T.astype(dqf.dtype)
        key_near = jnp.where(odd, key_up, k[:, at])
        dq, key_term, value_term = pair_terms(
            head, qn[:, at], gn[:, at], key_near, pr_near, pg_near, norm_near
        )
        dqn[:, at] = (dq * SCALE).T.astype(dqn.dtype)
        zero = jnp.zeros_like(key_term)
        key_back = dk_up[:, at] + key_far + jnp.where(odd, key_term, zero)
        value_back = dv_up[:, at] + value_far + jnp.where(odd, value_term, zero)
        back[:rows, out] = (key_back * SCALE).astype(back.dtype)
        back[rows:, out] = value_back.astype(back.dtype)
        dk[:, out] = (dk_own[:, at] + jnp.where(odd, zero, key_term)) * SCALE
        dv[:, out] = dv_own[:, at] + jnp.where(odd, zero, value_term)

    each_head(first, dk.shape[1] // HDIM, step)


def body(queries, key_rows, value_rows, out_grad, out_proj, section_table, block_active):
    seq_count = lax.axis_size("seq")
    place = lax.axis_index("seq")
    spans = [seq_count // 2 ** (index + 1) for index in range(SECTIONS)]
    mid_span, near_span = spans[MID], spans[NEAR]
    assert spans[FAR] == 2 * mid_span and mid_span == 2 * near_span
    assert block_active.shape[0] == 1
    rows, cols = queries.shape
    heads = cols // HDIM
    group = heads // GROUPS
    pair_work = rows * rows * HDIM
    flags = [section_table, block_active, place.astype(jnp.int32).reshape(1)]

    wide_f32 = ((rows, cols), jnp.float32)
    wide_bf16 = ((rows, cols), jnp.bfloat16)
    stat = ((heads, STAT_ROWS, rows), jnp.float32)
    square = ((heads, rows, rows), jnp.float32)

    def with_spans(kernel, *fixed):
        def run(*refs):
            kernel(spans, *fixed, *refs)

        return run

    key_up = shift(key_rows, mid_span)
    value_up = shift(value_rows, mid_span)
    query_far = shift(queries, -mid_span)
    query_near = swap(queries, "seq", near_span)
    grads = attn_grad_of(out_grad, out_proj)
    grad_far = shift(grads, -mid_span)
    grad_near = swap(grads, "seq", near_span)
    local = (key_rows, value_rows, key_up, value_up)
    guests = (query_far, grad_far, query_near, grad_near)

    own_stats, *own_squares = call(
        with_spans(stats_own_kernel),
        flags,
        [queries, grads, *local],
        [stat] + [square] * 4,
        heads * 4 * pair_work,
    )
    far_stats, near_stats, *guest_squares = call(
        with_spans(stats_guest_kernel),
        flags,
        [*guests, *local],
        [stat] * 2 + [square] * 4,
        heads * 4 * pair_work,
    )
    far_stats = shift(far_stats, mid_span)
    near_stats = swap(near_stats, "seq", near_span)
    own_norm, far_norm, near_norm = call(
        with_spans(combine_kernel),
        flags,
        [own_stats, far_stats, near_stats],
        [stat] * 3,
        heads * rows * HDIM,
    )
    far_norm = shift(far_norm, -mid_span)
    near_norm = swap(near_norm, "seq", near_span)
    query_part, *own_terms = call(
        own_kernel,
        [],
        [queries, grads, key_rows, key_up, own_norm, *own_squares],
        [wide_f32] * 5,
        heads * 6 * pair_work,
    )

    partial_queries = []
    key_grad = jnp.zeros((rows, cols), jnp.bfloat16)
    value_grad = jnp.zeros((rows, cols), jnp.bfloat16)
    for index in range(GROUPS):
        first = index * group
        ins = [*guests, key_rows, key_up, far_norm, near_norm, *guest_squares, *own_terms]
        start = len(flags) + len(ins)
        aliases = {start + number: number for number in range(len(partial_queries))}
        half = (rows, group * HDIM)
        *partial_queries, back, key_part, value_part = call(
            with_spans(pairs_kernel, first),
            flags,
            ins + partial_queries,
            [wide_bf16] * 2
            + [((2 * rows, group * HDIM), jnp.bfloat16), (half, jnp.float32), (half, jnp.float32)],
            group * 6 * pair_work,
            aliases,
        )
        back = shift(back, -mid_span).astype(jnp.float32)
        key_part = (key_part + back[:rows]).astype(jnp.bfloat16)
        value_part = (value_part + back[rows:]).astype(jnp.bfloat16)
        at = (0, first * HDIM)
        key_grad = lax.dynamic_update_slice(key_grad, key_part, at)
        value_grad = lax.dynamic_update_slice(value_grad, value_part, at)
    query_far_part = shift(partial_queries[0], mid_span)
    query_near_part = swap(partial_queries[1], "seq", near_span)
    query_grad = query_part + query_far_part.astype(jnp.float32)
    query_grad = query_grad + query_near_part.astype(jnp.float32)
    return query_grad.astype(jnp.bfloat16), key_grad, value_grad


def solution(mesh):
    return jax.shard_map(
        body,
        mesh=mesh,
        in_specs=(
            P("seq", "head"),
            P("seq", "head"),
            P("seq", "head"),
            P("seq", "head"),
            P("head", None),
            P("head", None),
            P("seq", None),
        ),
        out_specs=(P("seq", "head"), P("seq", "head"), P("seq", "head")),
        check_vma=False,
    )
```

```python
import math

import jax
import jax.numpy as jnp
from jax import lax
from jax.experimental import pallas as pl
from jax.experimental.pallas import tpu as pltpu
from jax.sharding import PartitionSpec as P


HDIM = 128
FAR, MID, NEAR = range(3)
SECTIONS = 3
GROUPS = (2, 4, 2)
HEADS_PER_STEP = 2
KERNEL_VMEM = 8 * 2**20
BIG = 1e30
SCALE = 1.0 / math.sqrt(HDIM)
LOG2E = math.log2(math.e)
EXP_SCALE = SCALE * LOG2E


def shift(value, steps):
    count = lax.axis_size("seq")
    low, high = max(0, -steps), min(count, count - steps)
    return lax.ppermute(value, "seq", [(src, src + steps) for src in range(low, high)])


def swap(value, axis, bit):
    pairs = [(src, src ^ bit) for src in range(lax.axis_size(axis))]
    return lax.ppermute(value, axis, pairs)


def dot(lhs, rhs, lhs_dim, rhs_dim):
    return lax.dot_general(
        lhs, rhs, (((lhs_dim,), (rhs_dim,)), ((), ())), preferred_element_type=jnp.float32
    )


def on_chip(array):
    return pltpu.with_memory_space_constraint(array, pltpu.VMEM)


def in_hbm(array):
    return pltpu.with_memory_space_constraint(array, pltpu.HBM)


def call(kernel, scalars, ins, outs, work, aliases=None, grid=None, streams=(), blocks=None):
    smem = pl.BlockSpec(memory_space=pltpu.SMEM)
    vmem = pl.BlockSpec(memory_space=pltpu.VMEM)
    return pl.pallas_call(
        kernel,
        grid=grid or (),
        in_specs=[smem] * len(scalars) + [vmem] * len(ins) + [spec for _, spec in streams],
        out_specs=blocks or [vmem] * len(outs),
        out_shape=[
            (jax.ShapeDtypeStruct if blocks else pltpu.VMEM)(shape, dtype)
            for shape, dtype in outs
        ],
        input_output_aliases=aliases or {},
        compiler_params=pltpu.CompilerParams(vmem_limit_bytes=KERNEL_VMEM),
        cost_estimate=pl.CostEstimate(
            flops=2 * work, bytes_accessed=0, transcendentals=work // HDIM
        ),
    )(*scalars, *[on_chip(array) for array in ins], *[array for array, _ in streams])


def each_head(first, count, step):
    def pair(index, carry):
        for offset in range(HEADS_PER_STEP):
            step(first + index * HEADS_PER_STEP + offset)
        return carry

    lax.fori_loop(0, count // HEADS_PER_STEP, pair, None)


def columns(head):
    return pl.ds(pl.multiple_of(head * HDIM, HDIM), HDIM)


def gathered_pieces(out_grad):
    pieces = {0: out_grad}
    bit = lax.axis_size("head") // 2
    while bit:
        for offset in list(pieces):
            pieces[offset | bit] = swap(pieces[offset], "head", bit)
        bit //= 2
    return [pieces[offset] for offset in range(len(pieces))]


def grad_kernel(head_ref, *refs):
    *piece_refs, own_ref, proj_ref, out_ref = refs
    piece_refs = [own_ref, *piece_refs]
    width = own_ref.shape[1]
    block = proj_ref.shape[0]
    total = None
    for offset, piece in enumerate(piece_refs):
        start = pl.multiple_of((head_ref[0] ^ offset) * width, width)
        part = dot(piece[...], proj_ref[:, pl.ds(start, width)], 1, 1)
        total = part if total is None else total + part
    at = pl.ds(pl.multiple_of(pl.program_id(0) * block, block), block)
    out_ref[:, at] = total.astype(out_ref.dtype)


def attn_grad_of(out_grad, out_proj):
    pieces = gathered_pieces(out_grad)
    rows, width = out_grad.shape
    cols, features = out_proj.shape
    block = 2 * HDIM
    head = lax.axis_index("head").astype(jnp.int32).reshape(1)
    (result,) = call(
        grad_kernel,
        [head],
        pieces[1:],
        [((rows, cols), jnp.bfloat16)],
        rows * cols * features,
        grid=(cols // block,),
        streams=[
            (in_hbm(out_grad), pl.BlockSpec((rows, width), lambda i: (0, 0))),
            (in_hbm(out_proj), pl.BlockSpec((block, features), lambda i: (i, 0))),
        ],
    )
    return result


def stage_kernel(*refs):
    count = len(refs) // 3
    sources, targets, sems = refs[:count], refs[count : 2 * count], refs[2 * count :]
    copies = [pltpu.make_async_copy(*each) for each in zip(sources, targets, sems)]
    for copy in copies:
        copy.start()
    for copy in copies:
        copy.wait()


def staged(*arrays):
    return pl.pallas_call(
        stage_kernel,
        in_specs=[pl.BlockSpec(memory_space=pltpu.HBM)] * len(arrays),
        out_specs=[pl.BlockSpec(memory_space=pltpu.VMEM)] * len(arrays),
        out_shape=[pltpu.VMEM(array.shape, array.dtype) for array in arrays],
        scratch_shapes=[pltpu.SemaphoreType.DMA] * len(arrays),
        compiler_params=pltpu.CompilerParams(vmem_limit_bytes=KERNEL_VMEM),
        cost_estimate=pl.CostEstimate(flops=10**6, bytes_accessed=0, transcendentals=0),
        name="stage",
    )(*[in_hbm(array) for array in arrays])


def causal(raw, fill):
    key_at = lax.broadcasted_iota(jnp.int32, raw.shape, 0)
    query_at = lax.broadcasted_iota(jnp.int32, raw.shape, 1)
    return jnp.where(key_at <= query_at, raw, fill)


class Flags:
    def __init__(self, spans, table_ref, active_ref, place_ref):
        self.spans, self.table = spans, table_ref
        self.active, self.place = active_ref, place_ref

    def usable(self, head, section):
        used = self.table[head, section] * self.active[0, section] > 0
        return used & (self.place[0] >= self.spans[section])

    def is_odd(self):
        return (self.place[0] // self.spans[NEAR]) % 2 == 1


def set_stats(head, raw, pgrad, probs, pgrads, stats):
    top = jnp.max(raw, axis=0, keepdims=True)
    prob = jnp.exp2((raw - top) * EXP_SCALE)
    probs[head] = prob
    pgrads[head] = pgrad
    norm = jnp.sum(prob, axis=0, keepdims=True)
    delta = jnp.sum(prob * pgrad, axis=0, keepdims=True)
    for index, row in enumerate((top, norm, delta)):
        stats[index, pl.ds(head, 1), :] = row


def stats_kernel(diagonal, q, g, k, v, stats, probs, pgrads):
    def step(head):
        at = columns(head)
        raw = dot(k[:, at], q[:, at], 1, 1)
        if diagonal:
            raw = causal(raw, -BIG)
        set_stats(head, raw, dot(v[:, at], g[:, at], 1, 1), probs, pgrads, stats)

    each_head(0, probs.shape[0], step)


def stats_near_kernel(spans, t, a, p, q, g, k, v, k_up, v_up, stats, probs, pgrads):
    odd = Flags(spans, t, a, p).is_odd()

    def step(head):
        at = columns(head)
        keys = jnp.where(odd, k_up[:, at], k[:, at])
        values = jnp.where(odd, v_up[:, at], v[:, at])
        raw = dot(keys, q[:, at], 1, 1)
        set_stats(head, raw, dot(values, g[:, at], 1, 1), probs, pgrads, stats)

    each_head(0, probs.shape[0], step)


def combine_kernel(spans, t, a, p, *refs):
    flags = Flags(spans, t, a, p)
    ins, outs = refs[:4], refs[4:]
    for head in range(ins[0].shape[1]):
        at = slice(head, head + 1)
        peaks = [ins[0][0, at, :]]
        for ref, section in zip(ins[1:], (MID, FAR, NEAR)):
            peaks.append(jnp.where(flags.usable(head, section), ref[0, at, :], -BIG))
        top = jnp.maximum(jnp.maximum(peaks[0], peaks[1]), jnp.maximum(peaks[2], peaks[3]))
        factors = [jnp.exp2((peak - top) * EXP_SCALE) for peak in peaks]
        norm, delta = 0.0, 0.0
        for ref, factor in zip(ins, factors):
            norm = norm + factor * ref[1, at, :]
            delta = delta + factor * ref[2, at, :]
        inverse = 1.0 / norm
        delta = delta * inverse
        for out, factor in zip(outs, factors):
            out[0, at, :] = factor * inverse
            out[1, at, :] = delta


def pair_terms(head, query, grad, keys, probs, pgrads, norm):
    factor, delta = norm[0, pl.ds(head, 1), :], norm[1, pl.ds(head, 1), :]
    prob = probs[head] * factor
    weight = prob.astype(jnp.bfloat16)
    dlogit = (prob * (pgrads[head] - delta)).astype(jnp.bfloat16)
    return dot(keys, dlogit, 0, 0), dot(dlogit, query, 1, 0), dot(weight, grad, 1, 0)


def terms_kernel(q, g, k, norm, probs, pgrads, *refs):
    dq, dk, dv = refs[-3:]

    def step(head):
        at = columns(head)
        query_term, dk[:, at], dv[:, at] = pair_terms(
            head, q[:, at], g[:, at], k[:, at], probs, pgrads, norm
        )
        query_term = query_term.T
        dq[:, at] = query_term + refs[0][:, at] if len(refs) > 3 else query_term

    each_head(0, probs.shape[0], step)


def pairs_kernel(
    spans, first, t, a, p, qf, gf, qn, gn, k, k_up, norm_far, norm_near,
    pr_far, pg_far, pr_near, pg_near, dk_mid, dv_mid, *refs,
):
    dqf, dqn, back, dk, dv = refs[-5:]
    odd = Flags(spans, t, a, p).is_odd()
    rows = qf.shape[0]

    def step(head):
        at, out = columns(head), columns(head - first)
        key_up = k_up[:, at]
        dq, key_far, value_far = pair_terms(
            head, qf[:, at], gf[:, at], key_up, pr_far, pg_far, norm_far
        )
        dqf[:, at] = (dq * SCALE).T.astype(dqf.dtype)
        key_near = jnp.where(odd, key_up, k[:, at])
        dq, key_term, value_term = pair_terms(
            head, qn[:, at], gn[:, at], key_near, pr_near, pg_near, norm_near
        )
        dqn[:, at] = (dq * SCALE).T.astype(dqn.dtype)
        zero = jnp.zeros_like(key_term)
        key_back = dk_mid[:, at] + key_far + jnp.where(odd, key_term, zero)
        value_back = dv_mid[:, at] + value_far + jnp.where(odd, value_term, zero)
        back[:rows, out] = (key_back * SCALE).astype(back.dtype)
        back[rows:, out] = value_back.astype(back.dtype)
        dk[:, out] = jnp.where(odd, zero, key_term)
        dv[:, out] = jnp.where(odd, zero, value_term)

    each_head(first, dk.shape[1] // HDIM, step)


def step_columns(block, first=0):
    return pl.ds(pl.multiple_of(pl.program_id(0) * block + first, block), block)


def finish_kernel(first, dk, dv, near_k, near_v, back, *refs):
    key_out, value_out = refs[-2:]
    rows, block = key_out.shape
    here, at = step_columns(block), step_columns(block, first)
    key_out[...] = (
        (dk[:, at] + near_k[:, here]) * SCALE + back[:rows, here].astype(jnp.float32)
    ).astype(key_out.dtype)
    value_out[...] = (
        dv[:, at] + near_v[:, here] + back[rows:, here].astype(jnp.float32)
    ).astype(value_out.dtype)


def finish_query_kernel(dq, far, near, out):
    at = step_columns(out.shape[1])
    total = dq[:, at] * SCALE + far[:, at].astype(jnp.float32) + near[:, at].astype(jnp.float32)
    out[...] = total.astype(out.dtype)


def body(queries, key_rows, value_rows, out_grad, out_proj, section_table, block_active):
    seq_count = lax.axis_size("seq")
    place = lax.axis_index("seq")
    spans = [seq_count // 2 ** (index + 1) for index in range(SECTIONS)]
    mid_span, near_span = spans[MID], spans[NEAR]
    assert spans[FAR] == 2 * mid_span and mid_span == 2 * near_span
    assert block_active.shape[0] == 1
    rows, cols = queries.shape
    heads = cols // HDIM
    assert heads == sum(GROUPS)
    pair_work = rows * rows * HDIM
    flags = [section_table, block_active, place.astype(jnp.int32).reshape(1)]

    wide_f32 = ((rows, cols), jnp.float32)
    wide_bf16 = ((rows, cols), jnp.bfloat16)
    stat = ((3, heads, rows), jnp.float32)
    norm = ((2, heads, rows), jnp.float32)
    square = ((heads, rows, rows), jnp.float32)

    def bound(kernel, *fixed):
        def run(*refs):
            kernel(*fixed, *refs)

        return run

    key_up = shift(key_rows, mid_span)
    value_up = shift(value_rows, mid_span)
    query_far = shift(queries, -mid_span)
    query_near = swap(queries, "seq", near_span)
    grads = attn_grad_of(out_grad, out_proj)
    grad_far = shift(grads, -mid_span)
    grad_near = swap(grads, "seq", near_span)
    query, key, value = staged(queries, key_rows, value_rows)

    def stats(kernel, scalars, *ins):
        outs = [stat, square, square]
        return call(kernel, scalars, ins, outs, heads * 2 * pair_work)

    self_stats, *self_squares = stats(bound(stats_kernel, True), [], query, grads, key, value)
    mid_stats, *mid_squares = stats(bound(stats_kernel, False), [], query, grads, key_up, value_up)
    near_stats, *near_squares = stats(
        bound(stats_near_kernel, spans), flags,
        query_near, grad_near, key, value, key_up, value_up,
    )
    near_stats = swap(near_stats, "seq", near_span)
    far_stats, *far_squares = stats(
        bound(stats_kernel, False), [], query_far, grad_far, key_up, value_up
    )
    far_stats = shift(far_stats, mid_span)
    self_norm, mid_norm, far_norm, near_norm = call(
        bound(combine_kernel, spans),
        flags,
        [self_stats, mid_stats, far_stats, near_stats],
        [norm] * 4,
        heads * rows * HDIM,
    )
    far_norm = shift(far_norm, -mid_span)
    near_norm = swap(near_norm, "seq", near_span)

    def terms(keys, row_norm, squares, *added):
        ins = [query, grads, keys, row_norm, *squares, *added]
        return call(terms_kernel, [], ins, [wide_f32] * 3, heads * 3 * pair_work)

    mid_query, *mid_terms = terms(key_up, mid_norm, mid_squares)
    guests = [query_far, grad_far, query_near, grad_near, key, key_up, far_norm, near_norm]
    guests += [*far_squares, *near_squares, *mid_terms]
    partial_queries, returned = [], []
    first = 0
    for group in GROUPS:
        width = group * HDIM
        start = len(flags) + len(guests)
        aliases = {start + number: number for number in range(len(partial_queries))}
        *partial_queries, back, near_key, near_value = call(
            bound(pairs_kernel, spans, first),
            flags,
            guests + partial_queries,
            [wide_bf16] * 2 + [((2 * rows, width), jnp.bfloat16)]
            + [((rows, width), jnp.float32)] * 2,
            group * 6 * pair_work,
            aliases,
        )
        returned.append((near_key, near_value, shift(back, -mid_span)))
        first += group
    query_far_part = shift(partial_queries[0], mid_span)
    query_near_part = swap(partial_queries[1], "seq", near_span)
    query_sum, *self_terms = terms(key, self_norm, self_squares, mid_query)

    block = 2 * HDIM
    outputs = []
    first = 0
    for index, group in enumerate(GROUPS):
        start = first * HDIM
        place_of = start // block
        ins = [*self_terms, *returned[index]]
        outputs = call(
            bound(finish_kernel, start),
            [],
            ins,
            [wide_bf16] * 2,
            group * rows * HDIM * HDIM,
            {len(ins) + number: number for number in range(len(outputs))},
            grid=(group * HDIM // block,),
            streams=[(array, pl.BlockSpec(memory_space=pl.ANY)) for array in outputs],
            blocks=[pl.BlockSpec((rows, block), lambda i, j=place_of: (0, i + j))] * 2,
        )
        first += group
    (query_grad,) = call(
        finish_query_kernel,
        [],
        [query_sum, query_far_part, query_near_part],
        [wide_bf16],
        heads * rows * HDIM,
        grid=(cols // block,),
        blocks=[pl.BlockSpec((rows, block), lambda i: (0, i))],
    )
    return query_grad, *outputs


def solution(mesh):
    return jax.shard_map(
        body,
        mesh=mesh,
        in_specs=(
            P("seq", "head"),
            P("seq", "head"),
            P("seq", "head"),
            P("seq", "head"),
            P("head", None),
            P("head", None),
            P("seq", None),
        ),
        out_specs=(P("seq", "head"), P("seq", "head"), P("seq", "head")),
        check_vma=False,
    )
```

```python
import math

import jax
import jax.numpy as jnp
from jax import lax
from jax.experimental import pallas as pl
from jax.experimental.pallas import tpu as pltpu
from jax.sharding import PartitionSpec as P


HDIM = 128
FAR, MID, NEAR = range(3)
SECTIONS = 3
GROUPS = (2, 4, 2)
HEADS_PER_STEP = 2
KERNEL_VMEM = 8 * 2**20
BIG = 1e30
SCALE = 1.0 / math.sqrt(HDIM)
LOG2E = math.log2(math.e)
EXP_SCALE = SCALE * LOG2E


def shift(value, steps):
    count = lax.axis_size("seq")
    low, high = max(0, -steps), min(count, count - steps)
    return lax.ppermute(value, "seq", [(src, src + steps) for src in range(low, high)])


def swap(value, axis, bit):
    pairs = [(src, src ^ bit) for src in range(lax.axis_size(axis))]
    return lax.ppermute(value, axis, pairs)


def dot(lhs, rhs, lhs_dim, rhs_dim):
    return lax.dot_general(
        lhs, rhs, (((lhs_dim,), (rhs_dim,)), ((), ())), preferred_element_type=jnp.float32
    )


def on_chip(array):
    return pltpu.with_memory_space_constraint(array, pltpu.VMEM)


def in_hbm(array):
    return pltpu.with_memory_space_constraint(array, pltpu.HBM)


def call(kernel, scalars, ins, outs, work, aliases=None, grid=None, streams=(), blocks=None, scratch=()):
    smem = pl.BlockSpec(memory_space=pltpu.SMEM)
    vmem = pl.BlockSpec(memory_space=pltpu.VMEM)
    return pl.pallas_call(
        kernel,
        grid=grid or (),
        in_specs=[smem] * len(scalars) + [vmem] * len(ins) + [spec for _, spec in streams],
        out_specs=blocks or [vmem] * len(outs),
        out_shape=[
            (jax.ShapeDtypeStruct if blocks else pltpu.VMEM)(shape, dtype)
            for shape, dtype in outs
        ],
        scratch_shapes=scratch,
        input_output_aliases=aliases or {},
        compiler_params=pltpu.CompilerParams(vmem_limit_bytes=KERNEL_VMEM),
        cost_estimate=pl.CostEstimate(
            flops=2 * work, bytes_accessed=0, transcendentals=work // HDIM
        ),
    )(*scalars, *[on_chip(array) for array in ins], *[array for array, _ in streams])


def each_head(first, count, step):
    def pair(index, carry):
        for offset in range(HEADS_PER_STEP):
            step(first + index * HEADS_PER_STEP + offset)
        return carry

    lax.fori_loop(0, count // HEADS_PER_STEP, pair, None)


def columns(head):
    return pl.ds(pl.multiple_of(head * HDIM, HDIM), HDIM)


def gathered_pieces(out_grad):
    pieces = {0: out_grad}
    bit = lax.axis_size("head") // 2
    while bit:
        for offset in list(pieces):
            pieces[offset | bit] = swap(pieces[offset], "head", bit)
        bit //= 2
    return [pieces[offset] for offset in range(len(pieces))]


def grad_kernel(head_ref, *refs):
    *piece_refs, own_hbm, proj_hbm, out_ref, own_ref, proj, sems, own_sem = refs
    pieces = [own_ref, *piece_refs]
    width = own_ref.shape[1]
    count = sems.shape[0]
    block = proj.shape[0] // count
    own_copy = pltpu.make_async_copy(own_hbm, own_ref, own_sem)
    own_copy.start()
    copies = []
    for index in range(count):
        at = pl.ds(index * block, block)
        copies.append(pltpu.make_async_copy(proj_hbm.at[at], proj.at[at], sems.at[index]))
        copies[-1].start()
    own_copy.wait()
    for index, copy in enumerate(copies):
        copy.wait()
        at = slice(index * block, (index + 1) * block)
        total = None
        for offset, piece in enumerate(pieces):
            start = pl.multiple_of((head_ref[0] ^ offset) * width, width)
            part = dot(piece[...], proj[at, pl.ds(start, width)], 1, 1)
            total = part if total is None else total + part
        out_ref[:, at] = total.astype(out_ref.dtype)


def attn_grad_of(out_grad, out_proj):
    pieces = gathered_pieces(out_grad)
    rows, width = out_grad.shape
    cols, features = out_proj.shape
    count = cols // (2 * HDIM)
    head = lax.axis_index("head").astype(jnp.int32).reshape(1)
    (result,) = call(
        grad_kernel,
        [head],
        pieces[1:],
        [((rows, cols), jnp.bfloat16)],
        rows * cols * features,
        streams=[
            (in_hbm(array), pl.BlockSpec(memory_space=pltpu.HBM)) for array in (out_grad, out_proj)
        ],
        scratch=[
            pltpu.VMEM((rows, width), out_grad.dtype),
            pltpu.VMEM((cols, features), out_proj.dtype),
            pltpu.SemaphoreType.DMA((count,)),
            pltpu.SemaphoreType.DMA,
        ],
    )
    return result


def stage_kernel(*refs):
    count = len(refs) // 3
    sources, targets, sems = refs[:count], refs[count : 2 * count], refs[2 * count :]
    copies = [pltpu.make_async_copy(*each) for each in zip(sources, targets, sems)]
    for copy in copies:
        copy.start()
    for copy in copies:
        copy.wait()


def staged(*arrays):
    return pl.pallas_call(
        stage_kernel,
        in_specs=[pl.BlockSpec(memory_space=pltpu.HBM)] * len(arrays),
        out_specs=[pl.BlockSpec(memory_space=pltpu.VMEM)] * len(arrays),
        out_shape=[pltpu.VMEM(array.shape, array.dtype) for array in arrays],
        scratch_shapes=[pltpu.SemaphoreType.DMA] * len(arrays),
        compiler_params=pltpu.CompilerParams(vmem_limit_bytes=KERNEL_VMEM),
        cost_estimate=pl.CostEstimate(flops=10**6, bytes_accessed=0, transcendentals=0),
        name="stage",
    )(*[in_hbm(array) for array in arrays])


def causal(raw, fill):
    key_at = lax.broadcasted_iota(jnp.int32, raw.shape, 0)
    query_at = lax.broadcasted_iota(jnp.int32, raw.shape, 1)
    return jnp.where(key_at <= query_at, raw, fill)


class Flags:
    def __init__(self, spans, table_ref, active_ref, place_ref):
        self.spans, self.table = spans, table_ref
        self.active, self.place = active_ref, place_ref

    def usable(self, head, section):
        used = self.table[head, section] * self.active[0, section] > 0
        return used & (self.place[0] >= self.spans[section])

    def is_odd(self):
        return (self.place[0] // self.spans[NEAR]) % 2 == 1


def soft_set(head, keys, query, probs, stats, diagonal=False):
    raw = dot(keys, query, 1, 1)
    if diagonal:
        raw = causal(raw, -BIG)
    top = jnp.max(raw, axis=0, keepdims=True)
    prob = jnp.exp2((raw - top) * EXP_SCALE)
    probs[head] = prob
    stats[0, pl.ds(head, 1), :] = top
    stats[1, pl.ds(head, 1), :] = jnp.sum(prob, axis=0, keepdims=True)


def delta_set(head, values, grad, probs, pgrads, stats):
    pgrad = dot(values, grad, 1, 1)
    pgrads[head] = pgrad
    stats[2, pl.ds(head, 1), :] = jnp.sum(probs[head] * pgrad, axis=0, keepdims=True)


def soft_kernel(
    spans, t, a, p, q, g, k, v, qf, qn, k_up, *refs,
):
    odd = Flags(spans, t, a, p).is_odd()
    own, mid, far, near, pr_own, pr_mid, pr_far, pr_near, pg_own = refs

    def step(head):
        at = columns(head)
        key_up, key, query = k_up[:, at], k[:, at], q[:, at]
        soft_set(head, key, query, pr_own, own, True)
        delta_set(head, v[:, at], g[:, at], pr_own, pg_own, own)
        soft_set(head, key_up, query, pr_mid, mid)
        soft_set(head, key_up, qf[:, at], pr_far, far)
        soft_set(head, jnp.where(odd, key_up, key), qn[:, at], pr_near, near)

    each_head(0, pg_own.shape[0], step)


def delta_kernel(g, v_up, probs, soft, stats, pgrads):
    stats[0:2] = soft[0:2]

    def step(head):
        at = columns(head)
        delta_set(head, v_up[:, at], g[:, at], probs, pgrads, stats)

    each_head(0, probs.shape[0], step)


def delta_near_kernel(spans, t, a, p, g, v, v_up, probs, soft, stats, pgrads):
    odd = Flags(spans, t, a, p).is_odd()
    stats[0:2] = soft[0:2]

    def step(head):
        at = columns(head)
        values = jnp.where(odd, v_up[:, at], v[:, at])
        delta_set(head, values, g[:, at], probs, pgrads, stats)

    each_head(0, probs.shape[0], step)


def combine_kernel(spans, t, a, p, *refs):
    flags = Flags(spans, t, a, p)
    ins, outs = refs[:4], refs[4:]
    for head in range(ins[0].shape[1]):
        at = slice(head, head + 1)
        peaks = [ins[0][0, at, :]]
        for ref, section in zip(ins[1:], (MID, FAR, NEAR)):
            peaks.append(jnp.where(flags.usable(head, section), ref[0, at, :], -BIG))
        top = jnp.maximum(jnp.maximum(peaks[0], peaks[1]), jnp.maximum(peaks[2], peaks[3]))
        factors = [jnp.exp2((peak - top) * EXP_SCALE) for peak in peaks]
        norm, delta = 0.0, 0.0
        for ref, factor in zip(ins, factors):
            norm = norm + factor * ref[1, at, :]
            delta = delta + factor * ref[2, at, :]
        inverse = 1.0 / norm
        delta = delta * inverse
        for out, factor in zip(outs, factors):
            out[0, at, :] = factor * inverse
            out[1, at, :] = delta


def pair_terms(head, query, grad, keys, probs, pgrads, norm):
    factor, delta = norm[0, pl.ds(head, 1), :], norm[1, pl.ds(head, 1), :]
    prob = probs[head] * factor
    weight = prob.astype(jnp.bfloat16)
    dlogit = (prob * (pgrads[head] - delta)).astype(jnp.bfloat16)
    return dot(keys, dlogit, 0, 0), dot(dlogit, query, 1, 0), dot(weight, grad, 1, 0)


def terms_kernel(q, g, k, norm, probs, pgrads, *refs):
    dq, dk, dv = refs[-3:]

    def step(head):
        at = columns(head)
        query_term, dk[:, at], dv[:, at] = pair_terms(
            head, q[:, at], g[:, at], k[:, at], probs, pgrads, norm
        )
        query_term = query_term.T
        dq[:, at] = query_term + refs[0][:, at] if len(refs) > 3 else query_term

    each_head(0, probs.shape[0], step)


def pairs_kernel(
    spans, first, t, a, p, qf, gf, qn, gn, k, k_up, _, norm_far, norm_near,
    pr_far, pg_far, pr_near, pg_near, dk_mid, dv_mid, *refs,
):
    dqf, dqn, back, dk, dv = refs[-5:]
    odd = Flags(spans, t, a, p).is_odd()
    rows = qf.shape[0]

    def step(head):
        at, out = columns(head), columns(head - first)
        key_up = k_up[:, at]
        dq, key_far, value_far = pair_terms(
            head, qf[:, at], gf[:, at], key_up, pr_far, pg_far, norm_far
        )
        dqf[:, at] = (dq * SCALE).T.astype(dqf.dtype)
        key_near = jnp.where(odd, key_up, k[:, at])
        dq, key_term, value_term = pair_terms(
            head, qn[:, at], gn[:, at], key_near, pr_near, pg_near, norm_near
        )
        dqn[:, at] = (dq * SCALE).T.astype(dqn.dtype)
        zero = jnp.zeros_like(key_term)
        key_back = dk_mid[:, at] + key_far + jnp.where(odd, key_term, zero)
        value_back = dv_mid[:, at] + value_far + jnp.where(odd, value_term, zero)
        back[:rows, out] = (key_back * SCALE).astype(back.dtype)
        back[rows:, out] = value_back.astype(back.dtype)
        dk[:, out] = jnp.where(odd, zero, key_term)
        dv[:, out] = jnp.where(odd, zero, value_term)

    each_head(first, dk.shape[1] // HDIM, step)


def step_columns(block, first=0):
    return pl.ds(pl.multiple_of(pl.program_id(0) * block + first, block), block)


def finish_kernel(first, dk, dv, near_k, near_v, back, *refs):
    key_out, value_out = refs[-2:]
    rows, block = key_out.shape
    here, at = step_columns(block), step_columns(block, first)
    key_out[...] = (
        (dk[:, at] + near_k[:, here]) * SCALE + back[:rows, here].astype(jnp.float32)
    ).astype(key_out.dtype)
    value_out[...] = (
        dv[:, at] + near_v[:, here] + back[rows:, here].astype(jnp.float32)
    ).astype(value_out.dtype)


def finish_query_kernel(dq, far, near, out):
    at = step_columns(out.shape[1])
    total = dq[:, at] * SCALE + far[:, at].astype(jnp.float32) + near[:, at].astype(jnp.float32)
    out[...] = total.astype(out.dtype)


def body(queries, key_rows, value_rows, out_grad, out_proj, section_table, block_active):
    seq_count = lax.axis_size("seq")
    place = lax.axis_index("seq")
    spans = [seq_count // 2 ** (index + 1) for index in range(SECTIONS)]
    mid_span, near_span = spans[MID], spans[NEAR]
    assert spans[FAR] == 2 * mid_span and mid_span == 2 * near_span
    assert block_active.shape[0] == 1
    rows, cols = queries.shape
    heads = cols // HDIM
    assert heads == sum(GROUPS)
    pair_work = rows * rows * HDIM
    flags = [section_table, block_active, place.astype(jnp.int32).reshape(1)]

    wide_f32 = ((rows, cols), jnp.float32)
    wide_bf16 = ((rows, cols), jnp.bfloat16)
    stat = ((3, heads, rows), jnp.float32)
    norm = ((2, heads, rows), jnp.float32)
    square = ((heads, rows, rows), jnp.float32)

    def bound(kernel, *fixed):
        def run(*refs):
            kernel(*fixed, *refs)

        return run

    key_up = shift(key_rows, mid_span)
    value_up = shift(value_rows, mid_span)
    query_far = shift(queries, -mid_span)
    query_near = swap(queries, "seq", near_span)
    grads = attn_grad_of(out_grad, out_proj)
    grad_far = shift(grads, -mid_span)
    grad_near = swap(grads, "seq", near_span)
    query, key, value = staged(queries, key_rows, value_rows)

    self_stats, mid_soft, far_soft, near_soft, *probs, self_pgrad = call(
        bound(soft_kernel, spans),
        flags,
        [query, grads, key, value, query_far, query_near, key_up],
        [stat] * 4 + [square] * 5,
        heads * 5 * pair_work,
    )
    self_prob, mid_prob, far_prob, near_prob = probs

    def deltas(kernel, scalars, *ins):
        return call(kernel, scalars, ins, [stat, square], heads * pair_work)

    near_stats, near_pgrad = deltas(
        bound(delta_near_kernel, spans), flags,
        grad_near, value, value_up, near_prob, near_soft,
    )
    near_stats = swap(near_stats, "seq", near_span)
    far_stats, far_pgrad = deltas(delta_kernel, [], grad_far, value_up, far_prob, far_soft)
    far_stats = shift(far_stats, mid_span)
    mid_stats, mid_pgrad = deltas(delta_kernel, [], grads, value_up, mid_prob, mid_soft)
    self_squares, mid_squares = (self_prob, self_pgrad), (mid_prob, mid_pgrad)
    far_squares, near_squares = (far_prob, far_pgrad), (near_prob, near_pgrad)
    self_norm, mid_norm, far_norm, near_norm = call(
        bound(combine_kernel, spans),
        flags,
        [self_stats, mid_stats, far_stats, near_stats],
        [norm] * 4,
        heads * rows * HDIM,
    )
    far_norm = shift(far_norm, -mid_span)
    near_norm = swap(near_norm, "seq", near_span)

    def terms(keys, row_norm, squares, *added):
        ins = [query, grads, keys, row_norm, *squares, *added]
        return call(terms_kernel, [], ins, [wide_f32] * 3, heads * 3 * pair_work)

    mid_query, *mid_terms = terms(key_up, mid_norm, mid_squares)
    guests = [query_far, grad_far, query_near, grad_near, key, key_up, value_up, far_norm, near_norm]
    guests += [*far_squares, *near_squares, *mid_terms]
    partial_queries, returned = [], []
    first = 0
    for group in GROUPS:
        width = group * HDIM
        start = len(flags) + len(guests)
        aliases = {start + number: number for number in range(len(partial_queries))}
        *partial_queries, back, near_key, near_value = call(
            bound(pairs_kernel, spans, first),
            flags,
            guests + partial_queries,
            [wide_bf16] * 2 + [((2 * rows, width), jnp.bfloat16)]
            + [((rows, width), jnp.float32)] * 2,
            group * 6 * pair_work,
            aliases,
        )
        returned.append((near_key, near_value, shift(back, -mid_span)))
        first += group
    query_far_part = shift(partial_queries[0], mid_span)
    query_near_part = swap(partial_queries[1], "seq", near_span)
    query_sum, *self_terms = terms(key, self_norm, self_squares, mid_query)

    block = 2 * HDIM
    outputs = []
    first = 0
    for index, group in enumerate(GROUPS):
        start = first * HDIM
        place_of = start // block
        ins = [*self_terms, *returned[index]]
        outputs = call(
            bound(finish_kernel, start),
            [],
            ins,
            [wide_bf16] * 2,
            group * rows * HDIM * HDIM,
            {len(ins) + number: number for number in range(len(outputs))},
            grid=(group * HDIM // block,),
            streams=[(array, pl.BlockSpec(memory_space=pl.ANY)) for array in outputs],
            blocks=[pl.BlockSpec((rows, block), lambda i, j=place_of: (0, i + j))] * 2,
        )
        first += group
    (query_grad,) = call(
        finish_query_kernel,
        [],
        [query_sum, query_far_part, query_near_part],
        [wide_bf16],
        heads * rows * HDIM,
        grid=(cols // block,),
        blocks=[pl.BlockSpec((rows, block), lambda i: (0, i))],
    )
    return query_grad, *outputs


def solution(mesh):
    return jax.shard_map(
        body,
        mesh=mesh,
        in_specs=(
            P("seq", "head"),
            P("seq", "head"),
            P("seq", "head"),
            P("seq", "head"),
            P("head", None),
            P("head", None),
            P("seq", None),
        ),
        out_specs=(P("seq", "head"), P("seq", "head"), P("seq", "head")),
        check_vma=False,
    )
```

```python
import math

import jax
import jax.numpy as jnp
from jax import lax
from jax.experimental import pallas as pl
from jax.experimental.pallas import tpu as pltpu
from jax.sharding import PartitionSpec as P


HDIM = 128
FAR, MID, NEAR = range(3)
SECTIONS = 3
GROUPS = (2, 4, 2)
HEADS_PER_STEP = 2
KERNEL_VMEM = 8 * 2**20
BIG = 1e30
SCALE = 1.0 / math.sqrt(HDIM)
LOG2E = math.log2(math.e)
EXP_SCALE = SCALE * LOG2E


def shift(value, steps):
    count = lax.axis_size("seq")
    low, high = max(0, -steps), min(count, count - steps)
    return lax.ppermute(value, "seq", [(src, src + steps) for src in range(low, high)])


def swap(value, axis, bit):
    pairs = [(src, src ^ bit) for src in range(lax.axis_size(axis))]
    return lax.ppermute(value, axis, pairs)


def dot(lhs, rhs, lhs_dim, rhs_dim):
    return lax.dot_general(
        lhs, rhs, (((lhs_dim,), (rhs_dim,)), ((), ())), preferred_element_type=jnp.float32
    )


def on_chip(array):
    return pltpu.with_memory_space_constraint(array, pltpu.VMEM)


def in_hbm(array):
    return pltpu.with_memory_space_constraint(array, pltpu.HBM)


def call(kernel, scalars, ins, outs, work, aliases=None, grid=None, streams=(), blocks=None, scratch=()):
    smem = pl.BlockSpec(memory_space=pltpu.SMEM)
    vmem = pl.BlockSpec(memory_space=pltpu.VMEM)
    return pl.pallas_call(
        kernel,
        grid=grid or (),
        in_specs=[smem] * len(scalars) + [vmem] * len(ins) + [spec for _, spec in streams],
        out_specs=blocks or [vmem] * len(outs),
        out_shape=[
            (jax.ShapeDtypeStruct if blocks else pltpu.VMEM)(shape, dtype)
            for shape, dtype in outs
        ],
        scratch_shapes=scratch,
        input_output_aliases=aliases or {},
        compiler_params=pltpu.CompilerParams(vmem_limit_bytes=KERNEL_VMEM),
        cost_estimate=pl.CostEstimate(
            flops=2 * work, bytes_accessed=0, transcendentals=work // HDIM
        ),
    )(*scalars, *[on_chip(array) for array in ins], *[array for array, _ in streams])


def each_head(first, count, step):
    def pair(index, carry):
        for offset in range(HEADS_PER_STEP):
            step(first + index * HEADS_PER_STEP + offset)
        return carry

    lax.fori_loop(0, count // HEADS_PER_STEP, pair, None)


def columns(head):
    return pl.ds(pl.multiple_of(head * HDIM, HDIM), HDIM)


def gathered_pieces(out_grad):
    pieces = {0: out_grad}
    bit = lax.axis_size("head") // 2
    while bit:
        for offset in list(pieces):
            pieces[offset | bit] = swap(pieces[offset], "head", bit)
        bit //= 2
    return [pieces[offset] for offset in range(len(pieces))]


def grad_kernel(*refs):
    head = lax.axis_index("head")
    *piece_refs, own_hbm, proj_hbm, out_ref, own_ref, proj, sems, own_sem = refs
    pieces = [own_ref, *piece_refs]
    width = own_ref.shape[1]
    count = sems.shape[0]
    block = proj.shape[0] // count
    own_copy = pltpu.make_async_copy(own_hbm, own_ref, own_sem)
    own_copy.start()
    copies = []
    for index in range(count):
        at = pl.ds(index * block, block)
        copies.append(pltpu.make_async_copy(proj_hbm.at[at], proj.at[at], sems.at[index]))
        copies[-1].start()
    own_copy.wait()
    for index, copy in enumerate(copies):
        copy.wait()
        at = slice(index * block, (index + 1) * block)
        total = None
        for offset, piece in enumerate(pieces):
            start = pl.multiple_of((head ^ offset) * width, width)
            part = dot(piece[...], proj[at, pl.ds(start, width)], 1, 1)
            total = part if total is None else total + part
        out_ref[:, at] = total.astype(out_ref.dtype)


def attn_grad_of(out_grad, out_proj):
    pieces = gathered_pieces(out_grad)
    rows, width = out_grad.shape
    cols, features = out_proj.shape
    count = cols // (2 * HDIM)
    (result,) = call(
        grad_kernel,
        [],
        pieces[1:],
        [((rows, cols), jnp.bfloat16)],
        rows * cols * features,
        streams=[
            (in_hbm(array), pl.BlockSpec(memory_space=pltpu.HBM)) for array in (out_grad, out_proj)
        ],
        scratch=[
            pltpu.VMEM((rows, width), out_grad.dtype),
            pltpu.VMEM((cols, features), out_proj.dtype),
            pltpu.SemaphoreType.DMA((count,)),
            pltpu.SemaphoreType.DMA,
        ],
    )
    return result


def stage_kernel(*refs):
    count = len(refs) // 3
    sources, targets, sems = refs[:count], refs[count : 2 * count], refs[2 * count :]
    copies = [pltpu.make_async_copy(*each) for each in zip(sources, targets, sems)]
    for copy in copies:
        copy.start()
    for copy in copies:
        copy.wait()


def staged(*arrays):
    return pl.pallas_call(
        stage_kernel,
        in_specs=[pl.BlockSpec(memory_space=pltpu.HBM)] * len(arrays),
        out_specs=[pl.BlockSpec(memory_space=pltpu.VMEM)] * len(arrays),
        out_shape=[pltpu.VMEM(array.shape, array.dtype) for array in arrays],
        scratch_shapes=[pltpu.SemaphoreType.DMA] * len(arrays),
        compiler_params=pltpu.CompilerParams(vmem_limit_bytes=KERNEL_VMEM),
        cost_estimate=pl.CostEstimate(flops=10**6, bytes_accessed=0, transcendentals=0),
        name="stage",
    )(*[in_hbm(array) for array in arrays])


def causal(raw, fill):
    key_at = lax.broadcasted_iota(jnp.int32, raw.shape, 0)
    query_at = lax.broadcasted_iota(jnp.int32, raw.shape, 1)
    return jnp.where(key_at <= query_at, raw, fill)


class Flags:
    def __init__(self, spans, table_ref, active_ref):
        self.spans, self.table, self.active = spans, table_ref, active_ref
        self.place = lax.axis_index("seq")

    def usable(self, head, section):
        used = self.table[section, head] * self.active[0, section] > 0
        return used & (self.place >= self.spans[section])


def by_parity(near_span, run):
    odd = (lax.axis_index("seq") // near_span) % 2 == 1
    pl.when(odd)(lambda: run(True))
    pl.when(jnp.logical_not(odd))(lambda: run(False))


def soft_set(head, keys, query, probs, stats, diagonal=False):
    raw = dot(keys, query, 1, 1)
    if diagonal:
        raw = causal(raw, -BIG)
    top = jnp.max(raw, axis=0, keepdims=True)
    prob = jnp.exp2((raw - top) * EXP_SCALE)
    probs[head] = prob
    stats[0, pl.ds(head, 1), :] = top
    stats[1, pl.ds(head, 1), :] = jnp.sum(prob, axis=0, keepdims=True)


def delta_set(head, values, grad, probs, pgrads, stats):
    pgrad = dot(values, grad, 1, 1)
    pgrads[head] = pgrad
    stats[2, pl.ds(head, 1), :] = jnp.sum(probs[head] * pgrad, axis=0, keepdims=True)


def soft_kernel(near_span, q, g, k, v, qf, qn, k_up, *refs):
    own, mid, far, near, pr_own, pr_mid, pr_far, pr_near, pg_own = refs

    def run(odd):
        def step(head):
            at = columns(head)
            key_up, key, query = k_up[:, at], k[:, at], q[:, at]
            soft_set(head, key, query, pr_own, own, True)
            delta_set(head, v[:, at], g[:, at], pr_own, pg_own, own)
            soft_set(head, key_up, query, pr_mid, mid)
            soft_set(head, key_up, qf[:, at], pr_far, far)
            soft_set(head, key_up if odd else key, qn[:, at], pr_near, near)

        each_head(0, pg_own.shape[0], step)

    by_parity(near_span, run)


def delta_kernel(g, v_up, probs, soft, stats, pgrads):
    stats[0:2] = soft[0:2]

    def step(head):
        at = columns(head)
        delta_set(head, v_up[:, at], g[:, at], probs, pgrads, stats)

    each_head(0, probs.shape[0], step)


def delta_near_kernel(near_span, g, v, v_up, *refs):
    by_parity(near_span, lambda odd: delta_kernel(g, v_up if odd else v, *refs))


def combine_kernel(spans, t, a, *refs):
    flags = Flags(spans, t, a)
    ins, outs = refs[:4], refs[4:]
    for head in range(ins[0].shape[1]):
        at = slice(head, head + 1)
        peaks = [ins[0][0, at, :]]
        for ref, section in zip(ins[1:], (MID, FAR, NEAR)):
            peaks.append(jnp.where(flags.usable(head, section), ref[0, at, :], -BIG))
        top = jnp.maximum(jnp.maximum(peaks[0], peaks[1]), jnp.maximum(peaks[2], peaks[3]))
        factors = [jnp.exp2((peak - top) * EXP_SCALE) for peak in peaks]
        norm, delta = 0.0, 0.0
        for ref, factor in zip(ins, factors):
            norm = norm + factor * ref[1, at, :]
            delta = delta + factor * ref[2, at, :]
        inverse = 1.0 / norm
        delta = delta * inverse
        for out, factor in zip(outs, factors):
            out[0, at, :] = factor * inverse
            out[1, at, :] = delta


def pair_terms(head, query, grad, keys, probs, pgrads, norm):
    factor, delta = norm[0, pl.ds(head, 1), :], norm[1, pl.ds(head, 1), :]
    prob = probs[head] * factor
    weight = prob.astype(jnp.bfloat16)
    dlogit = (prob * (pgrads[head] - delta)).astype(jnp.bfloat16)
    return dot(keys, dlogit, 0, 0), dot(dlogit, query, 1, 0), dot(weight, grad, 1, 0)


def terms_kernel(q, g, k, norm, probs, pgrads, *refs):
    dq, dk, dv = refs[-3:]

    def step(head):
        at = columns(head)
        query_term, dk[:, at], dv[:, at] = pair_terms(
            head, q[:, at], g[:, at], k[:, at], probs, pgrads, norm
        )
        query_term = query_term.T
        dq[:, at] = query_term + refs[0][:, at] if len(refs) > 3 else query_term

    each_head(0, probs.shape[0], step)


def pairs_kernel(
    near_span, first, qf, gf, qn, gn, k, k_up, norm_far, norm_near,
    pr_far, pg_far, pr_near, pg_near, dk_mid, dv_mid, *refs,
):
    dqf, dqn, back, dk, dv = refs[-5:]
    rows = qf.shape[0]

    def run(odd):
        def step(head):
            at, out = columns(head), columns(head - first)
            key_up = k_up[:, at]
            dq, key_back, value_back = pair_terms(
                head, qf[:, at], gf[:, at], key_up, pr_far, pg_far, norm_far
            )
            dqf[:, at] = (dq * SCALE).T.astype(dqf.dtype)
            key_near = key_up if odd else k[:, at]
            dq, key_term, value_term = pair_terms(
                head, qn[:, at], gn[:, at], key_near, pr_near, pg_near, norm_near
            )
            dqn[:, at] = (dq * SCALE).T.astype(dqn.dtype)
            key_back, value_back = dk_mid[:, at] + key_back, dv_mid[:, at] + value_back
            if odd:
                key_back, value_back = key_back + key_term, value_back + value_term
                key_term, value_term = jnp.zeros_like(key_term), jnp.zeros_like(value_term)
            back[:rows, out] = (key_back * SCALE).astype(back.dtype)
            back[rows:, out] = value_back.astype(back.dtype)
            dk[:, out] = key_term
            dv[:, out] = value_term

        each_head(first, dk.shape[1] // HDIM, step)

    by_parity(near_span, run)


def step_columns(block, first=0):
    return pl.ds(pl.multiple_of(pl.program_id(0) * block + first, block), block)


def finish_kernel(first, dk, dv, near_k, near_v, back, *refs):
    key_out, value_out = refs[-2:]
    rows, block = key_out.shape
    here, at = step_columns(block), step_columns(block, first)
    key_out[...] = (
        (dk[:, at] + near_k[:, here]) * SCALE + back[:rows, here].astype(jnp.float32)
    ).astype(key_out.dtype)
    value_out[...] = (
        dv[:, at] + near_v[:, here] + back[rows:, here].astype(jnp.float32)
    ).astype(value_out.dtype)


def finish_query_kernel(dq, far, near, out):
    at = step_columns(out.shape[1])
    total = dq[:, at] * SCALE + far[:, at].astype(jnp.float32) + near[:, at].astype(jnp.float32)
    out[...] = total.astype(out.dtype)


def body(queries, key_rows, value_rows, out_grad, out_proj, section_table, block_active):
    seq_count = lax.axis_size("seq")
    spans = [seq_count // 2 ** (index + 1) for index in range(SECTIONS)]
    mid_span, near_span = spans[MID], spans[NEAR]
    assert spans[FAR] == 2 * mid_span and mid_span == 2 * near_span
    assert block_active.shape[0] == 1
    rows, cols = queries.shape
    heads = cols // HDIM
    assert heads == sum(GROUPS)
    pair_work = rows * rows * HDIM
    flags = [section_table.T, block_active]

    wide_f32 = ((rows, cols), jnp.float32)
    wide_bf16 = ((rows, cols), jnp.bfloat16)
    stat = ((3, heads, rows), jnp.float32)
    norm = ((2, heads, rows), jnp.float32)
    square = ((heads, rows, rows), jnp.float32)

    def bound(kernel, *fixed):
        def run(*refs):
            kernel(*fixed, *refs)

        return run

    key_up = shift(key_rows, mid_span)
    value_up = shift(value_rows, mid_span)
    query_far = shift(queries, -mid_span)
    query_near = swap(queries, "seq", near_span)
    grads = attn_grad_of(out_grad, out_proj)
    grad_far = shift(grads, -mid_span)
    grad_near = swap(grads, "seq", near_span)
    query, key, value = staged(queries, key_rows, value_rows)

    self_stats, mid_soft, far_soft, near_soft, *probs, self_pgrad = call(
        bound(soft_kernel, near_span),
        [],
        [query, grads, key, value, query_far, query_near, key_up],
        [stat] * 4 + [square] * 5,
        heads * 5 * pair_work,
    )
    self_prob, mid_prob, far_prob, near_prob = probs

    def deltas(kernel, scalars, *ins):
        return call(kernel, scalars, ins, [stat, square], heads * pair_work)

    near_stats, near_pgrad = deltas(
        bound(delta_near_kernel, near_span), [],
        grad_near, value, value_up, near_prob, near_soft,
    )
    near_stats = swap(near_stats, "seq", near_span)
    far_stats, far_pgrad = deltas(delta_kernel, [], grad_far, value_up, far_prob, far_soft)
    far_stats = shift(far_stats, mid_span)
    mid_stats, mid_pgrad = deltas(delta_kernel, [], grads, value_up, mid_prob, mid_soft)
    self_squares, mid_squares = (self_prob, self_pgrad), (mid_prob, mid_pgrad)
    far_squares, near_squares = (far_prob, far_pgrad), (near_prob, near_pgrad)
    self_norm, mid_norm, far_norm, near_norm = call(
        bound(combine_kernel, spans),
        flags,
        [self_stats, mid_stats, far_stats, near_stats],
        [norm] * 4,
        heads * rows * HDIM,
    )
    far_norm = shift(far_norm, -mid_span)
    near_norm = swap(near_norm, "seq", near_span)

    def terms(keys, row_norm, squares, *added):
        ins = [query, grads, keys, row_norm, *squares, *added]
        return call(terms_kernel, [], ins, [wide_f32] * 3, heads * 3 * pair_work)

    mid_query, *mid_terms = terms(key_up, mid_norm, mid_squares)
    guests = [query_far, grad_far, query_near, grad_near, key, key_up, far_norm, near_norm]
    guests += [*far_squares, *near_squares, *mid_terms]
    partial_queries, returned = [], []
    first = 0
    for group in GROUPS:
        width = group * HDIM
        start = len(guests)
        aliases = {start + number: number for number in range(len(partial_queries))}
        *partial_queries, back, near_key, near_value = call(
            bound(pairs_kernel, near_span, first),
            [],
            guests + partial_queries,
            [wide_bf16] * 2 + [((2 * rows, width), jnp.bfloat16)]
            + [((rows, width), jnp.float32)] * 2,
            group * 6 * pair_work,
            aliases,
        )
        returned.append((near_key, near_value, shift(back, -mid_span)))
        first += group
    query_far_part = shift(partial_queries[0], mid_span)
    query_near_part = swap(partial_queries[1], "seq", near_span)
    query_sum, *self_terms = terms(key, self_norm, self_squares, mid_query)

    block = 2 * HDIM
    outputs = []
    first = 0
    for index, group in enumerate(GROUPS):
        start = first * HDIM
        place_of = start // block
        ins = [*self_terms, *returned[index]]
        outputs = call(
            bound(finish_kernel, start),
            [],
            ins,
            [wide_bf16] * 2,
            group * rows * HDIM * HDIM,
            {len(ins) + number: number for number in range(len(outputs))},
            grid=(group * HDIM // block,),
            streams=[(array, pl.BlockSpec(memory_space=pl.ANY)) for array in outputs],
            blocks=[pl.BlockSpec((rows, block), lambda i, j=place_of: (0, i + j))] * 2,
        )
        first += group
    (query_grad,) = call(
        finish_query_kernel,
        [],
        [query_sum, query_far_part, query_near_part],
        [wide_bf16],
        heads * rows * HDIM,
        grid=(cols // block,),
        blocks=[pl.BlockSpec((rows, block), lambda i: (0, i))],
    )
    return query_grad, *outputs


def solution(mesh):
    return jax.shard_map(
        body,
        mesh=mesh,
        in_specs=(
            P("seq", "head"),
            P("seq", "head"),
            P("seq", "head"),
            P("seq", "head"),
            P("head", None),
            P("head", None),
            P("seq", None),
        ),
        out_specs=(P("seq", "head"), P("seq", "head"), P("seq", "head")),
        check_vma=False,
    )
```

```python
import math

import jax
import jax.numpy as jnp
from jax import lax
from jax.experimental import pallas as pl
from jax.experimental.pallas import tpu as pltpu
from jax.sharding import PartitionSpec as P


HDIM = 128
FAR, MID, NEAR = range(3)
SECTIONS = 3
GROUPS = (2, 4, 2)
HEADS_PER_STEP = 2
KERNEL_VMEM = 8 * 2**20
BIG = 1e30
SCALE = 1.0 / math.sqrt(HDIM)
LOG2E = math.log2(math.e)
EXP_SCALE = SCALE * LOG2E


def shift(value, steps):
    count = lax.axis_size("seq")
    low, high = max(0, -steps), min(count, count - steps)
    return lax.ppermute(value, "seq", [(src, src + steps) for src in range(low, high)])


def swap(value, axis, bit):
    pairs = [(src, src ^ bit) for src in range(lax.axis_size(axis))]
    return lax.ppermute(value, axis, pairs)


def dot(lhs, rhs, lhs_dim, rhs_dim):
    return lax.dot_general(
        lhs, rhs, (((lhs_dim,), (rhs_dim,)), ((), ())), preferred_element_type=jnp.float32
    )


def on_chip(array):
    return pltpu.with_memory_space_constraint(array, pltpu.VMEM)


def in_hbm(array):
    return pltpu.with_memory_space_constraint(array, pltpu.HBM)


def call(kernel, scalars, ins, outs, work, aliases=None, grid=None, streams=(), blocks=None, scratch=()):
    smem = pl.BlockSpec(memory_space=pltpu.SMEM)
    vmem = pl.BlockSpec(memory_space=pltpu.VMEM)
    return pl.pallas_call(
        kernel,
        grid=grid or (),
        in_specs=[smem] * len(scalars) + [vmem] * len(ins) + [spec for _, spec in streams],
        out_specs=blocks or [vmem] * len(outs),
        out_shape=[
            (jax.ShapeDtypeStruct if blocks else pltpu.VMEM)(shape, dtype)
            for shape, dtype in outs
        ],
        scratch_shapes=scratch,
        input_output_aliases=aliases or {},
        compiler_params=pltpu.CompilerParams(vmem_limit_bytes=KERNEL_VMEM),
        cost_estimate=pl.CostEstimate(
            flops=2 * work, bytes_accessed=0, transcendentals=work // HDIM
        ),
    )(*scalars, *[on_chip(array) for array in ins], *[array for array, _ in streams])


def each_head(first, count, step):
    def pair(index, carry):
        for offset in range(HEADS_PER_STEP):
            step(first + index * HEADS_PER_STEP + offset)
        return carry

    lax.fori_loop(0, count // HEADS_PER_STEP, pair, None)


def columns(head):
    return pl.ds(pl.multiple_of(head * HDIM, HDIM), HDIM)


def gathered_pieces(out_grad):
    pieces = {0: out_grad}
    bit = lax.axis_size("head") // 2
    while bit:
        for offset in list(pieces):
            pieces[offset | bit] = swap(pieces[offset], "head", bit)
        bit //= 2
    return [pieces[offset] for offset in range(len(pieces))]


def grad_kernel(*refs):
    head = lax.axis_index("head")
    *piece_refs, own_hbm, proj_hbm, out_ref, own_ref, proj, sems, own_sem = refs
    pieces = [own_ref, *piece_refs]
    width = own_ref.shape[1]
    count = sems.shape[0]
    block = proj.shape[0] // count
    own_copy = pltpu.make_async_copy(own_hbm, own_ref, own_sem)
    own_copy.start()
    copies = []
    for index in range(count):
        at = pl.ds(index * block, block)
        copies.append(pltpu.make_async_copy(proj_hbm.at[at], proj.at[at], sems.at[index]))
    for copy in copies[:2]:
        copy.start()
    own_copy.wait()
    for index, copy in enumerate(copies):
        copy.wait()
        if index + 2 < count:
            copies[index + 2].start()
        at = slice(index * block, (index + 1) * block)
        total = None
        for offset, piece in enumerate(pieces):
            start = pl.multiple_of((head ^ offset) * width, width)
            part = dot(piece[...], proj[at, pl.ds(start, width)], 1, 1)
            total = part if total is None else total + part
        out_ref[:, at] = total.astype(out_ref.dtype)


def attn_grad_of(out_grad, out_proj):
    pieces = gathered_pieces(out_grad)
    rows, width = out_grad.shape
    cols, features = out_proj.shape
    count = cols // (2 * HDIM)
    (result,) = call(
        grad_kernel,
        [],
        pieces[1:],
        [((rows, cols), jnp.bfloat16)],
        rows * cols * features,
        streams=[
            (in_hbm(array), pl.BlockSpec(memory_space=pltpu.HBM)) for array in (out_grad, out_proj)
        ],
        scratch=[
            pltpu.VMEM((rows, width), out_grad.dtype),
            pltpu.VMEM((cols, features), out_proj.dtype),
            pltpu.SemaphoreType.DMA((count,)),
            pltpu.SemaphoreType.DMA,
        ],
    )
    return result


def stage_kernel(*refs):
    count = len(refs) // 3
    sources, targets, sems = refs[:count], refs[count : 2 * count], refs[2 * count :]
    copies = [pltpu.make_async_copy(*each) for each in zip(sources, targets, sems)]
    for copy in copies:
        copy.start()
    for copy in copies:
        copy.wait()


def staged(*arrays):
    return pl.pallas_call(
        stage_kernel,
        in_specs=[pl.BlockSpec(memory_space=pltpu.HBM)] * len(arrays),
        out_specs=[pl.BlockSpec(memory_space=pltpu.VMEM)] * len(arrays),
        out_shape=[pltpu.VMEM(array.shape, array.dtype) for array in arrays],
        scratch_shapes=[pltpu.SemaphoreType.DMA] * len(arrays),
        compiler_params=pltpu.CompilerParams(vmem_limit_bytes=KERNEL_VMEM),
        cost_estimate=pl.CostEstimate(flops=10**6, bytes_accessed=0, transcendentals=0),
        name="stage",
    )(*[in_hbm(array) for array in arrays])


def causal(raw, fill):
    key_at = lax.broadcasted_iota(jnp.int32, raw.shape, 0)
    query_at = lax.broadcasted_iota(jnp.int32, raw.shape, 1)
    return jnp.where(key_at <= query_at, raw, fill)


class Flags:
    def __init__(self, spans, table_ref, active_ref):
        self.spans, self.table, self.active = spans, table_ref, active_ref
        self.place = lax.axis_index("seq")

    def usable(self, head, section):
        used = self.table[section, head] * self.active[0, section] > 0
        return used & (self.place >= self.spans[section])


def by_parity(near_span, run):
    odd = (lax.axis_index("seq") // near_span) % 2 == 1
    pl.when(odd)(lambda: run(True))
    pl.when(jnp.logical_not(odd))(lambda: run(False))


def soft_set(head, keys, query, probs, stats, diagonal=False):
    raw = dot(keys, query, 1, 1)
    if diagonal:
        raw = causal(raw, -BIG)
    top = jnp.max(raw, axis=0, keepdims=True)
    prob = jnp.exp2((raw - top) * EXP_SCALE)
    probs[head] = prob
    stats[0, pl.ds(head, 1), :] = top
    stats[1, pl.ds(head, 1), :] = jnp.sum(prob, axis=0, keepdims=True)


def delta_set(head, values, grad, probs, pgrads, stats):
    pgrad = dot(values, grad, 1, 1)
    pgrads[head] = pgrad
    stats[2, pl.ds(head, 1), :] = jnp.sum(probs[head] * pgrad, axis=0, keepdims=True)


def soft_kernel(near_span, q, g, k, v, qf, qn, k_up, *refs):
    own, mid, far, near, pr_own, pr_mid, pr_far, pr_near, pg_own = refs

    def run(odd):
        def step(head):
            at = columns(head)
            key_up, key, query = k_up[:, at], k[:, at], q[:, at]
            soft_set(head, key, query, pr_own, own, True)
            delta_set(head, v[:, at], g[:, at], pr_own, pg_own, own)
            soft_set(head, key_up, query, pr_mid, mid)
            soft_set(head, key_up, qf[:, at], pr_far, far)
            soft_set(head, key_up if odd else key, qn[:, at], pr_near, near)

        each_head(0, pg_own.shape[0], step)

    by_parity(near_span, run)


def delta_kernel(g, v_up, probs, soft, stats, pgrads):
    stats[0:2] = soft[0:2]

    def step(head):
        at = columns(head)
        delta_set(head, v_up[:, at], g[:, at], probs, pgrads, stats)

    each_head(0, probs.shape[0], step)


def delta_near_kernel(near_span, g, v, v_up, *refs):
    by_parity(near_span, lambda odd: delta_kernel(g, v_up if odd else v, *refs))


def merge(parts):
    top = parts[0][0]
    for part in parts[1:]:
        top = jnp.maximum(top, part[0])
    factors = [jnp.exp2((part[0] - top) * EXP_SCALE) for part in parts]
    norm, delta = 0.0, 0.0
    for part, factor in zip(parts, factors):
        norm = norm + factor * part[1]
        delta = delta + factor * part[2]
    return (top, norm, delta), factors


def rows_of(ref, at):
    return ref[0, at, :], ref[1, at, :], ref[2, at, :]


def masked_rows(ref, at, usable):
    top, norm, delta = rows_of(ref, at)
    return jnp.where(usable, top, -BIG), norm, delta


def put_norm(outs, at, factors, merged):
    inverse = 1.0 / merged[1]
    for out, factor in zip(outs, factors):
        out[0, at, :] = factor * inverse
        out[1, at, :] = merged[2] * inverse


def combine_local_kernel(spans, t, a, own, mid, near, out):
    flags = Flags(spans, t, a)
    for head in range(own.shape[1]):
        at = slice(head, head + 1)
        parts = [rows_of(own, at)]
        parts.append(masked_rows(mid, at, flags.usable(head, MID)))
        parts.append(masked_rows(near, at, flags.usable(head, NEAR)))
        merged, _ = merge(parts)
        bias = jnp.full_like(merged[0], 0.0)
        bias = jnp.where(flags.usable(head, FAR), bias, -BIG)
        for index, row in enumerate((*merged, bias)):
            out[index, at, :] = row


def combine_own_kernel(spans, t, a, own, mid, near, far, *outs):
    flags = Flags(spans, t, a)
    for head in range(own.shape[1]):
        at = slice(head, head + 1)
        parts = [rows_of(own, at)]
        for ref, section in ((mid, MID), (near, NEAR), (far, FAR)):
            parts.append(masked_rows(ref, at, flags.usable(head, section)))
        merged, factors = merge(parts)
        put_norm(outs, at, factors[:3], merged)


def combine_far_kernel(guest, far, out):
    for head in range(far.shape[1]):
        at = slice(head, head + 1)
        top, norm, delta = rows_of(far, at)
        parts = [(top + guest[3, at, :], norm, delta), rows_of(guest, at)]
        merged, factors = merge(parts)
        put_norm([out], at, factors[:1], merged)


def pair_terms(head, query, grad, keys, probs, pgrads, norm):
    factor, delta = norm[0, pl.ds(head, 1), :], norm[1, pl.ds(head, 1), :]
    prob = probs[head] * factor
    weight = prob.astype(jnp.bfloat16)
    dlogit = (prob * (pgrads[head] - delta)).astype(jnp.bfloat16)
    return dot(keys, dlogit, 0, 0), dot(dlogit, query, 1, 0), dot(weight, grad, 1, 0)


def terms_kernel(q, g, k, norm, probs, pgrads, *refs):
    dq, dk, dv = refs[-3:]

    def step(head):
        at = columns(head)
        query_term, dk[:, at], dv[:, at] = pair_terms(
            head, q[:, at], g[:, at], k[:, at], probs, pgrads, norm
        )
        query_term = query_term.T
        dq[:, at] = query_term + refs[0][:, at] if len(refs) > 3 else query_term

    each_head(0, probs.shape[0], step)


def pairs_kernel(
    near_span, first, qf, gf, qn, gn, k, k_up, norm_far, norm_near,
    pr_far, pg_far, pr_near, pg_near, dk_mid, dv_mid, *refs,
):
    dqf, dqn, back, dk, dv = refs[-5:]
    rows = qf.shape[0]

    def run(odd):
        def step(head):
            at, out = columns(head), columns(head - first)
            key_up = k_up[:, at]
            dq, key_back, value_back = pair_terms(
                head, qf[:, at], gf[:, at], key_up, pr_far, pg_far, norm_far
            )
            dqf[:, at] = (dq * SCALE).T.astype(dqf.dtype)
            key_near = key_up if odd else k[:, at]
            dq, key_term, value_term = pair_terms(
                head, qn[:, at], gn[:, at], key_near, pr_near, pg_near, norm_near
            )
            dqn[:, at] = (dq * SCALE).T.astype(dqn.dtype)
            key_back, value_back = dk_mid[:, at] + key_back, dv_mid[:, at] + value_back
            if odd:
                key_back, value_back = key_back + key_term, value_back + value_term
                key_term, value_term = jnp.zeros_like(key_term), jnp.zeros_like(value_term)
            back[:rows, out] = (key_back * SCALE).astype(back.dtype)
            back[rows:, out] = value_back.astype(back.dtype)
            dk[:, out] = key_term
            dv[:, out] = value_term

        each_head(first, dk.shape[1] // HDIM, step)

    by_parity(near_span, run)


def step_columns(block, first=0):
    return pl.ds(pl.multiple_of(pl.program_id(0) * block + first, block), block)


def finish_kernel(first, dk, dv, near_k, near_v, back, *refs):
    key_out, value_out = refs[-2:]
    rows, block = key_out.shape
    here, at = step_columns(block), step_columns(block, first)
    key_out[...] = (
        (dk[:, at] + near_k[:, here]) * SCALE + back[:rows, here].astype(jnp.float32)
    ).astype(key_out.dtype)
    value_out[...] = (
        dv[:, at] + near_v[:, here] + back[rows:, here].astype(jnp.float32)
    ).astype(value_out.dtype)


def finish_query_kernel(dq, far, near, out):
    at = step_columns(out.shape[1])
    total = dq[:, at] * SCALE + far[:, at].astype(jnp.float32) + near[:, at].astype(jnp.float32)
    out[...] = total.astype(out.dtype)


def body(queries, key_rows, value_rows, out_grad, out_proj, section_table, block_active):
    seq_count = lax.axis_size("seq")
    spans = [seq_count // 2 ** (index + 1) for index in range(SECTIONS)]
    mid_span, near_span = spans[MID], spans[NEAR]
    assert spans[FAR] == 2 * mid_span and mid_span == 2 * near_span
    assert block_active.shape[0] == 1
    rows, cols = queries.shape
    heads = cols // HDIM
    assert heads == sum(GROUPS)
    pair_work = rows * rows * HDIM
    flags = [section_table.T, block_active]

    wide_f32 = ((rows, cols), jnp.float32)
    wide_bf16 = ((rows, cols), jnp.bfloat16)
    stat = ((3, heads, rows), jnp.float32)
    norm = ((2, heads, rows), jnp.float32)
    square = ((heads, rows, rows), jnp.float32)

    def bound(kernel, *fixed):
        def run(*refs):
            kernel(*fixed, *refs)

        return run

    key_up = shift(key_rows, mid_span)
    value_up = shift(value_rows, mid_span)
    query_far = shift(queries, -mid_span)
    query_near = swap(queries, "seq", near_span)
    grads = attn_grad_of(out_grad, out_proj)
    grad_far = shift(grads, -mid_span)
    grad_near = swap(grads, "seq", near_span)
    query, key, value = staged(queries, key_rows, value_rows)

    self_stats, mid_soft, far_soft, near_soft, *probs, self_pgrad = call(
        bound(soft_kernel, near_span),
        [],
        [query, grads, key, value, query_far, query_near, key_up],
        [stat] * 4 + [square] * 5,
        heads * 5 * pair_work,
    )
    self_prob, mid_prob, far_prob, near_prob = probs

    def deltas(kernel, scalars, *ins):
        return call(kernel, scalars, ins, [stat, square], heads * pair_work)

    mid_stats, mid_pgrad = deltas(delta_kernel, [], grads, value_up, mid_prob, mid_soft)
    near_part, near_pgrad = deltas(
        bound(delta_near_kernel, near_span), [],
        grad_near, value, value_up, near_prob, near_soft,
    )
    near_stats = swap(near_part, "seq", near_span)
    far_part, far_pgrad = deltas(delta_kernel, [], grad_far, value_up, far_prob, far_soft)
    far_stats = shift(far_part, mid_span)
    self_squares, mid_squares = (self_prob, self_pgrad), (mid_prob, mid_pgrad)
    far_squares, near_squares = (far_prob, far_pgrad), (near_prob, near_pgrad)

    row_work = heads * rows * HDIM
    (merged,) = call(
        bound(combine_local_kernel, spans),
        flags,
        [self_stats, mid_stats, near_stats],
        [((4, heads, rows), jnp.float32)],
        row_work,
    )
    guest_stats = shift(merged, -mid_span)
    self_norm, mid_norm, near_norm = call(
        bound(combine_own_kernel, spans),
        flags,
        [self_stats, mid_stats, near_stats, far_stats],
        [norm] * 3,
        row_work,
    )
    near_norm = swap(near_norm, "seq", near_span)
    (far_norm,) = call(combine_far_kernel, [], [guest_stats, far_part], [norm], row_work)

    def terms(keys, row_norm, squares, *added):
        ins = [query, grads, keys, row_norm, *squares, *added]
        return call(terms_kernel, [], ins, [wide_f32] * 3, heads * 3 * pair_work)

    mid_query, *mid_terms = terms(key_up, mid_norm, mid_squares)
    guests = [query_far, grad_far, query_near, grad_near, key, key_up, far_norm, near_norm]
    guests += [*far_squares, *near_squares, *mid_terms]
    partial_queries, returned = [], []
    first = 0
    for group in GROUPS:
        width = group * HDIM
        start = len(guests)
        aliases = {start + number: number for number in range(len(partial_queries))}
        *partial_queries, back, near_key, near_value = call(
            bound(pairs_kernel, near_span, first),
            [],
            guests + partial_queries,
            [wide_bf16] * 2 + [((2 * rows, width), jnp.bfloat16)]
            + [((rows, width), jnp.float32)] * 2,
            group * 6 * pair_work,
            aliases,
        )
        returned.append((near_key, near_value, shift(back, -mid_span)))
        first += group
    query_far_part = shift(partial_queries[0], mid_span)
    query_near_part = swap(partial_queries[1], "seq", near_span)
    query_sum, *self_terms = terms(key, self_norm, self_squares, mid_query)

    block = 2 * HDIM
    outputs = []
    first = 0
    for index, group in enumerate(GROUPS):
        start = first * HDIM
        place_of = start // block
        ins = [*self_terms, *returned[index]]
        outputs = call(
            bound(finish_kernel, start),
            [],
            ins,
            [wide_bf16] * 2,
            group * rows * HDIM * HDIM,
            {len(ins) + number: number for number in range(len(outputs))},
            grid=(group * HDIM // block,),
            streams=[(array, pl.BlockSpec(memory_space=pl.ANY)) for array in outputs],
            blocks=[pl.BlockSpec((rows, block), lambda i, j=place_of: (0, i + j))] * 2,
        )
        first += group
    (query_grad,) = call(
        finish_query_kernel,
        [],
        [query_sum, query_far_part, query_near_part],
        [wide_bf16],
        heads * rows * HDIM,
        grid=(cols // block,),
        blocks=[pl.BlockSpec((rows, block), lambda i: (0, i))],
    )
    return query_grad, *outputs


def solution(mesh):
    return jax.shard_map(
        body,
        mesh=mesh,
        in_specs=(
            P("seq", "head"),
            P("seq", "head"),
            P("seq", "head"),
            P("seq", "head"),
            P("head", None),
            P("head", None),
            P("seq", None),
        ),
        out_specs=(P("seq", "head"), P("seq", "head"), P("seq", "head")),
        check_vma=False,
    )
```

```python
import math

import jax
import jax.numpy as jnp
from jax import lax
from jax.experimental import pallas as pl
from jax.experimental.pallas import tpu as pltpu
from jax.sharding import PartitionSpec as P


HDIM = 128
FAR, MID, NEAR = range(3)
SECTIONS = 3
GROUPS = (2, 4, 2)
HEADS_PER_STEP = 2
KERNEL_VMEM = 8 * 2**20
BIG = 1e30
SCALE = 1.0 / math.sqrt(HDIM)
LOG2E = math.log2(math.e)
EXP_SCALE = SCALE * LOG2E


def shift(value, steps):
    count = lax.axis_size("seq")
    low, high = max(0, -steps), min(count, count - steps)
    return lax.ppermute(value, "seq", [(src, src + steps) for src in range(low, high)])


def swap(value, axis, bit):
    pairs = [(src, src ^ bit) for src in range(lax.axis_size(axis))]
    return lax.ppermute(value, axis, pairs)


def dot(lhs, rhs, lhs_dim, rhs_dim):
    return lax.dot_general(
        lhs, rhs, (((lhs_dim,), (rhs_dim,)), ((), ())), preferred_element_type=jnp.float32
    )


def on_chip(array):
    return pltpu.with_memory_space_constraint(array, pltpu.VMEM)


def in_hbm(array):
    return pltpu.with_memory_space_constraint(array, pltpu.HBM)


def call(kernel, scalars, ins, outs, work, aliases=None, grid=None, streams=(), blocks=None, scratch=()):
    smem = pl.BlockSpec(memory_space=pltpu.SMEM)
    vmem = pl.BlockSpec(memory_space=pltpu.VMEM)
    return pl.pallas_call(
        kernel,
        grid=grid or (),
        in_specs=[smem] * len(scalars) + [vmem] * len(ins) + [spec for _, spec in streams],
        out_specs=blocks or [vmem] * len(outs),
        out_shape=[
            (jax.ShapeDtypeStruct if blocks else pltpu.VMEM)(shape, dtype)
            for shape, dtype in outs
        ],
        scratch_shapes=scratch,
        input_output_aliases=aliases or {},
        compiler_params=pltpu.CompilerParams(vmem_limit_bytes=KERNEL_VMEM),
        cost_estimate=pl.CostEstimate(
            flops=2 * work, bytes_accessed=0, transcendentals=work // HDIM
        ),
    )(*scalars, *[on_chip(array) for array in ins], *[array for array, _ in streams])


def each_head(first, count, step):
    def pair(index, carry):
        for offset in range(HEADS_PER_STEP):
            step(first + index * HEADS_PER_STEP + offset)
        return carry

    lax.fori_loop(0, count // HEADS_PER_STEP, pair, None)


def columns(head):
    return pl.ds(pl.multiple_of(head * HDIM, HDIM), HDIM)


def gathered_pieces(out_grad):
    pieces = {0: out_grad}
    bit = lax.axis_size("head") // 2
    while bit:
        for offset in list(pieces):
            pieces[offset | bit] = swap(pieces[offset], "head", bit)
        bit //= 2
    return [pieces[offset] for offset in range(len(pieces))]


def grad_kernel(*refs):
    head = lax.axis_index("head")
    *piece_refs, own_hbm, proj_hbm, out_ref, own_ref, proj, sems, own_sem = refs
    pieces = [own_ref, *piece_refs]
    width = own_ref.shape[1]
    count = sems.shape[0]
    block = proj.shape[0] // count
    own_copy = pltpu.make_async_copy(own_hbm, own_ref, own_sem)
    own_copy.start()
    copies = []
    for index in range(count):
        at = pl.ds(index * block, block)
        copies.append(pltpu.make_async_copy(proj_hbm.at[at], proj.at[at], sems.at[index]))
    for copy in copies[:2]:
        copy.start()
    own_copy.wait()
    for index, copy in enumerate(copies):
        copy.wait()
        if index + 2 < count:
            copies[index + 2].start()
        at = slice(index * block, (index + 1) * block)
        total = None
        for offset, piece in enumerate(pieces):
            start = pl.multiple_of((head ^ offset) * width, width)
            part = dot(piece[...], proj[at, pl.ds(start, width)], 1, 1)
            total = part if total is None else total + part
        out_ref[:, at] = total.astype(out_ref.dtype)


def attn_grad_of(out_grad, out_proj):
    pieces = gathered_pieces(out_grad)
    rows, width = out_grad.shape
    cols, features = out_proj.shape
    count = cols // (2 * HDIM)
    (result,) = call(
        grad_kernel,
        [],
        pieces[1:],
        [((rows, cols), jnp.bfloat16)],
        rows * cols * features,
        streams=[
            (in_hbm(array), pl.BlockSpec(memory_space=pltpu.HBM)) for array in (out_grad, out_proj)
        ],
        scratch=[
            pltpu.VMEM((rows, width), out_grad.dtype),
            pltpu.VMEM((cols, features), out_proj.dtype),
            pltpu.SemaphoreType.DMA((count,)),
            pltpu.SemaphoreType.DMA,
        ],
    )
    return result


def stage_kernel(*refs):
    count = len(refs) // 3
    sources, targets, sems = refs[:count], refs[count : 2 * count], refs[2 * count :]
    copies = [pltpu.make_async_copy(*each) for each in zip(sources, targets, sems)]
    for copy in copies:
        copy.start()
    for copy in copies:
        copy.wait()


def staged(*arrays):
    return pl.pallas_call(
        stage_kernel,
        in_specs=[pl.BlockSpec(memory_space=pltpu.HBM)] * len(arrays),
        out_specs=[pl.BlockSpec(memory_space=pltpu.VMEM)] * len(arrays),
        out_shape=[pltpu.VMEM(array.shape, array.dtype) for array in arrays],
        scratch_shapes=[pltpu.SemaphoreType.DMA] * len(arrays),
        compiler_params=pltpu.CompilerParams(vmem_limit_bytes=KERNEL_VMEM),
        cost_estimate=pl.CostEstimate(flops=10**6, bytes_accessed=0, transcendentals=0),
        name="stage",
    )(*[in_hbm(array) for array in arrays])


def causal(raw, fill):
    key_at = lax.broadcasted_iota(jnp.int32, raw.shape, 0)
    query_at = lax.broadcasted_iota(jnp.int32, raw.shape, 1)
    return jnp.where(key_at <= query_at, raw, fill)


class Flags:
    def __init__(self, spans, table_ref, active_ref):
        self.spans, self.table, self.active = spans, table_ref, active_ref
        self.place = lax.axis_index("seq")

    def usable(self, head, section):
        used = self.table[section, head] * self.active[0, section] > 0
        return used & (self.place >= self.spans[section])

    def bias(self, section, shape):
        head_at = lax.broadcasted_iota(jnp.int32, shape, 0)
        total = jnp.zeros(shape, jnp.float32)
        for head in range(shape[0]):
            value = jnp.where(self.usable(head, section), 0.0, -BIG)
            total = jnp.where(head_at == head, value, total)
        return total


def by_parity(near_span, run):
    odd = (lax.axis_index("seq") // near_span) % 2 == 1
    pl.when(odd)(lambda: run(True))
    pl.when(jnp.logical_not(odd))(lambda: run(False))


def soft_set(head, keys, query, probs, stats, base=0, diagonal=False):
    raw = dot(keys, query, 1, 1)
    if diagonal:
        raw = causal(raw, -BIG)
    top = jnp.max(raw, axis=0, keepdims=True)
    prob = jnp.exp2((raw - top) * EXP_SCALE)
    probs[head] = prob
    stats[base, pl.ds(head, 1), :] = top
    stats[base + 1, pl.ds(head, 1), :] = jnp.sum(prob, axis=0, keepdims=True)


def delta_set(head, values, grad, probs, pgrads, stats, base=0):
    pgrad = dot(values, grad, 1, 1)
    pgrads[head] = pgrad
    row = jnp.sum(probs[head] * pgrad, axis=0, keepdims=True)
    stats[base + 2, pl.ds(head, 1), :] = row


def soft_kernel(near_span, q, g, k, v, qf, k_up, k_x, *refs):
    own, mid, far, near, pr_own, pr_mid, pr_far, pr_near, pg_own = refs

    def run(odd):
        def step(head):
            at = columns(head)
            key_up, query, guest = k_up[:, at], q[:, at], qf[:, at]
            soft_set(head, k[:, at], query, pr_own, own, diagonal=True)
            delta_set(head, v[:, at], g[:, at], pr_own, pg_own, own)
            soft_set(head, key_up, query, pr_mid, mid)
            soft_set(head, key_up, guest, pr_far, far)
            soft_set(head, k_x[:, at], query if odd else guest, pr_near, near)

        each_head(0, pg_own.shape[0], step)

    by_parity(near_span, run)


def delta_mid_kernel(g, v_up, probs, soft, stats, pgrads):
    stats[0:2] = soft[0:2]

    def step(head):
        at = columns(head)
        delta_set(head, v_up[:, at], g[:, at], probs, pgrads, stats)

    each_head(0, probs.shape[0], step)


def delta_near_kernel(near_span, g, v_x, probs, soft, stats, pgrads):
    def run(odd):
        if odd:
            delta_mid_kernel(g, v_x, probs, soft, stats, pgrads)

    by_parity(near_span, run)


def delta_guest_kernel(near_span, gf, v_up, v_x, pr_far, far, pr_near, near, _, up, pg_far, pg_near):
    up[0:2] = far[0:2]
    up[3:5] = near[0:2]

    def run(odd):
        def step(head):
            at = columns(head)
            grad = gf[:, at]
            delta_set(head, v_up[:, at], grad, pr_far, pg_far, up)
            if not odd:
                delta_set(head, v_x[:, at], grad, pr_near, pg_near, up, 3)

        each_head(0, pr_far.shape[0], step)

    by_parity(near_span, run)


def merge(parts):
    top = parts[0][0]
    for part in parts[1:]:
        top = jnp.maximum(top, part[0])
    factors = [jnp.exp2((part[0] - top) * EXP_SCALE) for part in parts]
    norm, delta = 0.0, 0.0
    for part, factor in zip(parts, factors):
        norm = norm + factor * part[1]
        delta = delta + factor * part[2]
    return (top, norm, delta), factors


def part_of(ref, bias=0.0, base=0):
    return ref[base] + bias, ref[base + 1], ref[base + 2]


def put_norm(outs, factors, merged):
    inverse = 1.0 / merged[1]
    delta = merged[2] * inverse
    for out, factor in zip(outs, factors):
        out[0] = factor * inverse
        out[1] = delta


def combine_local_kernel(spans, t, a, own, mid, near, out):
    flags = Flags(spans, t, a)

    def run(odd):
        shape = own.shape[1:]
        near_bias = flags.bias(NEAR, shape)
        parts = [part_of(own), part_of(mid, flags.bias(MID, shape))]
        if odd:
            parts.append(part_of(near, near_bias))
            near_bias = jnp.full(shape, -BIG, jnp.float32)
        merged, _ = merge(parts)
        for index, row in enumerate((*merged, flags.bias(FAR, shape), near_bias)):
            out[index] = row

    by_parity(spans[NEAR], run)


def combine_own_kernel(spans, t, a, own, mid, near, up, *outs):
    flags = Flags(spans, t, a)

    def run(odd):
        shape = own.shape[1:]
        near_bias = flags.bias(NEAR, shape)
        parts = [part_of(own), part_of(mid, flags.bias(MID, shape))]
        parts.append(part_of(near, near_bias) if odd else part_of(up, near_bias, 3))
        parts.append(part_of(up, flags.bias(FAR, shape)))
        merged, factors = merge(parts)
        put_norm(outs if odd else outs[:2], factors, merged)

    by_parity(spans[NEAR], run)


def combine_guest_kernel(near_span, guest, up, far_out, near_out):
    def run(odd):
        parts = [part_of(up, guest[3])]
        if not odd:
            parts.append(part_of(up, guest[4], 3))
        parts.append(part_of(guest))
        merged, factors = merge(parts)
        put_norm((far_out, near_out), factors[:-1], merged)

    by_parity(near_span, run)


def pair_terms(head, query, grad, keys, probs, pgrads, norm):
    factor, delta = norm[0, pl.ds(head, 1), :], norm[1, pl.ds(head, 1), :]
    prob = probs[head] * factor
    weight = prob.astype(jnp.bfloat16)
    dlogit = (prob * (pgrads[head] - delta)).astype(jnp.bfloat16)
    return dot(keys, dlogit, 0, 0), dot(dlogit, query, 1, 0), dot(weight, grad, 1, 0)


def self_kernel(q, g, k, norm, probs, pgrads, dq_part, dq, dk, dv):
    def step(head):
        at = columns(head)
        query_term, dk[:, at], dv[:, at] = pair_terms(
            head, q[:, at], g[:, at], k[:, at], probs, pgrads, norm
        )
        dq[:, at] = query_term.T + dq_part[:, at]

    each_head(0, probs.shape[0], step)


def guest_terms_kernel(
    near_span, q, g, k_up, k_x, norm_far, norm_near, pr_far, pg_far, pr_near, pg_near,
    dq, dk_far, dv_far, dk_near, dv_near,
):
    def run(odd):
        def step(head):
            at = columns(head)
            query, grad = q[:, at], g[:, at]
            query_term, dk_far[:, at], dv_far[:, at] = pair_terms(
                head, query, grad, k_up[:, at], pr_far, pg_far, norm_far
            )
            if not odd:
                more, dk_near[:, at], dv_near[:, at] = pair_terms(
                    head, query, grad, k_x[:, at], pr_near, pg_near, norm_near
                )
                query_term = query_term + more
            dq[:, at] = (query_term * SCALE).T.astype(dq.dtype)

        each_head(0, pr_far.shape[0], step)

    by_parity(near_span, run)


def own_terms_kernel(
    near_span, first, q, g, k_up, k_x, norm_mid, norm_near, pr_mid, pg_mid, pr_near, pg_near,
    dk_far, dv_far, dk_near, dv_near, *refs,
):
    dq, back, cross = refs[-3:]
    rows = q.shape[0]

    def run(odd):
        def step(head):
            at, out = columns(head), columns(head - first)
            query, grad = q[:, at], g[:, at]
            query_term, key_term, value_term = pair_terms(
                head, query, grad, k_up[:, at], pr_mid, pg_mid, norm_mid
            )
            back[:rows, out] = ((key_term + dk_far[:, at]) * SCALE).astype(back.dtype)
            back[rows:, out] = (value_term + dv_far[:, at]).astype(back.dtype)
            if odd:
                more, key_term, value_term = pair_terms(
                    head, query, grad, k_x[:, at], pr_near, pg_near, norm_near
                )
                query_term = query_term + more
            else:
                key_term, value_term = dk_near[:, at], dv_near[:, at]
            cross[:rows, out] = (key_term * SCALE).astype(cross.dtype)
            cross[rows:, out] = value_term.astype(cross.dtype)
            dq[:, at] = query_term.T

        each_head(first, cross.shape[1] // HDIM, step)

    by_parity(near_span, run)


def step_columns(block, first=0):
    return pl.ds(pl.multiple_of(pl.program_id(0) * block + first, block), block)


def finish_kernel(first, dk, dv, back, cross, *refs):
    key_out, value_out = refs[-2:]
    rows, block = key_out.shape
    here, at = step_columns(block), step_columns(block, first)
    for rows_at, total, out in (
        (slice(0, rows), dk[:, at] * SCALE, key_out),
        (slice(rows, 2 * rows), dv[:, at], value_out),
    ):
        for ref in (back, cross):
            total = total + ref[rows_at, here].astype(jnp.float32)
        out[...] = total.astype(out.dtype)


def finish_query_kernel(dq, guest, out):
    at = step_columns(out.shape[1])
    total = dq[:, at] * SCALE + guest[:, at].astype(jnp.float32)
    out[...] = total.astype(out.dtype)


def body(queries, key_rows, value_rows, out_grad, out_proj, section_table, block_active):
    seq_count = lax.axis_size("seq")
    spans = [seq_count // 2 ** (index + 1) for index in range(SECTIONS)]
    mid_span, near_span = spans[MID], spans[NEAR]
    assert spans[FAR] == 2 * mid_span and mid_span == 2 * near_span
    assert block_active.shape[0] == 1
    rows, cols = queries.shape
    heads = cols // HDIM
    assert heads == sum(GROUPS)
    pair_work = rows * rows * HDIM
    flags = [section_table.T, block_active]

    wide_f32 = ((rows, cols), jnp.float32)
    wide_bf16 = ((rows, cols), jnp.bfloat16)

    def table(count):
        return ((count, heads, rows), jnp.float32)

    stat, norm = table(3), table(2)
    square = ((heads, rows, rows), jnp.float32)
    row_work = heads * rows * HDIM

    def bound(kernel, *fixed):
        def run(*refs):
            kernel(*fixed, *refs)

        return run

    key_up = shift(key_rows, mid_span)
    value_up = shift(value_rows, mid_span)
    key_x = swap(key_rows, "seq", near_span)
    value_x = swap(value_rows, "seq", near_span)
    guest_query = shift(queries, -mid_span)
    grads = attn_grad_of(out_grad, out_proj)
    guest_grad = shift(grads, -mid_span)
    query, key, value = staged(queries, key_rows, value_rows)

    self_stats, mid_soft, far_soft, near_soft, *probs, self_pgrad = call(
        bound(soft_kernel, near_span),
        [],
        [query, grads, key, value, guest_query, key_up, key_x],
        [stat] * 4 + [square] * 5,
        heads * 5 * pair_work,
    )
    self_prob, mid_prob, far_prob, near_prob = probs

    def deltas(kernel, *ins):
        return call(kernel, [], ins, [stat, square], heads * pair_work)

    mid_stats, mid_pgrad = deltas(delta_mid_kernel, grads, value_up, mid_prob, mid_soft)
    near_stats, near_pgrad = deltas(
        bound(delta_near_kernel, near_span), grads, value_x, near_prob, near_soft
    )
    (merged,) = call(
        bound(combine_local_kernel, spans),
        flags,
        [self_stats, mid_stats, near_stats],
        [table(5)],
        row_work,
    )
    guest_stats = shift(merged, -mid_span)
    ins = [guest_grad, value_up, value_x, far_prob, far_soft, near_prob, near_soft, near_pgrad]
    up_part, far_pgrad, near_pgrad = call(
        bound(delta_guest_kernel, near_span),
        [],
        ins,
        [table(6), square, square],
        heads * 2 * pair_work,
        {len(ins) - 1: 2},
    )
    up_stats = shift(up_part, mid_span)
    far_norm, near_norm_guest = call(
        bound(combine_guest_kernel, near_span), [], [guest_stats, up_part], [norm] * 2, row_work
    )
    near_squares = [near_prob, near_pgrad]
    ins = [guest_query, guest_grad, key_up, key_x, far_norm, near_norm_guest]
    guest_part, *guest_terms = call(
        bound(guest_terms_kernel, near_span),
        [],
        [*ins, far_prob, far_pgrad, *near_squares],
        [wide_bf16] + [wide_f32] * 4,
        heads * 6 * pair_work,
    )
    self_norm, mid_norm, near_norm = call(
        bound(combine_own_kernel, spans),
        flags,
        [self_stats, mid_stats, near_stats, up_stats],
        [norm] * 3,
        row_work,
    )
    query_part, returned = [], []
    first = 0
    for group in GROUPS:
        ins = [query, grads, key_up, key_x, mid_norm, near_norm, mid_prob, mid_pgrad]
        ins += [*near_squares, *guest_terms]
        half = ((2 * rows, group * HDIM), jnp.bfloat16)
        *query_part, back, cross = call(
            bound(own_terms_kernel, near_span, first),
            [],
            ins + query_part,
            [wide_f32, half, half],
            group * 6 * pair_work,
            {len(ins): 0} if query_part else {},
        )
        cross = swap(cross, "seq", near_span)
        returned.append((shift(back, -mid_span), cross))
        first += group
    guest_part = shift(guest_part, mid_span)
    query_sum, *self_terms = call(
        self_kernel,
        [],
        [query, grads, key, self_norm, self_prob, self_pgrad, *query_part],
        [wide_f32] * 3,
        heads * 3 * pair_work,
    )

    block = 2 * HDIM
    outputs = []
    first = 0
    for index, group in enumerate(GROUPS):
        start = first * HDIM
        place_of = start // block
        ins = [*self_terms, *returned[index]]
        outputs = call(
            bound(finish_kernel, start),
            [],
            ins,
            [wide_bf16] * 2,
            group * rows * HDIM * HDIM,
            {len(ins) + number: number for number in range(len(outputs))},
            grid=(group * HDIM // block,),
            streams=[(array, pl.BlockSpec(memory_space=pl.ANY)) for array in outputs],
            blocks=[pl.BlockSpec((rows, block), lambda i, j=place_of: (0, i + j))] * 2,
        )
        first += group
    (query_grad,) = call(
        finish_query_kernel,
        [],
        [query_sum, guest_part],
        [wide_bf16],
        heads * rows * HDIM,
        grid=(cols // block,),
        blocks=[pl.BlockSpec((rows, block), lambda i: (0, i))],
    )
    return query_grad, *outputs


def solution(mesh):
    return jax.shard_map(
        body,
        mesh=mesh,
        in_specs=(
            P("seq", "head"),
            P("seq", "head"),
            P("seq", "head"),
            P("seq", "head"),
            P("head", None),
            P("head", None),
            P("seq", None),
        ),
        out_specs=(P("seq", "head"), P("seq", "head"), P("seq", "head")),
        check_vma=False,
    )
```

```python
import math

import jax
import jax.numpy as jnp
from jax import lax
from jax.experimental import pallas as pl
from jax.experimental.pallas import tpu as pltpu
from jax.sharding import PartitionSpec as P


HDIM = 128
FAR, MID, NEAR = range(3)
SECTIONS = 3
GROUPS = (2, 4, 2)
HEADS_PER_STEP = 2
KERNEL_VMEM = 8 * 2**20
BIG = 1e30
SCALE = 1.0 / math.sqrt(HDIM)
LOG2E = math.log2(math.e)
EXP_SCALE = SCALE * LOG2E


def shift(value, steps):
    count = lax.axis_size("seq")
    low, high = max(0, -steps), min(count, count - steps)
    return lax.ppermute(value, "seq", [(src, src + steps) for src in range(low, high)])


def swap(value, axis, bit):
    pairs = [(src, src ^ bit) for src in range(lax.axis_size(axis))]
    return lax.ppermute(value, axis, pairs)


def dot(lhs, rhs, lhs_dim, rhs_dim):
    return lax.dot_general(
        lhs, rhs, (((lhs_dim,), (rhs_dim,)), ((), ())), preferred_element_type=jnp.float32
    )


def on_chip(array):
    return pltpu.with_memory_space_constraint(array, pltpu.VMEM)


def in_hbm(array):
    return pltpu.with_memory_space_constraint(array, pltpu.HBM)


def call(kernel, scalars, ins, outs, work, aliases=None, grid=None, streams=(), blocks=None, scratch=()):
    smem = pl.BlockSpec(memory_space=pltpu.SMEM)
    vmem = pl.BlockSpec(memory_space=pltpu.VMEM)
    return pl.pallas_call(
        kernel,
        grid=grid or (),
        in_specs=[smem] * len(scalars) + [vmem] * len(ins) + [spec for _, spec in streams],
        out_specs=blocks or [vmem] * len(outs),
        out_shape=[
            (jax.ShapeDtypeStruct if blocks else pltpu.VMEM)(shape, dtype)
            for shape, dtype in outs
        ],
        scratch_shapes=scratch,
        input_output_aliases=aliases or {},
        compiler_params=pltpu.CompilerParams(vmem_limit_bytes=KERNEL_VMEM),
        cost_estimate=pl.CostEstimate(
            flops=2 * work, bytes_accessed=0, transcendentals=work // HDIM
        ),
    )(*scalars, *[on_chip(array) for array in ins], *[array for array, _ in streams])


def each_head(first, count, step):
    def pair(index, carry):
        for offset in range(HEADS_PER_STEP):
            step(first + index * HEADS_PER_STEP + offset)
        return carry

    lax.fori_loop(0, count // HEADS_PER_STEP, pair, None)


def columns(head):
    return pl.ds(pl.multiple_of(head * HDIM, HDIM), HDIM)


def gathered_pieces(out_grad):
    pieces = {0: out_grad}
    bit = lax.axis_size("head") // 2
    while bit:
        for offset in list(pieces):
            pieces[offset | bit] = swap(pieces[offset], "head", bit)
        bit //= 2
    return [pieces[offset] for offset in range(len(pieces))]


def grad_kernel(*refs):
    head = lax.axis_index("head")
    *piece_refs, own_hbm, proj_hbm, out_ref, own_ref, proj, sems, own_sem = refs
    pieces = [own_ref, *piece_refs]
    width = own_ref.shape[1]
    count = sems.shape[0]
    block = proj.shape[0] // count
    own_copy = pltpu.make_async_copy(own_hbm, own_ref, own_sem)
    own_copy.start()
    copies = []
    for index in range(count):
        at = pl.ds(index * block, block)
        copies.append(pltpu.make_async_copy(proj_hbm.at[at], proj.at[at], sems.at[index]))
    for copy in copies[:2]:
        copy.start()
    own_copy.wait()
    for index, copy in enumerate(copies):
        copy.wait()
        if index + 2 < count:
            copies[index + 2].start()
        at = slice(index * block, (index + 1) * block)
        total = None
        for offset, piece in enumerate(pieces):
            start = pl.multiple_of((head ^ offset) * width, width)
            part = dot(piece[...], proj[at, pl.ds(start, width)], 1, 1)
            total = part if total is None else total + part
        out_ref[:, at] = total.astype(out_ref.dtype)


def attn_grad_of(out_grad, out_proj):
    pieces = gathered_pieces(out_grad)
    rows, width = out_grad.shape
    cols, features = out_proj.shape
    count = cols // (2 * HDIM)
    (result,) = call(
        grad_kernel,
        [],
        pieces[1:],
        [((rows, cols), jnp.bfloat16)],
        rows * cols * features,
        streams=[
            (in_hbm(array), pl.BlockSpec(memory_space=pltpu.HBM)) for array in (out_grad, out_proj)
        ],
        scratch=[
            pltpu.VMEM((rows, width), out_grad.dtype),
            pltpu.VMEM((cols, features), out_proj.dtype),
            pltpu.SemaphoreType.DMA((count,)),
            pltpu.SemaphoreType.DMA,
        ],
    )
    return result


def stage_kernel(*refs):
    count = len(refs) // 3
    sources, targets, sems = refs[:count], refs[count : 2 * count], refs[2 * count :]
    copies = [pltpu.make_async_copy(*each) for each in zip(sources, targets, sems)]
    for copy in copies:
        copy.start()
    for copy in copies:
        copy.wait()


def staged(*arrays):
    return pl.pallas_call(
        stage_kernel,
        in_specs=[pl.BlockSpec(memory_space=pltpu.HBM)] * len(arrays),
        out_specs=[pl.BlockSpec(memory_space=pltpu.VMEM)] * len(arrays),
        out_shape=[pltpu.VMEM(array.shape, array.dtype) for array in arrays],
        scratch_shapes=[pltpu.SemaphoreType.DMA] * len(arrays),
        compiler_params=pltpu.CompilerParams(vmem_limit_bytes=KERNEL_VMEM),
        cost_estimate=pl.CostEstimate(flops=10**6, bytes_accessed=0, transcendentals=0),
        name="stage",
    )(*[in_hbm(array) for array in arrays])


def causal(raw, fill):
    key_at = lax.broadcasted_iota(jnp.int32, raw.shape, 0)
    query_at = lax.broadcasted_iota(jnp.int32, raw.shape, 1)
    return jnp.where(key_at <= query_at, raw, fill)


class Flags:
    def __init__(self, spans, table_ref, active_ref):
        self.spans, self.table, self.active = spans, table_ref, active_ref
        self.place = lax.axis_index("seq")

    def usable(self, head, section):
        used = self.table[section, head] * self.active[0, section] > 0
        return used & (self.place >= self.spans[section])

    def bias(self, section, shape):
        head_at = lax.broadcasted_iota(jnp.int32, shape, 0)
        total = jnp.zeros(shape, jnp.float32)
        for head in range(shape[0]):
            value = jnp.where(self.usable(head, section), 0.0, -BIG)
            total = jnp.where(head_at == head, value, total)
        return total


def by_parity(near_span, run):
    odd = (lax.axis_index("seq") // near_span) % 2 == 1
    pl.when(odd)(lambda: run(True))
    pl.when(jnp.logical_not(odd))(lambda: run(False))


def soft_set(head, keys, query, probs, stats, base=0, diagonal=False):
    raw = dot(keys, query, 1, 1)
    if diagonal:
        raw = causal(raw, -BIG)
    top = jnp.max(raw, axis=0, keepdims=True)
    prob = jnp.exp2((raw - top) * EXP_SCALE)
    probs[head] = prob
    stats[base, pl.ds(head, 1), :] = top
    stats[base + 1, pl.ds(head, 1), :] = jnp.sum(prob, axis=0, keepdims=True)


def delta_set(head, values, grad, probs, pgrads, stats, base=0):
    pgrad = dot(values, grad, 1, 1)
    pgrads[head] = pgrad
    row = jnp.sum(probs[head] * pgrad, axis=0, keepdims=True)
    stats[base + 2, pl.ds(head, 1), :] = row


def soft_kernel(near_span, q, g, k, v, qf, k_up, k_x, *refs):
    own, mid, far, near, pr_own, pr_mid, pr_far, pr_near, pg_own = refs

    def run(odd):
        def step(head):
            at = columns(head)
            key_up, query, guest = k_up[:, at], q[:, at], qf[:, at]
            soft_set(head, k[:, at], query, pr_own, own, diagonal=True)
            delta_set(head, v[:, at], g[:, at], pr_own, pg_own, own)
            soft_set(head, key_up, query, pr_mid, mid)
            soft_set(head, key_up, guest, pr_far, far)
            soft_set(head, k_x[:, at], query if odd else guest, pr_near, near)

        each_head(0, pg_own.shape[0], step)

    by_parity(near_span, run)


def delta_mid_kernel(g, v_up, probs, soft, stats, pgrads):
    stats[0:2] = soft[0:2]

    def step(head):
        at = columns(head)
        delta_set(head, v_up[:, at], g[:, at], probs, pgrads, stats)

    each_head(0, probs.shape[0], step)


def delta_near_kernel(near_span, g, v_x, probs, soft, stats, pgrads):
    def run(odd):
        if odd:
            delta_mid_kernel(g, v_x, probs, soft, stats, pgrads)

    by_parity(near_span, run)


def delta_guest_kernel(near_span, gf, v_up, v_x, pr_far, far, pr_near, near, _, up, pg_far, pg_near):
    up[0:2] = far[0:2]
    up[3:5] = near[0:2]

    def run(odd):
        def step(head):
            at = columns(head)
            grad = gf[:, at]
            delta_set(head, v_up[:, at], grad, pr_far, pg_far, up)
            if not odd:
                delta_set(head, v_x[:, at], grad, pr_near, pg_near, up, 3)

        each_head(0, pr_far.shape[0], step)

    by_parity(near_span, run)


def merge(parts):
    top = parts[0][0]
    for part in parts[1:]:
        top = jnp.maximum(top, part[0])
    factors = [jnp.exp2((part[0] - top) * EXP_SCALE) for part in parts]
    norm, delta = 0.0, 0.0
    for part, factor in zip(parts, factors):
        norm = norm + factor * part[1]
        delta = delta + factor * part[2]
    return (top, norm, delta), factors


def part_of(ref, bias=0.0, base=0):
    return ref[base] + bias, ref[base + 1], ref[base + 2]


def put_norm(outs, factors, merged):
    inverse = 1.0 / merged[1]
    delta = merged[2] * inverse
    for out, factor in zip(outs, factors):
        out[0] = factor * inverse
        out[1] = delta


def bias_kernel(spans, t, a, out):
    flags = Flags(spans, t, a)
    for section in range(SECTIONS):
        out[section] = flags.bias(section, out.shape[1:])


def combine_local_kernel(near_span, bias, own, mid, near, out):
    def run(odd):
        near_bias = bias[NEAR]
        parts = [part_of(own), part_of(mid, bias[MID])]
        if odd:
            parts.append(part_of(near, near_bias))
            near_bias = jnp.full(near_bias.shape, -BIG, jnp.float32)
        merged, _ = merge(parts)
        for index, row in enumerate((*merged, bias[FAR], near_bias)):
            out[index] = row

    by_parity(near_span, run)


def combine_own_kernel(near_span, bias, own, mid, near, up, *outs):
    def run(odd):
        parts = [part_of(own), part_of(mid, bias[MID])]
        parts.append(part_of(near, bias[NEAR]) if odd else part_of(up, bias[NEAR], 3))
        parts.append(part_of(up, bias[FAR]))
        merged, factors = merge(parts)
        put_norm(outs if odd else outs[:2], factors, merged)

    by_parity(near_span, run)


def combine_guest_kernel(near_span, guest, up, far_out, near_out):
    def run(odd):
        parts = [part_of(up, guest[3])]
        if not odd:
            parts.append(part_of(up, guest[4], 3))
        parts.append(part_of(guest))
        merged, factors = merge(parts)
        put_norm((far_out, near_out), factors[:-1], merged)

    by_parity(near_span, run)


def pair_terms(head, query, grad, keys, probs, pgrads, norm):
    factor, delta = norm[0, pl.ds(head, 1), :], norm[1, pl.ds(head, 1), :]
    prob = probs[head] * factor
    weight = prob.astype(jnp.bfloat16)
    dlogit = (prob * (pgrads[head] - delta)).astype(jnp.bfloat16)
    return dot(keys, dlogit, 0, 0), dot(dlogit, query, 1, 0), dot(weight, grad, 1, 0)


def self_kernel(q, g, k, norm, probs, pgrads, dq_part, dq, dk, dv):
    def step(head):
        at = columns(head)
        query_term, dk[:, at], dv[:, at] = pair_terms(
            head, q[:, at], g[:, at], k[:, at], probs, pgrads, norm
        )
        dq[:, at] = query_term.T + dq_part[:, at]

    each_head(0, probs.shape[0], step)


def guest_terms_kernel(
    near_span, first, q, g, k_up, k_x, norm_far, norm_near, pr_far, pg_far, pr_near, pg_near, *refs
):
    dq, dk_far, dv_far, dk_near, dv_near = refs[-5:]

    def run(odd):
        def step(head):
            at, out = columns(head), columns(head - first)
            query, grad = q[:, at], g[:, at]
            query_term, dk_far[:, out], dv_far[:, out] = pair_terms(
                head, query, grad, k_up[:, at], pr_far, pg_far, norm_far
            )
            if not odd:
                more, dk_near[:, out], dv_near[:, out] = pair_terms(
                    head, query, grad, k_x[:, at], pr_near, pg_near, norm_near
                )
                query_term = query_term + more
            dq[:, at] = (query_term * SCALE).T.astype(dq.dtype)

        each_head(first, dk_far.shape[1] // HDIM, step)

    by_parity(near_span, run)


def own_terms_kernel(
    near_span, first, q, g, k_up, k_x, norm_mid, norm_near, pr_mid, pg_mid, pr_near, pg_near,
    dk_far, dv_far, dk_near, dv_near, *refs,
):
    dq, back, cross = refs[-3:]
    rows = q.shape[0]

    def run(odd):
        def step(head):
            at, out = columns(head), columns(head - first)
            query, grad = q[:, at], g[:, at]
            query_term, key_term, value_term = pair_terms(
                head, query, grad, k_up[:, at], pr_mid, pg_mid, norm_mid
            )
            back[:rows, out] = ((key_term + dk_far[:, out]) * SCALE).astype(back.dtype)
            back[rows:, out] = (value_term + dv_far[:, out]).astype(back.dtype)
            if odd:
                more, key_term, value_term = pair_terms(
                    head, query, grad, k_x[:, at], pr_near, pg_near, norm_near
                )
                query_term = query_term + more
            else:
                key_term, value_term = dk_near[:, out], dv_near[:, out]
            cross[:rows, out] = (key_term * SCALE).astype(cross.dtype)
            cross[rows:, out] = value_term.astype(cross.dtype)
            dq[:, at] = query_term.T

        each_head(first, cross.shape[1] // HDIM, step)

    by_parity(near_span, run)


def step_columns(block, first=0):
    return pl.ds(pl.multiple_of(pl.program_id(0) * block + first, block), block)


def finish_kernel(first, dk, dv, back, cross, *refs):
    key_out, value_out = refs[-2:]
    rows, block = key_out.shape
    here, at = step_columns(block), step_columns(block, first)
    for rows_at, total, out in (
        (slice(0, rows), dk[:, at] * SCALE, key_out),
        (slice(rows, 2 * rows), dv[:, at], value_out),
    ):
        for ref in (back, cross):
            total = total + ref[rows_at, here].astype(jnp.float32)
        out[...] = total.astype(out.dtype)


def finish_query_kernel(dq, guest, out):
    at = step_columns(out.shape[1])
    total = dq[:, at] * SCALE + guest[:, at].astype(jnp.float32)
    out[...] = total.astype(out.dtype)


def body(queries, key_rows, value_rows, out_grad, out_proj, section_table, block_active):
    seq_count = lax.axis_size("seq")
    spans = [seq_count // 2 ** (index + 1) for index in range(SECTIONS)]
    mid_span, near_span = spans[MID], spans[NEAR]
    assert spans[FAR] == 2 * mid_span and mid_span == 2 * near_span
    assert block_active.shape[0] == 1
    rows, cols = queries.shape
    heads = cols // HDIM
    assert heads == sum(GROUPS)
    pair_work = rows * rows * HDIM
    flags = [section_table.T, block_active]

    wide_f32 = ((rows, cols), jnp.float32)
    wide_bf16 = ((rows, cols), jnp.bfloat16)

    def table(count):
        return ((count, heads, rows), jnp.float32)

    stat, norm = table(3), table(2)
    square = ((heads, rows, rows), jnp.float32)
    row_work = heads * rows * HDIM

    def bound(kernel, *fixed):
        def run(*refs):
            kernel(*fixed, *refs)

        return run

    key_up = shift(key_rows, mid_span)
    value_up = shift(value_rows, mid_span)
    key_x = swap(key_rows, "seq", near_span)
    value_x = swap(value_rows, "seq", near_span)
    guest_query = shift(queries, -mid_span)
    grads = attn_grad_of(out_grad, out_proj)
    guest_grad = shift(grads, -mid_span)
    query, key, value = staged(queries, key_rows, value_rows)

    (bias,) = call(bound(bias_kernel, spans), flags, [], [stat], row_work)
    self_stats, mid_soft, far_soft, near_soft, *probs, self_pgrad = call(
        bound(soft_kernel, near_span),
        [],
        [query, grads, key, value, guest_query, key_up, key_x],
        [stat] * 4 + [square] * 5,
        heads * 5 * pair_work,
    )
    self_prob, mid_prob, far_prob, near_prob = probs

    def deltas(kernel, *ins):
        return call(kernel, [], ins, [stat, square], heads * pair_work)

    mid_stats, mid_pgrad = deltas(delta_mid_kernel, grads, value_up, mid_prob, mid_soft)
    near_stats, near_pgrad = deltas(
        bound(delta_near_kernel, near_span), grads, value_x, near_prob, near_soft
    )
    (merged,) = call(
        bound(combine_local_kernel, near_span),
        [],
        [bias, self_stats, mid_stats, near_stats],
        [table(5)],
        row_work,
    )
    guest_stats = shift(merged, -mid_span)
    ins = [guest_grad, value_up, value_x, far_prob, far_soft, near_prob, near_soft, near_pgrad]
    up_part, far_pgrad, near_pgrad = call(
        bound(delta_guest_kernel, near_span),
        [],
        ins,
        [table(6), square, square],
        heads * 2 * pair_work,
        {len(ins) - 1: 2},
    )
    up_stats = shift(up_part, mid_span)
    far_norm, near_norm_guest = call(
        bound(combine_guest_kernel, near_span), [], [guest_stats, up_part], [norm] * 2, row_work
    )
    near_squares = [near_prob, near_pgrad]
    self_norm, mid_norm, near_norm = call(
        bound(combine_own_kernel, near_span),
        [],
        [bias, self_stats, mid_stats, near_stats, up_stats],
        [norm] * 3,
        row_work,
    )
    guest_part, query_part, returned = [], [], []
    first = 0
    for group in GROUPS:
        narrow = (rows, group * HDIM)
        ins = [guest_query, guest_grad, key_up, key_x, far_norm, near_norm_guest]
        ins += [far_prob, far_pgrad, *near_squares]
        *guest_part, far_key, far_value, near_key, near_value = call(
            bound(guest_terms_kernel, near_span, first),
            [],
            ins + guest_part,
            [wide_bf16] + [(narrow, jnp.float32)] * 4,
            group * 6 * pair_work,
            {len(ins): 0} if guest_part else {},
        )
        ins = [query, grads, key_up, key_x, mid_norm, near_norm, mid_prob, mid_pgrad]
        ins += [*near_squares, far_key, far_value, near_key, near_value]
        half = ((2 * rows, group * HDIM), jnp.bfloat16)
        *query_part, back, cross = call(
            bound(own_terms_kernel, near_span, first),
            [],
            ins + query_part,
            [wide_f32, half, half],
            group * 6 * pair_work,
            {len(ins): 0} if query_part else {},
        )
        back = shift(back, -mid_span)
        returned.append((back, swap(cross, "seq", near_span)))
        first += group
    (guest_part,) = guest_part
    guest_part = shift(guest_part, mid_span)
    query_sum, *self_terms = call(
        self_kernel,
        [],
        [query, grads, key, self_norm, self_prob, self_pgrad, *query_part],
        [wide_f32] * 3,
        heads * 3 * pair_work,
    )

    block = 2 * HDIM
    outputs = []
    first = 0
    for index, group in enumerate(GROUPS):
        start = first * HDIM
        place_of = start // block
        ins = [*self_terms, *returned[index]]
        outputs = call(
            bound(finish_kernel, start),
            [],
            ins,
            [wide_bf16] * 2,
            group * rows * HDIM * HDIM,
            {len(ins) + number: number for number in range(len(outputs))},
            grid=(group * HDIM // block,),
            streams=[(array, pl.BlockSpec(memory_space=pl.ANY)) for array in outputs],
            blocks=[pl.BlockSpec((rows, block), lambda i, j=place_of: (0, i + j))] * 2,
        )
        first += group
    (query_grad,) = call(
        finish_query_kernel,
        [],
        [query_sum, guest_part],
        [wide_bf16],
        heads * rows * HDIM,
        grid=(cols // block,),
        blocks=[pl.BlockSpec((rows, block), lambda i: (0, i))],
    )
    return query_grad, *outputs


def solution(mesh):
    return jax.shard_map(
        body,
        mesh=mesh,
        in_specs=(
            P("seq", "head"),
            P("seq", "head"),
            P("seq", "head"),
            P("seq", "head"),
            P("head", None),
            P("head", None),
            P("seq", None),
        ),
        out_specs=(P("seq", "head"), P("seq", "head"), P("seq", "head")),
        check_vma=False,
    )
```

```python
import math

import jax
import jax.numpy as jnp
from jax import lax
from jax.experimental import pallas as pl
from jax.experimental.pallas import tpu as pltpu
from jax.sharding import PartitionSpec as P


HDIM = 128
FAR, MID, NEAR = range(3)
SECTIONS = 3
GROUPS = (2, 4, 2)
HEADS_PER_STEP = 4
KERNEL_VMEM = 8 * 2**20
BIG = 1e30
SCALE = 1.0 / math.sqrt(HDIM)
LOG2E = math.log2(math.e)
EXP_SCALE = SCALE * LOG2E


def shift(value, steps):
    count = lax.axis_size("seq")
    low, high = max(0, -steps), min(count, count - steps)
    return lax.ppermute(value, "seq", [(src, src + steps) for src in range(low, high)])


def swap(value, axis, bit):
    pairs = [(src, src ^ bit) for src in range(lax.axis_size(axis))]
    return lax.ppermute(value, axis, pairs)


def dot(lhs, rhs, lhs_dim, rhs_dim):
    return lax.dot_general(
        lhs, rhs, (((lhs_dim,), (rhs_dim,)), ((), ())), preferred_element_type=jnp.float32
    )


def on_chip(array):
    return pltpu.with_memory_space_constraint(array, pltpu.VMEM)


def in_hbm(array):
    return pltpu.with_memory_space_constraint(array, pltpu.HBM)


def call(kernel, scalars, ins, outs, work, aliases=None, grid=None, streams=(), blocks=None, scratch=()):
    smem = pl.BlockSpec(memory_space=pltpu.SMEM)
    vmem = pl.BlockSpec(memory_space=pltpu.VMEM)
    return pl.pallas_call(
        kernel,
        grid=grid or (),
        in_specs=[smem] * len(scalars) + [vmem] * len(ins) + [spec for _, spec in streams],
        out_specs=blocks or [vmem] * len(outs),
        out_shape=[
            (jax.ShapeDtypeStruct if blocks else pltpu.VMEM)(shape, dtype)
            for shape, dtype in outs
        ],
        scratch_shapes=scratch,
        input_output_aliases=aliases or {},
        compiler_params=pltpu.CompilerParams(vmem_limit_bytes=KERNEL_VMEM),
        cost_estimate=pl.CostEstimate(
            flops=2 * work, bytes_accessed=0, transcendentals=work // HDIM
        ),
    )(*scalars, *[on_chip(array) for array in ins], *[array for array, _ in streams])


def each_head(first, count, step):
    width = math.gcd(count, HEADS_PER_STEP)

    def several(index, carry):
        for offset in range(width):
            step(first + index * width + offset)
        return carry

    lax.fori_loop(0, count // width, several, None)


def columns(head):
    return pl.ds(pl.multiple_of(head * HDIM, HDIM), HDIM)


def gathered_pieces(out_grad):
    pieces = {0: out_grad}
    bit = lax.axis_size("head") // 2
    while bit:
        for offset in list(pieces):
            pieces[offset | bit] = swap(pieces[offset], "head", bit)
        bit //= 2
    return [pieces[offset] for offset in range(len(pieces))]


def grad_kernel(*refs):
    head = lax.axis_index("head")
    *piece_refs, own_hbm, proj_hbm, out_ref, own_ref, proj, sems, own_sem = refs
    pieces = [own_ref, *piece_refs]
    width = own_ref.shape[1]
    count = sems.shape[0]
    block = proj.shape[0] // count
    own_copy = pltpu.make_async_copy(own_hbm, own_ref, own_sem)
    own_copy.start()
    copies = []
    for index in range(count):
        at = pl.ds(index * block, block)
        copies.append(pltpu.make_async_copy(proj_hbm.at[at], proj.at[at], sems.at[index]))
    for copy in copies[:2]:
        copy.start()
    own_copy.wait()
    for index, copy in enumerate(copies):
        copy.wait()
        if index + 2 < count:
            copies[index + 2].start()
        at = slice(index * block, (index + 1) * block)
        total = None
        for offset, piece in enumerate(pieces):
            start = pl.multiple_of((head ^ offset) * width, width)
            part = dot(piece[...], proj[at, pl.ds(start, width)], 1, 1)
            total = part if total is None else total + part
        out_ref[:, at] = total.astype(out_ref.dtype)


def attn_grad_of(out_grad, out_proj):
    pieces = gathered_pieces(out_grad)
    rows, width = out_grad.shape
    cols, features = out_proj.shape
    count = cols // (2 * HDIM)
    (result,) = call(
        grad_kernel,
        [],
        pieces[1:],
        [((rows, cols), jnp.bfloat16)],
        rows * cols * features,
        streams=[
            (in_hbm(array), pl.BlockSpec(memory_space=pltpu.HBM)) for array in (out_grad, out_proj)
        ],
        scratch=[
            pltpu.VMEM((rows, width), out_grad.dtype),
            pltpu.VMEM((cols, features), out_proj.dtype),
            pltpu.SemaphoreType.DMA((count,)),
            pltpu.SemaphoreType.DMA,
        ],
    )
    return result


def stage_kernel(*refs):
    count = len(refs) // 3
    sources, targets, sems = refs[:count], refs[count : 2 * count], refs[2 * count :]
    copies = [pltpu.make_async_copy(*each) for each in zip(sources, targets, sems)]
    for copy in copies:
        copy.start()
    for copy in copies:
        copy.wait()


def staged(*arrays):
    return pl.pallas_call(
        stage_kernel,
        in_specs=[pl.BlockSpec(memory_space=pltpu.HBM)] * len(arrays),
        out_specs=[pl.BlockSpec(memory_space=pltpu.VMEM)] * len(arrays),
        out_shape=[pltpu.VMEM(array.shape, array.dtype) for array in arrays],
        scratch_shapes=[pltpu.SemaphoreType.DMA] * len(arrays),
        compiler_params=pltpu.CompilerParams(vmem_limit_bytes=KERNEL_VMEM),
        cost_estimate=pl.CostEstimate(flops=10**6, bytes_accessed=0, transcendentals=0),
        name="stage",
    )(*[in_hbm(array) for array in arrays])


def causal(raw, fill):
    key_at = lax.broadcasted_iota(jnp.int32, raw.shape, 0)
    query_at = lax.broadcasted_iota(jnp.int32, raw.shape, 1)
    return jnp.where(key_at <= query_at, raw, fill)


class Flags:
    def __init__(self, spans, table_ref, active_ref):
        self.spans, self.table, self.active = spans, table_ref, active_ref
        self.place = lax.axis_index("seq")

    def usable(self, head, section):
        used = self.table[section, head] * self.active[0, section] > 0
        return used & (self.place >= self.spans[section])

    def bias(self, section, shape):
        head_at = lax.broadcasted_iota(jnp.int32, shape, 0)
        total = jnp.zeros(shape, jnp.float32)
        for head in range(shape[0]):
            value = jnp.where(self.usable(head, section), 0.0, -BIG)
            total = jnp.where(head_at == head, value, total)
        return total


def by_parity(near_span, run):
    odd = (lax.axis_index("seq") // near_span) % 2 == 1
    pl.when(odd)(lambda: run(True))
    pl.when(jnp.logical_not(odd))(lambda: run(False))


def soft_set(head, keys, query, probs, stats, base=0, diagonal=False):
    raw = dot(keys, query, 1, 1)
    if diagonal:
        raw = causal(raw, -BIG)
    top = jnp.max(raw, axis=0, keepdims=True)
    prob = jnp.exp2((raw - top) * EXP_SCALE)
    probs[head] = prob
    stats[base, pl.ds(head, 1), :] = top
    stats[base + 1, pl.ds(head, 1), :] = jnp.sum(prob, axis=0, keepdims=True)


def delta_set(head, values, grad, probs, pgrads, stats, base=0):
    pgrad = dot(values, grad, 1, 1)
    pgrads[head] = pgrad
    row = jnp.sum(probs[head] * pgrad, axis=0, keepdims=True)
    stats[base + 2, pl.ds(head, 1), :] = row


def soft_kernel(near_span, q, g, k, v, qf, k_up, k_x, *refs):
    own, mid, far, near, pr_own, pr_mid, pr_far, pr_near, pg_own = refs

    def run(odd):
        def step(head):
            at = columns(head)
            key_up, query, guest = k_up[:, at], q[:, at], qf[:, at]
            soft_set(head, k[:, at], query, pr_own, own, diagonal=True)
            delta_set(head, v[:, at], g[:, at], pr_own, pg_own, own)
            soft_set(head, key_up, query, pr_mid, mid)
            soft_set(head, key_up, guest, pr_far, far)
            soft_set(head, k_x[:, at], query if odd else guest, pr_near, near)

        each_head(0, pg_own.shape[0], step)

    by_parity(near_span, run)


def delta_mid_kernel(g, v_up, probs, soft, stats, pgrads):
    stats[0:2] = soft[0:2]

    def step(head):
        at = columns(head)
        delta_set(head, v_up[:, at], g[:, at], probs, pgrads, stats)

    each_head(0, probs.shape[0], step)


def delta_near_kernel(near_span, g, v_x, probs, soft, stats, pgrads):
    def run(odd):
        if odd:
            delta_mid_kernel(g, v_x, probs, soft, stats, pgrads)

    by_parity(near_span, run)


def delta_guest_kernel(near_span, gf, v_up, v_x, pr_far, far, pr_near, near, _, up, pg_far, pg_near):
    up[0:2] = far[0:2]
    up[3:5] = near[0:2]

    def run(odd):
        def step(head):
            at = columns(head)
            grad = gf[:, at]
            delta_set(head, v_up[:, at], grad, pr_far, pg_far, up)
            if not odd:
                delta_set(head, v_x[:, at], grad, pr_near, pg_near, up, 3)

        each_head(0, pr_far.shape[0], step)

    by_parity(near_span, run)


def merge(parts):
    top = parts[0][0]
    for part in parts[1:]:
        top = jnp.maximum(top, part[0])
    factors = [jnp.exp2((part[0] - top) * EXP_SCALE) for part in parts]
    norm, delta = 0.0, 0.0
    for part, factor in zip(parts, factors):
        norm = norm + factor * part[1]
        delta = delta + factor * part[2]
    return (top, norm, delta), factors


def part_of(ref, bias=0.0, base=0):
    return ref[base] + bias, ref[base + 1], ref[base + 2]


def put_norm(outs, factors, merged):
    inverse = 1.0 / merged[1]
    delta = merged[2] * inverse
    for out, factor in zip(outs, factors):
        out[0] = factor * inverse
        out[1] = delta


def bias_kernel(spans, t, a, out):
    flags = Flags(spans, t, a)
    for section in range(SECTIONS):
        out[section] = flags.bias(section, out.shape[1:])


def combine_local_kernel(near_span, bias, own, mid, near, out):
    def run(odd):
        near_bias = bias[NEAR]
        parts = [part_of(own), part_of(mid, bias[MID])]
        if odd:
            parts.append(part_of(near, near_bias))
            near_bias = jnp.full(near_bias.shape, -BIG, jnp.float32)
        merged, _ = merge(parts)
        for index, row in enumerate((*merged, bias[FAR], near_bias)):
            out[index] = row

    by_parity(near_span, run)


def combine_own_kernel(near_span, bias, own, mid, near, up, *outs):
    def run(odd):
        parts = [part_of(own), part_of(mid, bias[MID])]
        parts.append(part_of(near, bias[NEAR]) if odd else part_of(up, bias[NEAR], 3))
        parts.append(part_of(up, bias[FAR]))
        merged, factors = merge(parts)
        put_norm(outs if odd else outs[:2], factors, merged)

    by_parity(near_span, run)


def combine_guest_kernel(near_span, guest, up, far_out, near_out):
    def run(odd):
        parts = [part_of(up, guest[3])]
        if not odd:
            parts.append(part_of(up, guest[4], 3))
        parts.append(part_of(guest))
        merged, factors = merge(parts)
        put_norm((far_out, near_out), factors[:-1], merged)

    by_parity(near_span, run)


def pair_terms(head, query, grad, keys, probs, pgrads, norm):
    factor, delta = norm[0, pl.ds(head, 1), :], norm[1, pl.ds(head, 1), :]
    prob = probs[head] * factor
    weight = prob.astype(jnp.bfloat16)
    dlogit = (prob * (pgrads[head] - delta)).astype(jnp.bfloat16)
    return dot(keys, dlogit, 0, 0), dot(dlogit, query, 1, 0), dot(weight, grad, 1, 0)


def self_kernel(q, g, k, norm, probs, pgrads, dq_part, dq, dk, dv):
    def step(head):
        at = columns(head)
        query_term, dk[:, at], dv[:, at] = pair_terms(
            head, q[:, at], g[:, at], k[:, at], probs, pgrads, norm
        )
        dq[:, at] = query_term.T + dq_part[:, at]

    each_head(0, probs.shape[0], step)


def guest_terms_kernel(
    near_span, first, q, g, k_up, k_x, norm_far, norm_near, pr_far, pg_far, pr_near, pg_near, *refs
):
    dq, dk_far, dv_far, dk_near, dv_near = refs[-5:]

    def run(odd):
        def step(head):
            at, out = columns(head), columns(head - first)
            query, grad = q[:, at], g[:, at]
            query_term, dk_far[:, out], dv_far[:, out] = pair_terms(
                head, query, grad, k_up[:, at], pr_far, pg_far, norm_far
            )
            if not odd:
                more, dk_near[:, out], dv_near[:, out] = pair_terms(
                    head, query, grad, k_x[:, at], pr_near, pg_near, norm_near
                )
                query_term = query_term + more
            dq[:, at] = (query_term * SCALE).T.astype(dq.dtype)

        each_head(first, dk_far.shape[1] // HDIM, step)

    by_parity(near_span, run)


def own_terms_kernel(
    near_span, first, q, g, k_up, k_x, norm_mid, norm_near, pr_mid, pg_mid, pr_near, pg_near,
    dk_far, dv_far, dk_near, dv_near, *refs,
):
    dq, back, cross = refs[-3:]
    rows = q.shape[0]

    def run(odd):
        def step(head):
            at, out = columns(head), columns(head - first)
            query, grad = q[:, at], g[:, at]
            query_term, key_term, value_term = pair_terms(
                head, query, grad, k_up[:, at], pr_mid, pg_mid, norm_mid
            )
            back[:rows, out] = ((key_term + dk_far[:, out]) * SCALE).astype(back.dtype)
            back[rows:, out] = (value_term + dv_far[:, out]).astype(back.dtype)
            if odd:
                more, key_term, value_term = pair_terms(
                    head, query, grad, k_x[:, at], pr_near, pg_near, norm_near
                )
                query_term = query_term + more
            else:
                key_term, value_term = dk_near[:, out], dv_near[:, out]
            cross[:rows, out] = (key_term * SCALE).astype(cross.dtype)
            cross[rows:, out] = value_term.astype(cross.dtype)
            dq[:, at] = query_term.T

        each_head(first, cross.shape[1] // HDIM, step)

    by_parity(near_span, run)


def step_columns(block, first=0):
    return pl.ds(pl.multiple_of(pl.program_id(0) * block + first, block), block)


def finish_kernel(first, dk, dv, back, cross, *refs):
    key_out, value_out = refs[-2:]
    rows, block = key_out.shape
    here, at = step_columns(block), step_columns(block, first)
    for rows_at, total, out in (
        (slice(0, rows), dk[:, at] * SCALE, key_out),
        (slice(rows, 2 * rows), dv[:, at], value_out),
    ):
        for ref in (back, cross):
            total = total + ref[rows_at, here].astype(jnp.float32)
        out[...] = total.astype(out.dtype)


def finish_query_kernel(dq, guest, out):
    at = step_columns(out.shape[1])
    total = dq[:, at] * SCALE + guest[:, at].astype(jnp.float32)
    out[...] = total.astype(out.dtype)


def body(queries, key_rows, value_rows, out_grad, out_proj, section_table, block_active):
    seq_count = lax.axis_size("seq")
    spans = [seq_count // 2 ** (index + 1) for index in range(SECTIONS)]
    mid_span, near_span = spans[MID], spans[NEAR]
    assert spans[FAR] == 2 * mid_span and mid_span == 2 * near_span
    assert block_active.shape[0] == 1
    rows, cols = queries.shape
    heads = cols // HDIM
    assert heads == sum(GROUPS)
    pair_work = rows * rows * HDIM
    flags = [section_table.T, block_active]

    wide_f32 = ((rows, cols), jnp.float32)
    wide_bf16 = ((rows, cols), jnp.bfloat16)

    def table(count):
        return ((count, heads, rows), jnp.float32)

    stat, norm = table(3), table(2)
    square = ((heads, rows, rows), jnp.float32)
    row_work = heads * rows * HDIM

    def bound(kernel, *fixed):
        def run(*refs):
            kernel(*fixed, *refs)

        return run

    key_up = shift(key_rows, mid_span)
    value_up = shift(value_rows, mid_span)
    key_x = swap(key_rows, "seq", near_span)
    value_x = swap(value_rows, "seq", near_span)
    guest_query = shift(queries, -mid_span)
    grads = attn_grad_of(out_grad, out_proj)
    guest_grad = shift(grads, -mid_span)
    query, key, value = staged(queries, key_rows, value_rows)

    (bias,) = call(bound(bias_kernel, spans), flags, [], [stat], row_work)
    self_stats, mid_soft, far_soft, near_soft, *probs, self_pgrad = call(
        bound(soft_kernel, near_span),
        [],
        [query, grads, key, value, guest_query, key_up, key_x],
        [stat] * 4 + [square] * 5,
        heads * 5 * pair_work,
    )
    self_prob, mid_prob, far_prob, near_prob = probs

    def deltas(kernel, *ins):
        return call(kernel, [], ins, [stat, square], heads * pair_work)

    mid_stats, mid_pgrad = deltas(delta_mid_kernel, grads, value_up, mid_prob, mid_soft)
    near_stats, near_pgrad = deltas(
        bound(delta_near_kernel, near_span), grads, value_x, near_prob, near_soft
    )
    (merged,) = call(
        bound(combine_local_kernel, near_span),
        [],
        [bias, self_stats, mid_stats, near_stats],
        [table(5)],
        row_work,
    )
    guest_stats = shift(merged, -mid_span)
    ins = [guest_grad, value_up, value_x, far_prob, far_soft, near_prob, near_soft, near_pgrad]
    up_part, far_pgrad, near_pgrad = call(
        bound(delta_guest_kernel, near_span),
        [],
        ins,
        [table(6), square, square],
        heads * 2 * pair_work,
        {len(ins) - 1: 2},
    )
    up_stats = shift(up_part, mid_span)
    far_norm, near_norm_guest = call(
        bound(combine_guest_kernel, near_span), [], [guest_stats, up_part], [norm] * 2, row_work
    )
    near_squares = [near_prob, near_pgrad]
    self_norm, mid_norm, near_norm = call(
        bound(combine_own_kernel, near_span),
        [],
        [bias, self_stats, mid_stats, near_stats, up_stats],
        [norm] * 3,
        row_work,
    )
    guest_part, query_part, returned = [], [], []
    first = 0
    for group in GROUPS:
        narrow = (rows, group * HDIM)
        ins = [guest_query, guest_grad, key_up, key_x, far_norm, near_norm_guest]
        ins += [far_prob, far_pgrad, *near_squares]
        *guest_part, far_key, far_value, near_key, near_value = call(
            bound(guest_terms_kernel, near_span, first),
            [],
            ins + guest_part,
            [wide_bf16] + [(narrow, jnp.float32)] * 4,
            group * 6 * pair_work,
            {len(ins): 0} if guest_part else {},
        )
        ins = [query, grads, key_up, key_x, mid_norm, near_norm, mid_prob, mid_pgrad]
        ins += [*near_squares, far_key, far_value, near_key, near_value]
        half = ((2 * rows, group * HDIM), jnp.bfloat16)
        *query_part, back, cross = call(
            bound(own_terms_kernel, near_span, first),
            [],
            ins + query_part,
            [wide_f32, half, half],
            group * 6 * pair_work,
            {len(ins): 0} if query_part else {},
        )
        back = shift(back, -mid_span)
        returned.append((back, swap(cross, "seq", near_span)))
        first += group
    (guest_part,) = guest_part
    guest_part = shift(guest_part, mid_span)
    query_sum, *self_terms = call(
        self_kernel,
        [],
        [query, grads, key, self_norm, self_prob, self_pgrad, *query_part],
        [wide_f32] * 3,
        heads * 3 * pair_work,
    )

    block = 2 * HDIM
    outputs = []
    first = 0
    for index, group in enumerate(GROUPS):
        start = first * HDIM
        place_of = start // block
        ins = [*self_terms, *returned[index]]
        outputs = call(
            bound(finish_kernel, start),
            [],
            ins,
            [wide_bf16] * 2,
            group * rows * HDIM * HDIM,
            {len(ins) + number: number for number in range(len(outputs))},
            grid=(group * HDIM // block,),
            streams=[(array, pl.BlockSpec(memory_space=pl.ANY)) for array in outputs],
            blocks=[pl.BlockSpec((rows, block), lambda i, j=place_of: (0, i + j))] * 2,
        )
        first += group
    (query_grad,) = call(
        finish_query_kernel,
        [],
        [query_sum, guest_part],
        [wide_bf16],
        heads * rows * HDIM,
        grid=(cols // block,),
        blocks=[pl.BlockSpec((rows, block), lambda i: (0, i))],
    )
    return query_grad, *outputs


def solution(mesh):
    return jax.shard_map(
        body,
        mesh=mesh,
        in_specs=(
            P("seq", "head"),
            P("seq", "head"),
            P("seq", "head"),
            P("seq", "head"),
            P("head", None),
            P("head", None),
            P("seq", None),
        ),
        out_specs=(P("seq", "head"), P("seq", "head"), P("seq", "head")),
        check_vma=False,
    )
```

```python
import math

import jax
import jax.numpy as jnp
from jax import lax
from jax.experimental import pallas as pl
from jax.experimental.pallas import tpu as pltpu
from jax.sharding import PartitionSpec as P


HDIM = 128
FAR, MID, NEAR = range(3)
SECTIONS = 3
GROUPS = (2, 4, 2)
HEADS_PER_STEP = 4
KERNEL_VMEM = 8 * 2**20
BIG = 1e30
SCALE = 1.0 / math.sqrt(HDIM)
LOG2E = math.log2(math.e)
EXP_SCALE = SCALE * LOG2E


def shift(value, steps):
    count = lax.axis_size("seq")
    low, high = max(0, -steps), min(count, count - steps)
    return lax.ppermute(value, "seq", [(src, src + steps) for src in range(low, high)])


def swap(value, axis, bit):
    pairs = [(src, src ^ bit) for src in range(lax.axis_size(axis))]
    return lax.ppermute(value, axis, pairs)


def dot(lhs, rhs, lhs_dim, rhs_dim):
    return lax.dot_general(
        lhs, rhs, (((lhs_dim,), (rhs_dim,)), ((), ())), preferred_element_type=jnp.float32
    )


def on_chip(array):
    return pltpu.with_memory_space_constraint(array, pltpu.VMEM)


def in_hbm(array):
    return pltpu.with_memory_space_constraint(array, pltpu.HBM)


def call(kernel, scalars, ins, outs, work, aliases=None, grid=None, streams=(), blocks=None, scratch=()):
    smem = pl.BlockSpec(memory_space=pltpu.SMEM)
    vmem = pl.BlockSpec(memory_space=pltpu.VMEM)
    return pl.pallas_call(
        kernel,
        grid=grid or (),
        in_specs=[smem] * len(scalars) + [vmem] * len(ins) + [spec for _, spec in streams],
        out_specs=blocks or [vmem] * len(outs),
        out_shape=[
            (jax.ShapeDtypeStruct if blocks else pltpu.VMEM)(shape, dtype)
            for shape, dtype in outs
        ],
        scratch_shapes=scratch,
        input_output_aliases=aliases or {},
        compiler_params=pltpu.CompilerParams(vmem_limit_bytes=KERNEL_VMEM),
        cost_estimate=pl.CostEstimate(
            flops=2 * work, bytes_accessed=0, transcendentals=work // HDIM
        ),
    )(*scalars, *[on_chip(array) for array in ins], *[array for array, _ in streams])


def each_head(first, count, step):
    width = math.gcd(count, HEADS_PER_STEP)

    def several(index, carry):
        for offset in range(width):
            step(first + index * width + offset)
        return carry

    lax.fori_loop(0, count // width, several, None)


def columns(head):
    return pl.ds(pl.multiple_of(head * HDIM, HDIM), HDIM)


def gathered_pieces(out_grad):
    pieces = {0: out_grad}
    bit = lax.axis_size("head") // 2
    while bit:
        for offset in list(pieces):
            pieces[offset | bit] = swap(pieces[offset], "head", bit)
        bit //= 2
    return [pieces[offset] for offset in range(len(pieces))]


def grad_kernel(*refs):
    head = lax.axis_index("head")
    *piece_refs, own_hbm, proj_hbm, out_ref, own_ref, proj, sems, own_sem = refs
    pieces = [own_ref, *piece_refs]
    width = own_ref.shape[1]
    count = sems.shape[0]
    block = proj.shape[0] // count
    own_copy = pltpu.make_async_copy(own_hbm, own_ref, own_sem)
    own_copy.start()
    copies = []
    for index in range(count):
        at = pl.ds(index * block, block)
        copies.append(pltpu.make_async_copy(proj_hbm.at[at], proj.at[at], sems.at[index]))
    for copy in copies[:2]:
        copy.start()
    own_copy.wait()
    for index, copy in enumerate(copies):
        copy.wait()
        if index + 2 < count:
            copies[index + 2].start()
        at = slice(index * block, (index + 1) * block)
        total = None
        for offset, piece in enumerate(pieces):
            start = pl.multiple_of((head ^ offset) * width, width)
            part = dot(piece[...], proj[at, pl.ds(start, width)], 1, 1)
            total = part if total is None else total + part
        out_ref[:, at] = total.astype(out_ref.dtype)


def attn_grad_of(out_grad, out_proj):
    pieces = gathered_pieces(out_grad)
    rows, width = out_grad.shape
    cols, features = out_proj.shape
    count = cols // (2 * HDIM)
    (result,) = call(
        grad_kernel,
        [],
        pieces[1:],
        [((rows, cols), jnp.bfloat16)],
        rows * cols * features,
        streams=[
            (in_hbm(array), pl.BlockSpec(memory_space=pltpu.HBM)) for array in (out_grad, out_proj)
        ],
        scratch=[
            pltpu.VMEM((rows, width), out_grad.dtype),
            pltpu.VMEM((cols, features), out_proj.dtype),
            pltpu.SemaphoreType.DMA((count,)),
            pltpu.SemaphoreType.DMA,
        ],
    )
    return result


def stage_kernel(*refs):
    count = len(refs) // 3
    sources, targets, sems = refs[:count], refs[count : 2 * count], refs[2 * count :]
    copies = [pltpu.make_async_copy(*each) for each in zip(sources, targets, sems)]
    for copy in copies:
        copy.start()
    for copy in copies:
        copy.wait()


def staged(*arrays):
    return pl.pallas_call(
        stage_kernel,
        in_specs=[pl.BlockSpec(memory_space=pltpu.HBM)] * len(arrays),
        out_specs=[pl.BlockSpec(memory_space=pltpu.VMEM)] * len(arrays),
        out_shape=[pltpu.VMEM(array.shape, array.dtype) for array in arrays],
        scratch_shapes=[pltpu.SemaphoreType.DMA] * len(arrays),
        compiler_params=pltpu.CompilerParams(vmem_limit_bytes=KERNEL_VMEM),
        cost_estimate=pl.CostEstimate(flops=10**6, bytes_accessed=0, transcendentals=0),
        name="stage",
    )(*[in_hbm(array) for array in arrays])


def causal(raw, fill):
    key_at = lax.broadcasted_iota(jnp.int32, raw.shape, 0)
    query_at = lax.broadcasted_iota(jnp.int32, raw.shape, 1)
    return jnp.where(key_at <= query_at, raw, fill)


class Flags:
    def __init__(self, spans, table_ref, active_ref):
        self.spans, self.table, self.active = spans, table_ref, active_ref
        self.place = lax.axis_index("seq")

    def usable(self, head, section):
        used = self.table[section, head] * self.active[0, section] > 0
        return used & (self.place >= self.spans[section])

    def bias(self, section, shape):
        head_at = lax.broadcasted_iota(jnp.int32, shape, 0)
        total = jnp.zeros(shape, jnp.float32)
        for head in range(shape[0]):
            value = jnp.where(self.usable(head, section), 0.0, -BIG)
            total = jnp.where(head_at == head, value, total)
        return total


def by_parity(near_span, run):
    odd = (lax.axis_index("seq") // near_span) % 2 == 1
    pl.when(odd)(lambda: run(True))
    pl.when(jnp.logical_not(odd))(lambda: run(False))


def soft_set(head, keys, query, probs, stats, base=0, diagonal=False):
    raw = dot(keys, query, 1, 1)
    if diagonal:
        raw = causal(raw, -BIG)
    top = jnp.max(raw, axis=0, keepdims=True)
    prob = jnp.exp2((raw - top) * EXP_SCALE)
    probs[head] = prob
    stats[base, pl.ds(head, 1), :] = top
    stats[base + 1, pl.ds(head, 1), :] = jnp.sum(prob, axis=0, keepdims=True)


def delta_set(head, values, grad, probs, pgrads, stats, base=0):
    pgrad = dot(values, grad, 1, 1)
    pgrads[head] = pgrad
    row = jnp.sum(probs[head] * pgrad, axis=0, keepdims=True)
    stats[base + 2, pl.ds(head, 1), :] = row


def soft_kernel(near_span, q, g, k, v, qf, k_up, k_x, *refs):
    own, mid, far, near, pr_own, pr_mid, pr_far, pr_near, pg_own = refs

    def run(odd):
        def step(head):
            at = columns(head)
            key_up, query, guest = k_up[:, at], q[:, at], qf[:, at]
            soft_set(head, k[:, at], query, pr_own, own, diagonal=True)
            delta_set(head, v[:, at], g[:, at], pr_own, pg_own, own)
            soft_set(head, k[:, at], guest, pr_mid, mid)
            soft_set(head, key_up, guest, pr_far, far)
            soft_set(head, k_x[:, at], query if odd else guest, pr_near, near)

        each_head(0, pg_own.shape[0], step)

    by_parity(near_span, run)


def delta_kernel(g, values, probs, soft, stats, pgrads):
    stats[0:2] = soft[0:2]

    def step(head):
        at = columns(head)
        delta_set(head, values[:, at], g[:, at], probs, pgrads, stats)

    each_head(0, probs.shape[0], step)


def delta_near_kernel(near_span, g, v_x, probs, soft, stats, pgrads):
    def run(odd):
        if odd:
            delta_kernel(g, v_x, probs, soft, stats, pgrads)

    by_parity(near_span, run)


def delta_guest_kernel(
    near_span, gf, v, v_x, pr_mid, mid_soft, pr_near, near_soft, _stats, _pgrads,
    mid, pg_mid, near, pg_near,
):
    delta_kernel(gf, v, pr_mid, mid_soft, mid, pg_mid)

    def run(odd):
        if not odd:
            delta_kernel(gf, v_x, pr_near, near_soft, near, pg_near)

    by_parity(near_span, run)


def merge(parts):
    top = parts[0][0]
    for part in parts[1:]:
        top = jnp.maximum(top, part[0])
    factors = [jnp.exp2((part[0] - top) * EXP_SCALE) for part in parts]
    norm, delta = 0.0, 0.0
    for part, factor in zip(parts, factors):
        norm = norm + factor * part[1]
        delta = delta + factor * part[2]
    return (top, norm, delta), factors


def part_of(ref, bias=0.0, base=0):
    return ref[base] + bias, ref[base + 1], ref[base + 2]


def put_norm(outs, factors, merged):
    inverse = 1.0 / merged[1]
    delta = merged[2] * inverse
    for out, factor in zip(outs, factors):
        out[0] = factor * inverse
        out[1] = delta


def bias_kernel(spans, t, a, out):
    flags = Flags(spans, t, a)
    for section in range(SECTIONS):
        out[section] = flags.bias(section, out.shape[1:])


def combine_local_kernel(near_span, bias, own, near, out):
    out[3:6] = bias[0:3]

    def run(odd):
        parts = [part_of(own)]
        if odd:
            parts.append(part_of(near, bias[NEAR]))
        merged, _ = merge(parts)
        for index, row in enumerate(merged):
            out[index] = row

    by_parity(near_span, run)


def combine_guest_kernel(near_span, guest, far, mid, near, up, *outs):
    def run(odd):
        parts = [part_of(far, guest[3 + FAR]), part_of(mid, guest[3 + MID])]
        if not odd:
            parts.append(part_of(near, guest[3 + NEAR]))
        merged, _ = merge(parts)
        for index, row in enumerate(merged):
            up[index] = row
        merged, factors = merge([*parts, part_of(guest)])
        put_norm(outs, factors[:-1], merged)

    by_parity(near_span, run)


def combine_own_kernel(spans, bias, own, near, up, *outs):
    held = lax.axis_index("seq") >= spans[MID]

    def run(odd):
        parts = [part_of(own), part_of(up, jnp.where(held, 0.0, -BIG))]
        if odd:
            parts.insert(1, part_of(near, bias[NEAR]))
        merged, factors = merge(parts)
        put_norm(outs, factors[:-1], merged)

    by_parity(spans[NEAR], run)


def pair_terms(head, query, grad, keys, probs, pgrads, norm):
    factor, delta = norm[0, pl.ds(head, 1), :], norm[1, pl.ds(head, 1), :]
    prob = probs[head] * factor
    weight = prob.astype(jnp.bfloat16)
    dlogit = (prob * (pgrads[head] - delta)).astype(jnp.bfloat16)
    return dot(keys, dlogit, 0, 0), dot(dlogit, query, 1, 0), dot(weight, grad, 1, 0)


def self_kernel(q, g, k, norm, probs, pgrads, dq_part, dq, dk, dv):
    def step(head):
        at = columns(head)
        query_term, dk[:, at], dv[:, at] = pair_terms(
            head, q[:, at], g[:, at], k[:, at], probs, pgrads, norm
        )
        dq[:, at] = query_term.T + dq_part[:, at]

    each_head(0, probs.shape[0], step)


def guest_terms_kernel(
    near_span, first, q, g, k, k_up, k_x, norm_far, norm_mid, norm_near,
    pr_far, pg_far, pr_mid, pg_mid, pr_near, pg_near, *refs,
):
    dq, back, dk_mid, dv_mid, dk_near, dv_near = refs[-6:]
    rows = q.shape[0]

    def run(odd):
        def step(head):
            at, out = columns(head), columns(head - first)
            query, grad = q[:, at], g[:, at]
            query_term, key_term, value_term = pair_terms(
                head, query, grad, k_up[:, at], pr_far, pg_far, norm_far
            )
            back[:rows, out] = (key_term * SCALE).astype(back.dtype)
            back[rows:, out] = value_term.astype(back.dtype)
            more, dk_mid[:, out], dv_mid[:, out] = pair_terms(
                head, query, grad, k[:, at], pr_mid, pg_mid, norm_mid
            )
            query_term = query_term + more
            if not odd:
                more, dk_near[:, out], dv_near[:, out] = pair_terms(
                    head, query, grad, k_x[:, at], pr_near, pg_near, norm_near
                )
                query_term = query_term + more
            dq[:, at] = (query_term * SCALE).T.astype(dq.dtype)

        each_head(first, back.shape[1] // HDIM, step)

    by_parity(near_span, run)


def own_terms_kernel(
    near_span, first, q, g, k_x, norm_near, pr_near, pg_near, dk_near, dv_near, *refs
):
    dq, cross = refs[-2:]
    rows = q.shape[0]

    def run(odd):
        def step(head):
            at, out = columns(head), columns(head - first)
            if odd:
                query_term, key_term, value_term = pair_terms(
                    head, q[:, at], g[:, at], k_x[:, at], pr_near, pg_near, norm_near
                )
                dq[:, at] = query_term.T
            else:
                key_term, value_term = dk_near[:, out], dv_near[:, out]
                dq[:, at] = jnp.zeros_like(key_term)
            cross[:rows, out] = (key_term * SCALE).astype(cross.dtype)
            cross[rows:, out] = value_term.astype(cross.dtype)

        each_head(first, cross.shape[1] // HDIM, step)

    by_parity(near_span, run)


def step_columns(block, first=0):
    return pl.ds(pl.multiple_of(pl.program_id(0) * block + first, block), block)


def finish_kernel(first, dk, dv, dk_mid, dv_mid, back, cross, *refs):
    key_out, value_out = refs[-2:]
    rows, block = key_out.shape
    here, at = step_columns(block), step_columns(block, first)
    for rows_at, total, out in (
        (slice(0, rows), (dk[:, at] + dk_mid[:, here]) * SCALE, key_out),
        (slice(rows, 2 * rows), dv[:, at] + dv_mid[:, here], value_out),
    ):
        for ref in (back, cross):
            total = total + ref[rows_at, here].astype(jnp.float32)
        out[...] = total.astype(out.dtype)


def finish_query_kernel(dq, guest, out):
    at = step_columns(out.shape[1])
    total = dq[:, at] * SCALE + guest[:, at].astype(jnp.float32)
    out[...] = total.astype(out.dtype)


def body(queries, key_rows, value_rows, out_grad, out_proj, section_table, block_active):
    seq_count = lax.axis_size("seq")
    spans = [seq_count // 2 ** (index + 1) for index in range(SECTIONS)]
    mid_span, near_span = spans[MID], spans[NEAR]
    assert spans[FAR] == 2 * mid_span and mid_span == 2 * near_span
    assert block_active.shape[0] == 1
    rows, cols = queries.shape
    heads = cols // HDIM
    assert heads == sum(GROUPS)
    pair_work = rows * rows * HDIM
    flags = [section_table.T, block_active]

    wide_f32 = ((rows, cols), jnp.float32)
    wide_bf16 = ((rows, cols), jnp.bfloat16)

    def table(count):
        return ((count, heads, rows), jnp.float32)

    stat, norm = table(3), table(2)
    square = ((heads, rows, rows), jnp.float32)
    row_work = heads * rows * HDIM

    def bound(kernel, *fixed):
        def run(*refs):
            kernel(*fixed, *refs)

        return run

    key_up = shift(key_rows, mid_span)
    value_up = shift(value_rows, mid_span)
    key_x = swap(key_rows, "seq", near_span)
    value_x = swap(value_rows, "seq", near_span)
    guest_query = shift(queries, -mid_span)
    grads = attn_grad_of(out_grad, out_proj)
    guest_grad = shift(grads, -mid_span)
    query, key, value = staged(queries, key_rows, value_rows)

    (bias,) = call(bound(bias_kernel, spans), flags, [], [stat], row_work)
    self_stats, mid_soft, far_soft, near_soft, *probs, self_pgrad = call(
        bound(soft_kernel, near_span),
        [],
        [query, grads, key, value, guest_query, key_up, key_x],
        [stat] * 4 + [square] * 5,
        heads * 5 * pair_work,
    )
    self_prob, mid_prob, far_prob, near_prob = probs

    near_stats, near_pgrad = call(
        bound(delta_near_kernel, near_span),
        [],
        [grads, value_x, near_prob, near_soft],
        [stat, square],
        heads * pair_work,
    )
    (merged,) = call(
        bound(combine_local_kernel, near_span),
        [],
        [bias, self_stats, near_stats],
        [table(6)],
        row_work,
    )
    guest_stats = shift(merged, -mid_span)
    ins = [guest_grad, value, value_x, mid_prob, mid_soft, near_prob, near_soft]
    mid_stats, mid_pgrad, near_stats, near_pgrad = call(
        bound(delta_guest_kernel, near_span),
        [],
        [*ins, near_stats, near_pgrad],
        [stat, square] * 2,
        heads * 2 * pair_work,
        {len(ins): 2, len(ins) + 1: 3},
    )
    far_stats, far_pgrad = call(
        delta_kernel,
        [],
        [guest_grad, value_up, far_prob, far_soft],
        [stat, square],
        heads * pair_work,
    )
    up_part, *guest_norms = call(
        bound(combine_guest_kernel, near_span),
        [],
        [guest_stats, far_stats, mid_stats, near_stats],
        [stat] + [norm] * 3,
        row_work,
    )
    up_stats = shift(up_part, mid_span)
    self_norm, near_norm = call(
        bound(combine_own_kernel, spans),
        [],
        [bias, self_stats, near_stats, up_stats],
        [norm] * 2,
        row_work,
    )
    near_squares = [near_prob, near_pgrad]
    guest_part, query_part, returned = [], [], []
    first = 0
    for group in GROUPS:
        narrow = ((rows, group * HDIM), jnp.float32)
        half = ((2 * rows, group * HDIM), jnp.bfloat16)
        ins = [guest_query, guest_grad, key, key_up, key_x, *guest_norms]
        ins += [far_prob, far_pgrad, mid_prob, mid_pgrad, *near_squares]
        *guest_part, back, mid_key, mid_value, near_key, near_value = call(
            bound(guest_terms_kernel, near_span, first),
            [],
            ins + guest_part,
            [wide_bf16, half] + [narrow] * 4,
            group * 9 * pair_work,
            {len(ins): 0} if guest_part else {},
        )
        ins = [query, grads, key_x, near_norm, *near_squares, near_key, near_value]
        *query_part, cross = call(
            bound(own_terms_kernel, near_span, first),
            [],
            ins + query_part,
            [wide_f32, half],
            group * 3 * pair_work,
            {len(ins): 0} if query_part else {},
        )
        back = shift(back, -mid_span)
        cross = swap(cross, "seq", near_span)
        returned.append((mid_key, mid_value, back, cross))
        first += group
    (guest_part,) = guest_part
    guest_part = shift(guest_part, mid_span)
    query_sum, *self_terms = call(
        self_kernel,
        [],
        [query, grads, key, self_norm, self_prob, self_pgrad, *query_part],
        [wide_f32] * 3,
        heads * 3 * pair_work,
    )

    block = 2 * HDIM
    outputs = []
    first = 0
    for index, group in enumerate(GROUPS):
        start = first * HDIM
        place_of = start // block
        ins = [*self_terms, *returned[index]]
        outputs = call(
            bound(finish_kernel, start),
            [],
            ins,
            [wide_bf16] * 2,
            group * rows * HDIM * HDIM,
            {len(ins) + number: number for number in range(len(outputs))},
            grid=(group * HDIM // block,),
            streams=[(array, pl.BlockSpec(memory_space=pl.ANY)) for array in outputs],
            blocks=[pl.BlockSpec((rows, block), lambda i, j=place_of: (0, i + j))] * 2,
        )
        first += group
    (query_grad,) = call(
        finish_query_kernel,
        [],
        [query_sum, guest_part],
        [wide_bf16],
        heads * rows * HDIM,
        grid=(cols // block,),
        blocks=[pl.BlockSpec((rows, block), lambda i: (0, i))],
    )
    return query_grad, *outputs


def solution(mesh):
    return jax.shard_map(
        body,
        mesh=mesh,
        in_specs=(
            P("seq", "head"),
            P("seq", "head"),
            P("seq", "head"),
            P("seq", "head"),
            P("head", None),
            P("head", None),
            P("seq", None),
        ),
        out_specs=(P("seq", "head"), P("seq", "head"), P("seq", "head")),
        check_vma=False,
    )
```

```python
import math

import jax
import jax.numpy as jnp
from jax import lax
from jax.experimental import pallas as pl
from jax.experimental.pallas import tpu as pltpu
from jax.sharding import PartitionSpec as P


HDIM = 128
FAR, MID, NEAR = range(3)
SECTIONS = 3
GROUPS = (2, 4, 2)
HEADS_PER_STEP = 4
KERNEL_VMEM = 8 * 2**20
BIG = 1e30
SCALE = 1.0 / math.sqrt(HDIM)
LOG2E = math.log2(math.e)
EXP_SCALE = SCALE * LOG2E


def shift(value, steps):
    count = lax.axis_size("seq")
    low, high = max(0, -steps), min(count, count - steps)
    return lax.ppermute(value, "seq", [(src, src + steps) for src in range(low, high)])


def swap(value, axis, bit):
    pairs = [(src, src ^ bit) for src in range(lax.axis_size(axis))]
    return lax.ppermute(value, axis, pairs)


def dot(lhs, rhs, lhs_dim, rhs_dim):
    return lax.dot_general(
        lhs, rhs, (((lhs_dim,), (rhs_dim,)), ((), ())), preferred_element_type=jnp.float32
    )


def on_chip(array):
    return pltpu.with_memory_space_constraint(array, pltpu.VMEM)


def in_hbm(array):
    return pltpu.with_memory_space_constraint(array, pltpu.HBM)


def call(kernel, scalars, ins, outs, work, aliases=None, grid=None, streams=(), blocks=None, scratch=()):
    smem = pl.BlockSpec(memory_space=pltpu.SMEM)
    vmem = pl.BlockSpec(memory_space=pltpu.VMEM)
    return pl.pallas_call(
        kernel,
        grid=grid or (),
        in_specs=[smem] * len(scalars) + [vmem] * len(ins) + [spec for _, spec in streams],
        out_specs=blocks or [vmem] * len(outs),
        out_shape=[
            (jax.ShapeDtypeStruct if blocks else pltpu.VMEM)(shape, dtype)
            for shape, dtype in outs
        ],
        scratch_shapes=scratch,
        input_output_aliases=aliases or {},
        compiler_params=pltpu.CompilerParams(vmem_limit_bytes=KERNEL_VMEM),
        cost_estimate=pl.CostEstimate(
            flops=2 * work, bytes_accessed=0, transcendentals=work // HDIM
        ),
    )(*scalars, *[on_chip(array) for array in ins], *[array for array, _ in streams])


def each_head(first, count, step):
    width = math.gcd(count, HEADS_PER_STEP)

    def several(index, carry):
        for offset in range(width):
            step(first + index * width + offset)
        return carry

    lax.fori_loop(0, count // width, several, None)


def columns(head):
    return pl.ds(pl.multiple_of(head * HDIM, HDIM), HDIM)


def gathered_pieces(out_grad):
    pieces = {0: out_grad}
    bit = lax.axis_size("head") // 2
    while bit:
        for offset in list(pieces):
            pieces[offset | bit] = swap(pieces[offset], "head", bit)
        bit //= 2
    return [pieces[offset] for offset in range(len(pieces))]


def grad_kernel(*refs):
    head = lax.axis_index("head")
    *piece_refs, own_hbm, proj_hbm, out_ref, own_ref, proj, sems, own_sem = refs
    pieces = [own_ref, *piece_refs]
    width = own_ref.shape[1]
    count = sems.shape[0]
    block = proj.shape[0] // count
    own_copy = pltpu.make_async_copy(own_hbm, own_ref, own_sem)
    own_copy.start()
    copies = []
    for index in range(count):
        at = pl.ds(index * block, block)
        copies.append(pltpu.make_async_copy(proj_hbm.at[at], proj.at[at], sems.at[index]))
    for copy in copies[:2]:
        copy.start()
    own_copy.wait()
    for index, copy in enumerate(copies):
        copy.wait()
        if index + 2 < count:
            copies[index + 2].start()
        at = slice(index * block, (index + 1) * block)
        total = None
        for offset, piece in enumerate(pieces):
            start = pl.multiple_of((head ^ offset) * width, width)
            part = dot(piece[...], proj[at, pl.ds(start, width)], 1, 1)
            total = part if total is None else total + part
        out_ref[:, at] = total.astype(out_ref.dtype)


def attn_grad_of(out_grad, out_proj):
    pieces = gathered_pieces(out_grad)
    rows, width = out_grad.shape
    cols, features = out_proj.shape
    count = cols // (2 * HDIM)
    (result,) = call(
        grad_kernel,
        [],
        pieces[1:],
        [((rows, cols), jnp.bfloat16)],
        rows * cols * features,
        streams=[
            (in_hbm(array), pl.BlockSpec(memory_space=pltpu.HBM)) for array in (out_grad, out_proj)
        ],
        scratch=[
            pltpu.VMEM((rows, width), out_grad.dtype),
            pltpu.VMEM((cols, features), out_proj.dtype),
            pltpu.SemaphoreType.DMA((count,)),
            pltpu.SemaphoreType.DMA,
        ],
    )
    return result


def stage_kernel(*refs):
    count = len(refs) // 3
    sources, targets, sems = refs[:count], refs[count : 2 * count], refs[2 * count :]
    copies = [pltpu.make_async_copy(*each) for each in zip(sources, targets, sems)]
    for copy in copies:
        copy.start()
    for copy in copies:
        copy.wait()


def staged(*arrays):
    return pl.pallas_call(
        stage_kernel,
        in_specs=[pl.BlockSpec(memory_space=pltpu.HBM)] * len(arrays),
        out_specs=[pl.BlockSpec(memory_space=pltpu.VMEM)] * len(arrays),
        out_shape=[pltpu.VMEM(array.shape, array.dtype) for array in arrays],
        scratch_shapes=[pltpu.SemaphoreType.DMA] * len(arrays),
        compiler_params=pltpu.CompilerParams(vmem_limit_bytes=KERNEL_VMEM),
        cost_estimate=pl.CostEstimate(flops=10**6, bytes_accessed=0, transcendentals=0),
        name="stage",
    )(*[in_hbm(array) for array in arrays])


def causal(raw, fill):
    key_at = lax.broadcasted_iota(jnp.int32, raw.shape, 0)
    query_at = lax.broadcasted_iota(jnp.int32, raw.shape, 1)
    return jnp.where(key_at <= query_at, raw, fill)


class Flags:
    def __init__(self, spans, table_ref, active_ref):
        self.spans, self.table, self.active = spans, table_ref, active_ref
        self.place = lax.axis_index("seq")

    def usable(self, head, section):
        used = self.table[section, head] * self.active[0, section] > 0
        return used & (self.place >= self.spans[section])

    def bias(self, section, shape):
        head_at = lax.broadcasted_iota(jnp.int32, shape, 0)
        total = jnp.zeros(shape, jnp.float32)
        for head in range(shape[0]):
            value = jnp.where(self.usable(head, section), 0.0, -BIG)
            total = jnp.where(head_at == head, value, total)
        return total


def by_parity(near_span, run):
    odd = (lax.axis_index("seq") // near_span) % 2 == 1
    pl.when(odd)(lambda: run(True))
    pl.when(jnp.logical_not(odd))(lambda: run(False))


def soft_set(head, keys, query, probs, stats, base=0, diagonal=False):
    raw = dot(keys, query, 1, 1)
    if diagonal:
        raw = causal(raw, -BIG)
    top = jnp.max(raw, axis=0, keepdims=True)
    prob = jnp.exp2((raw - top) * EXP_SCALE)
    probs[head] = prob
    stats[base, pl.ds(head, 1), :] = top
    stats[base + 1, pl.ds(head, 1), :] = jnp.sum(prob, axis=0, keepdims=True)


def delta_set(head, values, grad, probs, pgrads, stats, base=0):
    pgrad = dot(values, grad, 1, 1)
    pgrads[head] = pgrad
    row = jnp.sum(probs[head] * pgrad, axis=0, keepdims=True)
    stats[base + 2, pl.ds(head, 1), :] = row


def soft_kernel(near_span, q, g, k, v, qf, k_up, k_x, *refs):
    own, mid, far, near, pr_own, pr_mid, pr_far, pr_near, pg_own = refs

    def run(odd):
        def step(head):
            at = columns(head)
            key_up, query, guest = k_up[:, at], q[:, at], qf[:, at]
            soft_set(head, k[:, at], query, pr_own, own, diagonal=True)
            delta_set(head, v[:, at], g[:, at], pr_own, pg_own, own)
            soft_set(head, k[:, at], guest, pr_mid, mid)
            soft_set(head, key_up, guest, pr_far, far)
            soft_set(head, k_x[:, at], query if odd else guest, pr_near, near)

        each_head(0, pg_own.shape[0], step)

    by_parity(near_span, run)


def delta_kernel(g, values, probs, soft, stats, pgrads):
    stats[0:2] = soft[0:2]

    def step(head):
        at = columns(head)
        delta_set(head, values[:, at], g[:, at], probs, pgrads, stats)

    each_head(0, probs.shape[0], step)


def delta_near_kernel(near_span, g, v_x, probs, soft, stats, pgrads):
    def run(odd):
        if odd:
            delta_kernel(g, v_x, probs, soft, stats, pgrads)

    by_parity(near_span, run)


def delta_guest_kernel(
    near_span, gf, v, v_x, pr_mid, mid_soft, pr_near, near_soft, _stats, _pgrads,
    mid, pg_mid, near, pg_near,
):
    delta_kernel(gf, v, pr_mid, mid_soft, mid, pg_mid)

    def run(odd):
        if not odd:
            delta_kernel(gf, v_x, pr_near, near_soft, near, pg_near)

    by_parity(near_span, run)


def merge(parts):
    top = parts[0][0]
    for part in parts[1:]:
        top = jnp.maximum(top, part[0])
    factors = [jnp.exp2((part[0] - top) * EXP_SCALE) for part in parts]
    norm, delta = 0.0, 0.0
    for part, factor in zip(parts, factors):
        norm = norm + factor * part[1]
        delta = delta + factor * part[2]
    return (top, norm, delta), factors


def part_of(ref, bias=0.0, base=0):
    return ref[base] + bias, ref[base + 1], ref[base + 2]


def put_norm(outs, factors, merged):
    inverse = 1.0 / merged[1]
    delta = merged[2] * inverse
    for out, factor in zip(outs, factors):
        out[0] = factor * inverse
        out[1] = delta


def bias_kernel(spans, t, a, out):
    flags = Flags(spans, t, a)
    for section in range(SECTIONS):
        out[section] = flags.bias(section, out.shape[1:])


def combine_local_kernel(near_span, bias, own, near, out):
    def run(odd):
        parts = [part_of(own)]
        if odd:
            parts.append(part_of(near, bias[NEAR]))
        merged, _ = merge(parts)
        for index, row in enumerate(merged):
            out[index] = row

    by_parity(near_span, run)


def guest_parts(odd, bias, far, mid, near):
    parts = [part_of(far, bias[FAR]), part_of(mid, bias[MID])]
    return parts if odd else [*parts, part_of(near, bias[NEAR])]


def merge_up_kernel(near_span, bias, far, mid, near, up):
    def run(odd):
        merged, _ = merge(guest_parts(odd, bias, far, mid, near))
        for index, row in enumerate(merged):
            up[index] = row

    by_parity(near_span, run)


def combine_guest_kernel(near_span, bias, guest, far, mid, near, *outs):
    def run(odd):
        merged, factors = merge([*guest_parts(odd, bias, far, mid, near), part_of(guest)])
        put_norm(outs, factors[:-1], merged)

    by_parity(near_span, run)


def combine_own_kernel(spans, bias, own, near, up, *outs):
    held = lax.axis_index("seq") >= spans[MID]

    def run(odd):
        parts = [part_of(own), part_of(up, jnp.where(held, 0.0, -BIG))]
        if odd:
            parts.insert(1, part_of(near, bias[NEAR]))
        merged, factors = merge(parts)
        put_norm(outs, factors[:-1], merged)

    by_parity(spans[NEAR], run)


def pair_terms(head, query, grad, keys, probs, pgrads, norm):
    factor, delta = norm[0, pl.ds(head, 1), :], norm[1, pl.ds(head, 1), :]
    prob = probs[head] * factor
    weight = prob.astype(jnp.bfloat16)
    dlogit = (prob * (pgrads[head] - delta)).astype(jnp.bfloat16)
    return dot(keys, dlogit, 0, 0), dot(dlogit, query, 1, 0), dot(weight, grad, 1, 0)


def self_kernel(q, g, k, norm, probs, pgrads, dq_part, dq, dk, dv):
    def step(head):
        at = columns(head)
        query_term, dk[:, at], dv[:, at] = pair_terms(
            head, q[:, at], g[:, at], k[:, at], probs, pgrads, norm
        )
        dq[:, at] = query_term.T + dq_part[:, at]

    each_head(0, probs.shape[0], step)


def far_terms_kernel(first, q, g, k_up, norm, probs, pgrads, dq, back):
    rows = q.shape[0]

    def step(head):
        at, out = columns(head), columns(head - first)
        query_term, key_term, value_term = pair_terms(
            head, q[:, at], g[:, at], k_up[:, at], probs, pgrads, norm
        )
        dq[:, out] = query_term.T
        back[:rows, out] = (key_term * SCALE).astype(back.dtype)
        back[rows:, out] = value_term.astype(back.dtype)

    each_head(first, back.shape[1] // HDIM, step)


def near_terms_kernel(
    near_span, first, q, g, qf, gf, k_x, norm_own, norm_guest, probs, pgrads, dq, cross
):
    rows = q.shape[0]

    def run(odd):
        query, grad, norm = (q, g, norm_own) if odd else (qf, gf, norm_guest)

        def step(head):
            at, out = columns(head), columns(head - first)
            query_term, key_term, value_term = pair_terms(
                head, query[:, at], grad[:, at], k_x[:, at], probs, pgrads, norm
            )
            dq[:, out] = query_term.T
            cross[:rows, out] = (key_term * SCALE).astype(cross.dtype)
            cross[rows:, out] = value_term.astype(cross.dtype)

        each_head(first, cross.shape[1] // HDIM, step)

    by_parity(near_span, run)


def mid_terms_kernel(
    near_span, first, q, g, k, norm, probs, pgrads, dq_far, dq_near, *refs
):
    guest_dq, own_dq, dk, dv = refs[-4:]

    def run(odd):
        def step(head):
            at, out = columns(head), columns(head - first)
            query_term, dk[:, out], dv[:, out] = pair_terms(
                head, q[:, at], g[:, at], k[:, at], probs, pgrads, norm
            )
            total = query_term.T + dq_far[:, out]
            if not odd:
                total = total + dq_near[:, out]
            guest_dq[:, at] = (total * SCALE).astype(guest_dq.dtype)
            own_dq[:, at] = dq_near[:, out] if odd else jnp.zeros_like(total)

        each_head(first, dk.shape[1] // HDIM, step)

    by_parity(near_span, run)


def step_columns(block, first=0):
    return pl.ds(pl.multiple_of(pl.program_id(0) * block + first, block), block)


def finish_kernel(first, dk, dv, dk_mid, dv_mid, back, cross, *refs):
    key_out, value_out = refs[-2:]
    rows, block = key_out.shape
    here, at = step_columns(block), step_columns(block, first)
    for rows_at, total, out in (
        (slice(0, rows), (dk[:, at] + dk_mid[:, here]) * SCALE, key_out),
        (slice(rows, 2 * rows), dv[:, at] + dv_mid[:, here], value_out),
    ):
        for ref in (back, cross):
            total = total + ref[rows_at, here].astype(jnp.float32)
        out[...] = total.astype(out.dtype)


def finish_query_kernel(dq, guest, out):
    at = step_columns(out.shape[1])
    total = dq[:, at] * SCALE + guest[:, at].astype(jnp.float32)
    out[...] = total.astype(out.dtype)


def body(queries, key_rows, value_rows, out_grad, out_proj, section_table, block_active):
    seq_count = lax.axis_size("seq")
    spans = [seq_count // 2 ** (index + 1) for index in range(SECTIONS)]
    mid_span, near_span = spans[MID], spans[NEAR]
    assert spans[FAR] == 2 * mid_span and mid_span == 2 * near_span
    assert block_active.shape[0] == 1
    rows, cols = queries.shape
    heads = cols // HDIM
    assert heads == sum(GROUPS)
    pair_work = rows * rows * HDIM
    flags = [section_table.T, block_active]

    wide_f32 = ((rows, cols), jnp.float32)
    wide_bf16 = ((rows, cols), jnp.bfloat16)

    def table(count):
        return ((count, heads, rows), jnp.float32)

    stat, norm = table(3), table(2)
    square = ((heads, rows, rows), jnp.float32)
    row_work = heads * rows * HDIM

    def bound(kernel, *fixed):
        def run(*refs):
            kernel(*fixed, *refs)

        return run

    key_up = shift(key_rows, mid_span)
    value_up = shift(value_rows, mid_span)
    key_x = swap(key_rows, "seq", near_span)
    value_x = swap(value_rows, "seq", near_span)
    guest_query = shift(queries, -mid_span)
    grads = attn_grad_of(out_grad, out_proj)
    guest_grad = shift(grads, -mid_span)
    query, key, value = staged(queries, key_rows, value_rows)

    (bias,) = call(bound(bias_kernel, spans), flags, [], [stat], row_work)
    guest_bias = shift(bias, -mid_span)
    self_stats, mid_soft, far_soft, near_soft, *probs, self_pgrad = call(
        bound(soft_kernel, near_span),
        [],
        [query, grads, key, value, guest_query, key_up, key_x],
        [stat] * 4 + [square] * 5,
        heads * 5 * pair_work,
    )
    self_prob, mid_prob, far_prob, near_prob = probs

    near_stats, near_pgrad = call(
        bound(delta_near_kernel, near_span),
        [],
        [grads, value_x, near_prob, near_soft],
        [stat, square],
        heads * pair_work,
    )
    (merged,) = call(
        bound(combine_local_kernel, near_span), [], [bias, self_stats, near_stats], [stat], row_work
    )
    guest_stats = shift(merged, -mid_span)
    ins = [guest_grad, value, value_x, mid_prob, mid_soft, near_prob, near_soft]
    mid_stats, mid_pgrad, near_stats, near_pgrad = call(
        bound(delta_guest_kernel, near_span),
        [],
        [*ins, near_stats, near_pgrad],
        [stat, square] * 2,
        heads * 2 * pair_work,
        {len(ins): 2, len(ins) + 1: 3},
    )
    far_stats, far_pgrad = call(
        delta_kernel,
        [],
        [guest_grad, value_up, far_prob, far_soft],
        [stat, square],
        heads * pair_work,
    )
    parts = [far_stats, mid_stats, near_stats]
    (up_part,) = call(bound(merge_up_kernel, near_span), [], [guest_bias, *parts], [stat], row_work)
    up_stats = shift(up_part, mid_span)
    guest_norms = call(
        bound(combine_guest_kernel, near_span),
        [],
        [guest_bias, guest_stats, *parts],
        [norm] * 3,
        row_work,
    )
    self_norm, near_norm = call(
        bound(combine_own_kernel, spans),
        [],
        [bias, self_stats, near_stats, up_stats],
        [norm] * 2,
        row_work,
    )
    far_norm, mid_norm, near_norm_guest = guest_norms
    near_ins = [query, grads, guest_query, guest_grad, key_x, near_norm, near_norm_guest]
    near_ins += [near_prob, near_pgrad]
    parts, returned = [], []
    first = 0
    for group in GROUPS:
        narrow = ((rows, group * HDIM), jnp.float32)
        half = ((2 * rows, group * HDIM), jnp.bfloat16)
        work = group * 3 * pair_work
        far_query, back = call(
            bound(far_terms_kernel, first),
            [],
            [guest_query, guest_grad, key_up, far_norm, far_prob, far_pgrad],
            [narrow, half],
            work,
        )
        near_query, cross = call(
            bound(near_terms_kernel, near_span, first), [], near_ins, [narrow, half], work
        )
        ins = [guest_query, guest_grad, key, mid_norm, mid_prob, mid_pgrad]
        ins += [far_query, near_query]
        *parts, mid_key, mid_value = call(
            bound(mid_terms_kernel, near_span, first),
            [],
            ins + parts,
            [wide_bf16, wide_f32, narrow, narrow],
            work,
            {len(ins) + number: number for number in range(len(parts))},
        )
        back = shift(back, -mid_span)
        cross = swap(cross, "seq", near_span)
        returned.append((mid_key, mid_value, back, cross))
        first += group
    guest_part, query_part = parts
    guest_part = shift(guest_part, mid_span)
    query_sum, *self_terms = call(
        self_kernel,
        [],
        [query, grads, key, self_norm, self_prob, self_pgrad, query_part],
        [wide_f32] * 3,
        heads * 3 * pair_work,
    )

    block = 2 * HDIM
    outputs = []
    first = 0
    for index, group in enumerate(GROUPS):
        start = first * HDIM
        place_of = start // block
        ins = [*self_terms, *returned[index]]
        outputs = call(
            bound(finish_kernel, start),
            [],
            ins,
            [wide_bf16] * 2,
            group * rows * HDIM * HDIM,
            {len(ins) + number: number for number in range(len(outputs))},
            grid=(group * HDIM // block,),
            streams=[(array, pl.BlockSpec(memory_space=pl.ANY)) for array in outputs],
            blocks=[pl.BlockSpec((rows, block), lambda i, j=place_of: (0, i + j))] * 2,
        )
        first += group
    (query_grad,) = call(
        finish_query_kernel,
        [],
        [query_sum, guest_part],
        [wide_bf16],
        heads * rows * HDIM,
        grid=(cols // block,),
        blocks=[pl.BlockSpec((rows, block), lambda i: (0, i))],
    )
    return query_grad, *outputs


def solution(mesh):
    return jax.shard_map(
        body,
        mesh=mesh,
        in_specs=(
            P("seq", "head"),
            P("seq", "head"),
            P("seq", "head"),
            P("seq", "head"),
            P("head", None),
            P("head", None),
            P("seq", None),
        ),
        out_specs=(P("seq", "head"), P("seq", "head"), P("seq", "head")),
        check_vma=False,
    )
```

```python
import math

import jax
import jax.numpy as jnp
from jax import lax
from jax.experimental import pallas as pl
from jax.experimental.pallas import tpu as pltpu
from jax.sharding import PartitionSpec as P


HDIM = 128
FAR, MID, NEAR = range(3)
SECTIONS = 3
GROUPS = (2, 4, 2)
HEADS_PER_STEP = 8
KERNEL_VMEM = 8 * 2**20
BIG = 1e30
SCALE = 1.0 / math.sqrt(HDIM)
LOG2E = math.log2(math.e)
EXP_SCALE = SCALE * LOG2E


def shift(value, steps):
    count = lax.axis_size("seq")
    low, high = max(0, -steps), min(count, count - steps)
    return lax.ppermute(value, "seq", [(src, src + steps) for src in range(low, high)])


def swap(value, axis, bit):
    pairs = [(src, src ^ bit) for src in range(lax.axis_size(axis))]
    return lax.ppermute(value, axis, pairs)


def dot(lhs, rhs, lhs_dim, rhs_dim):
    return lax.dot_general(
        lhs, rhs, (((lhs_dim,), (rhs_dim,)), ((), ())), preferred_element_type=jnp.float32
    )


def on_chip(array):
    return pltpu.with_memory_space_constraint(array, pltpu.VMEM)


def in_hbm(array):
    return pltpu.with_memory_space_constraint(array, pltpu.HBM)


def call(kernel, scalars, ins, outs, work, aliases=None, grid=None, streams=(), blocks=None, scratch=()):
    smem = pl.BlockSpec(memory_space=pltpu.SMEM)
    vmem = pl.BlockSpec(memory_space=pltpu.VMEM)
    return pl.pallas_call(
        kernel,
        grid=grid or (),
        in_specs=[smem] * len(scalars) + [vmem] * len(ins) + [spec for _, spec in streams],
        out_specs=blocks or [vmem] * len(outs),
        out_shape=[
            (jax.ShapeDtypeStruct if blocks else pltpu.VMEM)(shape, dtype)
            for shape, dtype in outs
        ],
        scratch_shapes=scratch,
        input_output_aliases=aliases or {},
        compiler_params=pltpu.CompilerParams(vmem_limit_bytes=KERNEL_VMEM),
        cost_estimate=pl.CostEstimate(
            flops=2 * work, bytes_accessed=0, transcendentals=work // HDIM
        ),
    )(*scalars, *[on_chip(array) for array in ins], *[array for array, _ in streams])


def each_head(first, count, step):
    width = math.gcd(count, HEADS_PER_STEP)

    def several(index, carry):
        for offset in range(width):
            step(first + index * width + offset)
        return carry

    lax.fori_loop(0, count // width, several, None)


def columns(head):
    return pl.ds(pl.multiple_of(head * HDIM, HDIM), HDIM)


def gathered_pieces(out_grad):
    pieces = {0: out_grad}
    bit = lax.axis_size("head") // 2
    while bit:
        for offset in list(pieces):
            pieces[offset | bit] = swap(pieces[offset], "head", bit)
        bit //= 2
    return [pieces[offset] for offset in range(len(pieces))]


def grad_kernel(*refs):
    head = lax.axis_index("head")
    *piece_refs, own_hbm, proj_hbm, out_ref, own_ref, proj, sems, own_sem = refs
    pieces = [own_ref, *piece_refs]
    width = own_ref.shape[1]
    count = sems.shape[0]
    block = proj.shape[0] // count
    own_copy = pltpu.make_async_copy(own_hbm, own_ref, own_sem)
    own_copy.start()
    copies = []
    for index in range(count):
        at = pl.ds(index * block, block)
        copies.append(pltpu.make_async_copy(proj_hbm.at[at], proj.at[at], sems.at[index]))
    for copy in copies[:2]:
        copy.start()
    own_copy.wait()
    for index, copy in enumerate(copies):
        copy.wait()
        if index + 2 < count:
            copies[index + 2].start()
        at = slice(index * block, (index + 1) * block)
        total = None
        for offset, piece in enumerate(pieces):
            start = pl.multiple_of((head ^ offset) * width, width)
            part = dot(piece[...], proj[at, pl.ds(start, width)], 1, 1)
            total = part if total is None else total + part
        out_ref[:, at] = total.astype(out_ref.dtype)


def attn_grad_of(out_grad, out_proj):
    pieces = gathered_pieces(out_grad)
    rows, width = out_grad.shape
    cols, features = out_proj.shape
    count = cols // (2 * HDIM)
    (result,) = call(
        grad_kernel,
        [],
        pieces[1:],
        [((rows, cols), jnp.bfloat16)],
        rows * cols * features,
        streams=[
            (in_hbm(array), pl.BlockSpec(memory_space=pltpu.HBM)) for array in (out_grad, out_proj)
        ],
        scratch=[
            pltpu.VMEM((rows, width), out_grad.dtype),
            pltpu.VMEM((cols, features), out_proj.dtype),
            pltpu.SemaphoreType.DMA((count,)),
            pltpu.SemaphoreType.DMA,
        ],
    )
    return result


def stage_kernel(*refs):
    count = len(refs) // 3
    sources, targets, sems = refs[:count], refs[count : 2 * count], refs[2 * count :]
    copies = [pltpu.make_async_copy(*each) for each in zip(sources, targets, sems)]
    for copy in copies:
        copy.start()
    for copy in copies:
        copy.wait()


def staged(*arrays):
    return pl.pallas_call(
        stage_kernel,
        in_specs=[pl.BlockSpec(memory_space=pltpu.HBM)] * len(arrays),
        out_specs=[pl.BlockSpec(memory_space=pltpu.VMEM)] * len(arrays),
        out_shape=[pltpu.VMEM(array.shape, array.dtype) for array in arrays],
        scratch_shapes=[pltpu.SemaphoreType.DMA] * len(arrays),
        compiler_params=pltpu.CompilerParams(vmem_limit_bytes=KERNEL_VMEM),
        cost_estimate=pl.CostEstimate(flops=10**6, bytes_accessed=0, transcendentals=0),
        name="stage",
    )(*[in_hbm(array) for array in arrays])


def causal(raw, fill):
    key_at = lax.broadcasted_iota(jnp.int32, raw.shape, 0)
    query_at = lax.broadcasted_iota(jnp.int32, raw.shape, 1)
    return jnp.where(key_at <= query_at, raw, fill)


class Flags:
    def __init__(self, spans, table_ref, active_ref):
        self.spans, self.table, self.active = spans, table_ref, active_ref
        self.place = lax.axis_index("seq")

    def usable(self, head, section):
        used = self.table[section, head] * self.active[0, section] > 0
        return used & (self.place >= self.spans[section])

    def bias(self, section, shape):
        head_at = lax.broadcasted_iota(jnp.int32, shape, 0)
        total = jnp.zeros(shape, jnp.float32)
        for head in range(shape[0]):
            value = jnp.where(self.usable(head, section), 0.0, -BIG)
            total = jnp.where(head_at == head, value, total)
        return total


def by_parity(near_span, run):
    odd = (lax.axis_index("seq") // near_span) % 2 == 1
    pl.when(odd)(lambda: run(True))
    pl.when(jnp.logical_not(odd))(lambda: run(False))


def soft_set(head, keys, query, probs, stats, base=0, diagonal=False):
    raw = dot(keys, query, 1, 1)
    if diagonal:
        raw = causal(raw, -BIG)
    top = jnp.max(raw, axis=0, keepdims=True)
    prob = jnp.exp2((raw - top) * EXP_SCALE)
    probs[head] = prob
    stats[base, pl.ds(head, 1), :] = top
    stats[base + 1, pl.ds(head, 1), :] = jnp.sum(prob, axis=0, keepdims=True)


def delta_set(head, values, grad, probs, pgrads, stats, base=0):
    pgrad = dot(values, grad, 1, 1)
    pgrads[head] = pgrad
    row = jnp.sum(probs[head] * pgrad, axis=0, keepdims=True)
    stats[base + 2, pl.ds(head, 1), :] = row


def soft_kernel(near_span, q, g, k, v, qf, k_up, k_x, *refs):
    own, mid, far, near, pr_own, pr_mid, pr_far, pr_near, pg_own = refs

    def run(odd):
        def step(head):
            at = columns(head)
            key_up, query, guest = k_up[:, at], q[:, at], qf[:, at]
            soft_set(head, k[:, at], query, pr_own, own, diagonal=True)
            delta_set(head, v[:, at], g[:, at], pr_own, pg_own, own)
            soft_set(head, k[:, at], guest, pr_mid, mid)
            soft_set(head, key_up, guest, pr_far, far)
            soft_set(head, k_x[:, at], query if odd else guest, pr_near, near)

        each_head(0, pg_own.shape[0], step)

    by_parity(near_span, run)


def delta_kernel(g, values, probs, soft, stats, pgrads):
    stats[0:2] = soft[0:2]

    def step(head):
        at = columns(head)
        delta_set(head, values[:, at], g[:, at], probs, pgrads, stats)

    each_head(0, probs.shape[0], step)


def delta_near_kernel(near_span, g, v_x, probs, soft, stats, pgrads):
    def run(odd):
        if odd:
            delta_kernel(g, v_x, probs, soft, stats, pgrads)

    by_parity(near_span, run)


def delta_guest_kernel(
    near_span, gf, v, v_x, pr_mid, mid_soft, pr_near, near_soft, _stats, _pgrads,
    mid, pg_mid, near, pg_near,
):
    delta_kernel(gf, v, pr_mid, mid_soft, mid, pg_mid)

    def run(odd):
        if not odd:
            delta_kernel(gf, v_x, pr_near, near_soft, near, pg_near)

    by_parity(near_span, run)


def merge(parts):
    top = parts[0][0]
    for part in parts[1:]:
        top = jnp.maximum(top, part[0])
    factors = [jnp.exp2((part[0] - top) * EXP_SCALE) for part in parts]
    norm, delta = 0.0, 0.0
    for part, factor in zip(parts, factors):
        norm = norm + factor * part[1]
        delta = delta + factor * part[2]
    return (top, norm, delta), factors


def part_of(ref, bias=0.0, base=0):
    return ref[base] + bias, ref[base + 1], ref[base + 2]


def put_norm(outs, factors, merged):
    inverse = 1.0 / merged[1]
    delta = merged[2] * inverse
    for out, factor in zip(outs, factors):
        out[0] = factor * inverse
        out[1] = delta


def bias_kernel(spans, t, a, out):
    flags = Flags(spans, t, a)
    for section in range(SECTIONS):
        out[section] = flags.bias(section, out.shape[1:])


def combine_local_kernel(near_span, bias, own, near, out):
    lane = lax.broadcasted_iota(jnp.int32, bias.shape[1:], 1)
    out[3] = jnp.where(lane == FAR, bias[FAR], jnp.where(lane == MID, bias[MID], bias[NEAR]))

    def run(odd):
        parts = [part_of(own)]
        if odd:
            parts.append(part_of(near, bias[NEAR]))
        merged, _ = merge(parts)
        for index, row in enumerate(merged):
            out[index] = row

    by_parity(near_span, run)


def combine_guest_kernel(near_span, guest, far, mid, near, up, *outs):
    def run(odd):
        def bias(section):
            return guest[3][:, section : section + 1]

        parts = [part_of(far, bias(FAR)), part_of(mid, bias(MID))]
        if not odd:
            parts.append(part_of(near, bias(NEAR)))
        merged, _ = merge(parts)
        for index, row in enumerate(merged):
            up[index] = row
        merged, factors = merge([*parts, part_of(guest)])
        put_norm(outs, factors[:-1], merged)

    by_parity(near_span, run)


def combine_own_kernel(spans, bias, own, near, up, *outs):
    held = lax.axis_index("seq") >= spans[MID]

    def run(odd):
        parts = [part_of(own), part_of(up, jnp.where(held, 0.0, -BIG))]
        if odd:
            parts.insert(1, part_of(near, bias[NEAR]))
        merged, factors = merge(parts)
        put_norm(outs, factors[:-1], merged)

    by_parity(spans[NEAR], run)


def pair_terms(head, query, grad, keys, probs, pgrads, norm):
    factor, delta = norm[0, pl.ds(head, 1), :], norm[1, pl.ds(head, 1), :]
    prob = probs[head] * factor
    weight = prob.astype(jnp.bfloat16)
    dlogit = (prob * (pgrads[head] - delta)).astype(jnp.bfloat16)
    return dot(keys, dlogit, 0, 0), dot(dlogit, query, 1, 0), dot(weight, grad, 1, 0)


def self_kernel(q, g, k, norm, probs, pgrads, dq_part, dq, dk, dv):
    def step(head):
        at = columns(head)
        query_term, dk[:, at], dv[:, at] = pair_terms(
            head, q[:, at], g[:, at], k[:, at], probs, pgrads, norm
        )
        dq[:, at] = query_term.T + dq_part[:, at]

    each_head(0, probs.shape[0], step)


def far_terms_kernel(first, q, g, k_up, norm, probs, pgrads, dq, back):
    rows = q.shape[0]

    def step(head):
        at, out = columns(head), columns(head - first)
        query_term, key_term, value_term = pair_terms(
            head, q[:, at], g[:, at], k_up[:, at], probs, pgrads, norm
        )
        dq[:, out] = query_term.T
        back[:rows, out] = (key_term * SCALE).astype(back.dtype)
        back[rows:, out] = value_term.astype(back.dtype)

    each_head(first, back.shape[1] // HDIM, step)


def near_terms_kernel(
    near_span, first, q, g, qf, gf, k_x, norm_own, norm_guest, probs, pgrads, dq, cross
):
    rows = q.shape[0]

    def run(odd):
        query, grad, norm = (q, g, norm_own) if odd else (qf, gf, norm_guest)

        def step(head):
            at, out = columns(head), columns(head - first)
            query_term, key_term, value_term = pair_terms(
                head, query[:, at], grad[:, at], k_x[:, at], probs, pgrads, norm
            )
            dq[:, out] = query_term.T
            cross[:rows, out] = (key_term * SCALE).astype(cross.dtype)
            cross[rows:, out] = value_term.astype(cross.dtype)

        each_head(first, cross.shape[1] // HDIM, step)

    by_parity(near_span, run)


def mid_terms_kernel(
    near_span, first, q, g, k, norm, probs, pgrads, dq_far, dq_near, *refs
):
    guest_dq, own_dq, dk, dv = refs[-4:]

    def run(odd):
        def step(head):
            at, out = columns(head), columns(head - first)
            query_term, dk[:, out], dv[:, out] = pair_terms(
                head, q[:, at], g[:, at], k[:, at], probs, pgrads, norm
            )
            total = query_term.T + dq_far[:, out]
            if not odd:
                total = total + dq_near[:, out]
            guest_dq[:, at] = (total * SCALE).astype(guest_dq.dtype)
            own_dq[:, at] = dq_near[:, out] if odd else jnp.zeros_like(total)

        each_head(first, dk.shape[1] // HDIM, step)

    by_parity(near_span, run)


def step_columns(block, first=0):
    return pl.ds(pl.multiple_of(pl.program_id(0) * block + first, block), block)


def finish_kernel(first, dk, dv, dk_mid, dv_mid, back, cross, *refs):
    key_out, value_out = refs[-2:]
    rows, block = key_out.shape
    here, at = step_columns(block), step_columns(block, first)
    for rows_at, total, out in (
        (slice(0, rows), (dk[:, at] + dk_mid[:, here]) * SCALE, key_out),
        (slice(rows, 2 * rows), dv[:, at] + dv_mid[:, here], value_out),
    ):
        for ref in (back, cross):
            total = total + ref[rows_at, here].astype(jnp.float32)
        out[...] = total.astype(out.dtype)


def finish_query_kernel(dq, guest, out):
    at = step_columns(out.shape[1])
    total = dq[:, at] * SCALE + guest[:, at].astype(jnp.float32)
    out[...] = total.astype(out.dtype)


def body(queries, key_rows, value_rows, out_grad, out_proj, section_table, block_active):
    seq_count = lax.axis_size("seq")
    spans = [seq_count // 2 ** (index + 1) for index in range(SECTIONS)]
    mid_span, near_span = spans[MID], spans[NEAR]
    assert spans[FAR] == 2 * mid_span and mid_span == 2 * near_span
    assert block_active.shape[0] == 1
    rows, cols = queries.shape
    heads = cols // HDIM
    assert heads == sum(GROUPS)
    pair_work = rows * rows * HDIM
    flags = [section_table.T, block_active]

    wide_f32 = ((rows, cols), jnp.float32)
    wide_bf16 = ((rows, cols), jnp.bfloat16)

    def table(count):
        return ((count, heads, rows), jnp.float32)

    stat, norm = table(3), table(2)
    square = ((heads, rows, rows), jnp.float32)
    row_work = heads * rows * HDIM

    def bound(kernel, *fixed):
        def run(*refs):
            kernel(*fixed, *refs)

        return run

    key_up = shift(key_rows, mid_span)
    value_up = shift(value_rows, mid_span)
    key_x = swap(key_rows, "seq", near_span)
    value_x = swap(value_rows, "seq", near_span)
    guest_query = shift(queries, -mid_span)
    grads = attn_grad_of(out_grad, out_proj)
    guest_grad = shift(grads, -mid_span)
    query, key, value = staged(queries, key_rows, value_rows)

    (bias,) = call(bound(bias_kernel, spans), flags, [], [stat], row_work)
    self_stats, mid_soft, far_soft, near_soft, *probs, self_pgrad = call(
        bound(soft_kernel, near_span),
        [],
        [query, grads, key, value, guest_query, key_up, key_x],
        [stat] * 4 + [square] * 5,
        heads * 5 * pair_work,
    )
    self_prob, mid_prob, far_prob, near_prob = probs

    near_stats, near_pgrad = call(
        bound(delta_near_kernel, near_span),
        [],
        [grads, value_x, near_prob, near_soft],
        [stat, square],
        heads * pair_work,
    )
    (merged,) = call(
        bound(combine_local_kernel, near_span),
        [],
        [bias, self_stats, near_stats],
        [table(4)],
        row_work,
    )
    guest_stats = shift(merged, -mid_span)
    ins = [guest_grad, value, value_x, mid_prob, mid_soft, near_prob, near_soft]
    mid_stats, mid_pgrad, near_stats, near_pgrad = call(
        bound(delta_guest_kernel, near_span),
        [],
        [*ins, near_stats, near_pgrad],
        [stat, square] * 2,
        heads * 2 * pair_work,
        {len(ins): 2, len(ins) + 1: 3},
    )
    far_stats, far_pgrad = call(
        delta_kernel,
        [],
        [guest_grad, value_up, far_prob, far_soft],
        [stat, square],
        heads * pair_work,
    )
    up_part, *guest_norms = call(
        bound(combine_guest_kernel, near_span),
        [],
        [guest_stats, far_stats, mid_stats, near_stats],
        [stat] + [norm] * 3,
        row_work,
    )
    up_stats = shift(up_part, mid_span)
    self_norm, near_norm = call(
        bound(combine_own_kernel, spans),
        [],
        [bias, self_stats, near_stats, up_stats],
        [norm] * 2,
        row_work,
    )
    far_norm, mid_norm, near_norm_guest = guest_norms
    near_ins = [query, grads, guest_query, guest_grad, key_x, near_norm, near_norm_guest]
    near_ins += [near_prob, near_pgrad]
    parts, returned = [], []
    first = 0
    for group in GROUPS:
        narrow = ((rows, group * HDIM), jnp.float32)
        half = ((2 * rows, group * HDIM), jnp.bfloat16)
        work = group * 3 * pair_work
        far_query, back = call(
            bound(far_terms_kernel, first),
            [],
            [guest_query, guest_grad, key_up, far_norm, far_prob, far_pgrad],
            [narrow, half],
            work,
        )
        near_query, cross = call(
            bound(near_terms_kernel, near_span, first), [], near_ins, [narrow, half], work
        )
        ins = [guest_query, guest_grad, key, mid_norm, mid_prob, mid_pgrad]
        ins += [far_query, near_query]
        *parts, mid_key, mid_value = call(
            bound(mid_terms_kernel, near_span, first),
            [],
            ins + parts,
            [wide_bf16, wide_f32, narrow, narrow],
            work,
            {len(ins) + number: number for number in range(len(parts))},
        )
        back = shift(back, -mid_span)
        cross = swap(cross, "seq", near_span)
        returned.append((mid_key, mid_value, back, cross))
        first += group
    guest_part, query_part = parts
    guest_part = shift(guest_part, mid_span)
    query_sum, *self_terms = call(
        self_kernel,
        [],
        [query, grads, key, self_norm, self_prob, self_pgrad, query_part],
        [wide_f32] * 3,
        heads * 3 * pair_work,
    )

    block = 2 * HDIM
    outputs = []
    first = 0
    for index, group in enumerate(GROUPS):
        start = first * HDIM
        place_of = start // block
        ins = [*self_terms, *returned[index]]
        outputs = call(
            bound(finish_kernel, start),
            [],
            ins,
            [wide_bf16] * 2,
            group * rows * HDIM * HDIM,
            {len(ins) + number: number for number in range(len(outputs))},
            grid=(group * HDIM // block,),
            streams=[(array, pl.BlockSpec(memory_space=pl.ANY)) for array in outputs],
            blocks=[pl.BlockSpec((rows, block), lambda i, j=place_of: (0, i + j))] * 2,
        )
        first += group
    (query_grad,) = call(
        finish_query_kernel,
        [],
        [query_sum, guest_part],
        [wide_bf16],
        heads * rows * HDIM,
        grid=(cols // block,),
        blocks=[pl.BlockSpec((rows, block), lambda i: (0, i))],
    )
    return query_grad, *outputs


def solution(mesh):
    return jax.shard_map(
        body,
        mesh=mesh,
        in_specs=(
            P("seq", "head"),
            P("seq", "head"),
            P("seq", "head"),
            P("seq", "head"),
            P("head", None),
            P("head", None),
            P("seq", None),
        ),
        out_specs=(P("seq", "head"), P("seq", "head"), P("seq", "head")),
        check_vma=False,
    )
```
